256 devices in a mesh: pb: 16 (over x, y), wa: 16 (over z, core).
Axes of the slice: x: 4, y: 4, z: 8, core: 2. Of those that a mesh axis runs over, the one named last changes fastest.
Arguments:
- quartets: int32 [8192, 4, 128], P(('pb', 'wa')), may hold values from -1 to 49151, as said below
- counts: int32 [256], P(('pb', 'wa')), may hold values from 1 to 32, as said below
- eig: bfloat16 [24, 49152], P(None, 'pb'), may hold values from -1.1953125 to 1.1953125
- freq: bfloat16 [49152], P('pb'), may hold values from 0.5 to 2
- phi: bfloat16 [144, 1152], replicated, may hold values from -0.5390625 to 0.5390625
- cells: int32 [8, 9], replicated, may hold values from -2 to 2
Outputs:
- rates: float32 [49152], P(('pb', 'wa'))
The draws below stay inside these ranges and needn't reach their ends.
Inputs may be any that keep to these rules, and one draw needn't show every extreme that they name: quartets[b, 0, n] is a mode of one of the 256 q-points of the owner group of slot b (from 0 to 3071); the other three entries are all -1 or all modes of the mesh, and then their q-points and that of the first add up as q1 + q2 = q3 + q4 on the mesh. The used slots of a device are its first counts slots; some device has exactly 32.
All inputs are finite; a program needn't handle non-finite values.
Results may differ from the reference program's by a relative error of at most 0.0023.
Values may be sent and summed in bfloat16 or wider, within the bound.
A program may use at most 64 MiB of HBM per device.

```python
import math
import jax
import jax.numpy as jnp
from jax import lax

QMESH = 16
BRANCHES = 12
CLUSTERS = 8
BLOCK = 128
BLK_DEV = 32
NQ = 4096
NMODE = 49152
Q_DEV = 256
WORKERS = 256
SHARD_BLK = 512
NBLK = 8192


def mesh_point(across, along, upward):
    return (across * QMESH + along) * QMESH + upward


def draw_quartets(key, part):
    local_q = jax.random.randint(jax.random.fold_in(key, 1), (NBLK, 1), 0, Q_DEV)
    owner = (jnp.arange(NBLK, dtype=jnp.int32) // SHARD_BLK)[:, None]
    first_q = owner * Q_DEV + local_q
    second_q = jax.random.randint(jax.random.fold_in(key, 2), (NBLK, BLOCK), 0, NQ)
    third_q = jax.random.randint(jax.random.fold_in(key, 3), (NBLK, BLOCK), 0, NQ)
    square = QMESH * QMESH
    fourth_q = mesh_point(jnp.remainder(first_q // square + second_q // square - third_q // square, QMESH), jnp.remainder(first_q // QMESH % QMESH + second_q // QMESH % QMESH - third_q // QMESH % QMESH, QMESH), jnp.remainder(first_q % QMESH + second_q % QMESH - third_q % QMESH, QMESH))
    branch_draw = jax.random.randint(jax.random.fold_in(key, 4), (4, NBLK, BLOCK), 0, BRANCHES)
    pad_length = jax.random.randint(jax.random.fold_in(key, 5), (NBLK, 1), 0, BLOCK // 2 + 1)
    padded = jnp.arange(BLOCK, dtype=jnp.int32)[None, :] >= BLOCK - pad_length
    first_mode = local_q * BRANCHES + branch_draw[0]
    second_mode = jnp.where(padded, -1, second_q * BRANCHES + branch_draw[1])
    third_mode = jnp.where(padded, -1, third_q * BRANCHES + branch_draw[2])
    fourth_mode = jnp.where(padded, -1, fourth_q * BRANCHES + branch_draw[3])
    return jnp.stack([first_mode, second_mode, third_mode, fourth_mode], axis=1).astype(jnp.int32)


def draw_counts(key, part):
    first_draw = jax.random.randint(jax.random.fold_in(key, 11), (WORKERS,), 1, BLK_DEV + 1)
    second_draw = jax.random.randint(jax.random.fold_in(key, 12), (WORKERS,), 1, BLK_DEV + 1)
    chosen = jax.random.randint(jax.random.fold_in(key, 13), (), 0, WORKERS)
    tally = jnp.maximum(1, first_draw * second_draw // BLK_DEV)
    tally = jnp.where(jnp.arange(WORKERS, dtype=jnp.int32) == chosen, BLK_DEV, tally)
    return tally.astype(jnp.int32)


def with_ends(values, key, low, high):
    place = [jax.random.randint(jax.random.fold_in(key, axis), (), 0, length) for axis, length in enumerate(values.shape)]
    widest = values.shape.index(max(values.shape))
    beside = place[:widest] + [(place[widest] + 1) % values.shape[widest]] + place[widest + 1:]
    return values.at[tuple(place)].set(low).at[tuple(beside)].set(high)


def steps_of(rng, extent, shards, low, largest):
    def one(position, shards_of):
        steps = jax.random.uniform(jax.random.fold_in(jax.random.fold_in(rng, 6), position), (shards_of,), jnp.float32, low / len(shards), largest / len(shards))
        return jnp.repeat(jnp.exp(steps), extent[position] // shards_of).reshape((-1,) + (1,) * (len(extent) - position - 1))

    factor_of = one(*shards[0])
    for cut in shards[1:]:
        factor_of = factor_of * one(*cut)
    return factor_of


def centred(rng, extent, spread, limit, shards=(), held_as=jnp.bfloat16):
    drawn = jax.random.normal(rng, extent, jnp.float32) * spread
    if len(shards) > 0:
        drawn = steps_of(rng, extent, shards, -0.22, 0.18) * drawn
    return jnp.clip(drawn, min=-limit, max=limit).astype(held_as)


def setup_inputs(seed: int = 0) -> dict:
    key_list = jax.random.split(jax.random.key(seed), 7)
    return {
        "quartets": draw_quartets(jax.random.fold_in(key_list[6], 71), 0),
        "counts": draw_counts(jax.random.fold_in(key_list[6], 71), 0),
        "eig": centred(key_list[2], (2 * BRANCHES, NMODE), 0.2, 1.1953125, ((1, 16),)),
        "freq": jnp.clip(jnp.exp(math.log(2.0) - 1.3862944 * jax.random.uniform(key_list[3], (NMODE,), jnp.float32) ** steps_of(key_list[3], (NMODE,), ((0, 16),), -0.2, 0.2)), 0.5, 2.0).astype(jnp.bfloat16),
        "phi": centred(key_list[4], (BRANCHES * BRANCHES, CLUSTERS * BRANCHES * BRANCHES), 0.09, 0.5390625),
        "cells": with_ends(jax.random.randint(key_list[5], (CLUSTERS, 9), -2, 3), jax.random.fold_in(key_list[5], 1), -2, 2).astype(jnp.int32),
    }


smearing = 0.5

def outer_pair(first, second, branches):
    count = first.shape[1]
    first_re = first[:branches][:, None, :]
    first_im = first[branches:][:, None, :]
    second_re = second[:branches][None, :, :]
    second_im = second[branches:][None, :, :]
    real = (first_re * second_re - first_im * second_im).reshape(branches * branches, count)
    imag = (first_re * second_im + first_im * second_re).reshape(branches * branches, count)
    return (real, imag)

def cluster_phase(other_modes, cells, branches):
    points = other_modes // branches
    coords = [points // (QMESH * QMESH), points // QMESH % QMESH, points % QMESH]
    shift = jnp.zeros((cells.shape[0], other_modes.shape[1]), jnp.int32)
    for which in range(3):
        sign = 1 if which == 0 else -1
        for axis_c in range(3):
            shift = shift + sign * cells[:, 3 * which + axis_c][:, None] * coords[axis_c][which][None, :]
    angle = jnp.remainder(shift, QMESH).astype(jnp.float32) * (2.0 * math.pi / QMESH)
    return (jnp.cos(angle), jnp.sin(angle))

def occupation(value):
    return 1.0 / (jnp.exp(value) - 1.0)

def contributions(first_modes, other_modes, other_spots, valid, first_vectors, first_freqs, vectors, frequencies, phi, cells):
    branches = vectors.shape[0] // 2
    count = first_modes.shape[0]
    clusters = cells.shape[0]
    first_vec = jnp.take(first_vectors, first_modes, axis=1).astype(jnp.float32)
    first_freq = jnp.take(first_freqs, first_modes).astype(jnp.float32)
    flat_spots = other_spots.reshape(3 * count)
    gathered = jnp.take(vectors, flat_spots, axis=1).astype(jnp.float32)
    other_freq = jnp.take(frequencies, flat_spots).astype(jnp.float32).reshape(3, count)
    second_vec = gathered[:, :count]
    third_vec = gathered[:, count:2 * count]
    fourth_vec = gathered[:, 2 * count:]
    far_re, far_im = outer_pair(third_vec, fourth_vec, branches)
    far_im = -far_im
    cosine, sine = cluster_phase(other_modes, cells, branches)
    wide_re = cosine[:, None, :] * far_re[None] - sine[:, None, :] * far_im[None]
    wide_im = cosine[:, None, :] * far_im[None] + sine[:, None, :] * far_re[None]
    wide_re = wide_re.reshape(clusters * branches * branches, count).astype(jnp.bfloat16)
    wide_im = wide_im.reshape(clusters * branches * branches, count).astype(jnp.bfloat16)
    weighted_re = jnp.dot(phi, wide_re, preferred_element_type=jnp.float32)
    weighted_im = jnp.dot(phi, wide_im, preferred_element_type=jnp.float32)
    near_re, near_im = outer_pair(first_vec, second_vec, branches)
    value_re = lax.optimization_barrier(jnp.sum(near_re * weighted_re - near_im * weighted_im, axis=0))
    value_im = lax.optimization_barrier(jnp.sum(near_re * weighted_im + near_im * weighted_re, axis=0))
    mismatch = first_freq + other_freq[0] - other_freq[1] - other_freq[2]
    delta = jnp.exp(-(mismatch / smearing) ** 2) / (smearing * math.sqrt(math.pi))
    weight = (1.0 + occupation(other_freq[0])) * occupation(other_freq[1]) * occupation(other_freq[2]) / occupation(first_freq)
    product = first_freq * other_freq[0] * other_freq[1] * other_freq[2]
    return jnp.where(valid, (value_re * value_re + value_im * value_im) * delta * weight / product, 0.0)

def reference(quartets, counts, eig, freq, phi, cells):
    total_blocks = quartets.shape[0]
    block = quartets.shape[2]
    group = math.gcd(BLK_DEV, 16)
    index = jnp.arange(total_blocks, dtype=jnp.int32)
    used = index % BLK_DEV < jnp.take(counts, index // BLK_DEV)
    rank = (jnp.cumsum(used.astype(jnp.int32)) - 1).astype(jnp.int32)
    target = jnp.where(used, rank, total_blocks).astype(jnp.int32)
    order = jnp.zeros((total_blocks,), jnp.int32).at[target].set(index, mode='drop')
    total = jnp.sum(used.astype(jnp.int32)).astype(jnp.int32)
    offsets = (index // SHARD_BLK * (Q_DEV * BRANCHES)).astype(jnp.int32)
    rounds = (total + group - 1) // group

    def one_round(step, rates):
        start = (step * group).astype(jnp.int32)
        picks = lax.dynamic_slice_in_dim(order, start, group, 0)
        blocks = jnp.take(quartets, picks, axis=0)
        live = start + jnp.arange(group, dtype=jnp.int32) < total
        first_modes = (blocks[:, 0, :] + jnp.take(offsets, picks)[:, None]).reshape(group * block)
        others = jnp.transpose(blocks[:, 1:, :], (1, 0, 2)).reshape(3, group * block)
        valid = (others[0] >= 0) & jnp.repeat(live, block)
        clamped = jnp.maximum(others, 0)
        terms = contributions(first_modes, clamped, clamped, valid, eig, freq, eig, freq, phi, cells)
        return rates.at[first_modes].add(terms)
    return lax.fori_loop(0, rounds, one_round, jnp.zeros((eig.shape[1],), jnp.float32))
```

```python
import functools
import math

import jax
import jax.numpy as jnp
import numpy as np
from jax import lax
from jax.experimental import pallas as pl
from jax.experimental.pallas import tpu as pltpu
from jax.sharding import PartitionSpec as P

QMESH = 16
BR = 12
NB = 16
LOCAL = 3072
GROUP = 768
LANES = 128
GROUP_AT = (0, 768, 1664, 2432)
FREQ_AT = 1536
WIDTH = 3200
SMEARING = 0.5
MESH = pl.DeviceIdType.MESH
NT = (((1,), (1,)), ((), ()))


def exchange_kernel(eig, freq, quartets, counts, tab, blocks, tallies, mine, send, got, lent, got_q, got_c, local):
    pb, wa = lax.axis_index("pb"), lax.axis_index("wa")
    x, y, core = pb // 4, pb % 4, wa % 2
    ahead = 1 - 2 * core
    sibling = (pb, wa + ahead)

    def place(dx, dy):
        return lax.rem(x + dx + 4, 4) * 4 + lax.rem(y + dy + 4, 4)

    mine[...] = jnp.full((1, LANES), counts[0], jnp.int32)

    barrier = pltpu.get_barrier_semaphore()
    for step in (1, -1):
        pl.semaphore_signal(barrier, inc=1, device_id=(place(step, 0), wa), device_id_type=MESH)
        pl.semaphore_signal(barrier, inc=1, device_id=(place(0, step), wa), device_id_type=MESH)
    for k in range(1, NB):
        pl.semaphore_signal(barrier, inc=1, device_id=(pb, lax.rem(wa + k, NB)), device_id_type=MESH)

    own = [
        pltpu.make_async_copy(eig.at[:, pl.ds(0, 1536)], tab.at[pb, :, pl.ds(0, 1536)], local.at[0]),
        pltpu.make_async_copy(eig.at[:, pl.ds(1536, 1536)], tab.at[pb, :, pl.ds(1664, 1536)], local.at[1]),
        pltpu.make_async_copy(freq, tab.at[pb, :, pl.ds(FREQ_AT, LANES)], local.at[2]),
        pltpu.make_async_copy(quartets.at[:, 0], blocks.at[wa], local.at[3]),
        pltpu.make_async_copy(mine, tallies.at[wa], local.at[4]),
    ]
    for copy in own:
        copy.start()
    for copy in own:
        copy.wait()

    pl.semaphore_wait(barrier, 4 + NB - 1)

    sent = []

    def push(src, dst, sem, device):
        copy = pltpu.make_async_remote_copy(
            src_ref=src, dst_ref=dst, send_sem=send.at[len(sent)], recv_sem=sem, device_id=device, device_id_type=MESH
        )
        copy.start()
        sent.append(copy)

    def piece(part, shard):
        if part == 0:
            return tab.at[shard, :, pl.ds(pl.multiple_of(core * 2432, LANES), 768)]
        return tab.at[shard, :, pl.ds(pl.multiple_of(768 + core * 768, LANES), 896)]

    def half(part, shard):
        if part == 0:
            return piece(part, shard)
        return tab.at[shard, :, pl.ds(pl.multiple_of(768 + core * 896, LANES), 768)]

    def half_of_sibling(part, shard):
        if part == 0:
            return tab.at[shard, :, pl.ds(pl.multiple_of((1 - core) * 2432, LANES), 768)]
        return tab.at[shard, :, pl.ds(pl.multiple_of(768 + (1 - core) * 896, LANES), 768)]

    def at(part, first, second):
        return place(first, second) if part == 0 else place(second, first)

    def relay(part, shard, first, second):
        view = piece(part, shard)
        push(view, view, got.at[part, shard], (at(part, first, second), wa))

    def lend(part, shard):
        view = half(part, shard)
        push(view, view, lent.at[part, shard], sibling)

    def arrived(part, shard):
        view = piece(part, shard)
        pltpu.make_async_remote_copy(
            src_ref=view, dst_ref=view, send_sem=send.at[0], recv_sem=got.at[part, shard], device_id=sibling, device_id_type=MESH
        ).wait_recv()

    def second_both(part, shard):
        relay(part, shard, 0, ahead)
        relay(part, shard, 0, -ahead)

    for part in (0, 1):
        relay(part, pb, ahead, 0)
        relay(part, pb, -ahead, 0)
    for part in (0, 1):
        second_both(part, pb)
    for k in range(1, NB):
        peer = lax.rem(wa + k, NB)
        push(quartets.at[:, k], blocks.at[wa], got_q.at[wa], (pb, peer))
        push(mine, tallies.at[wa], got_c.at[wa], (pb, peer))

    def first_axis(part, step):
        shard = at(part, step, 0)
        arrived(part, shard)
        if step is back:
            relay(part, shard, ahead, 0)
        second_both(part, shard)
        lend(part, shard)

    def second_axis(part, row, step):
        shard = at(part, row, step)
        arrived(part, shard)
        if step is back:
            relay(part, shard, 0, ahead)
        lend(part, shard)

    back, fore = -ahead, ahead
    order = [
        (first_axis, (back,)),
        (first_axis, (fore,)),
        (second_axis, (0, back)),
        (second_axis, (0, fore)),
        (first_axis, (2,)),
        (second_axis, (back, back)),
        (second_axis, (back, fore)),
        (second_axis, (0, 2)),
        (second_axis, (fore, back)),
        (second_axis, (fore, fore)),
        (second_axis, (back, 2)),
        (second_axis, (2, back)),
        (second_axis, (2, fore)),
        (second_axis, (fore, 2)),
        (second_axis, (2, 2)),
    ]
    for what, where in order:
        for part in (0, 1):
            what(part, *where)

    for k in range(1, NB):
        peer = lax.rem(wa + k, NB)
        for dst, sem in ((blocks.at[peer], got_q.at[peer]), (tallies.at[peer], got_c.at[peer])):
            pltpu.make_async_remote_copy(
                src_ref=dst, dst_ref=dst, send_sem=send.at[0], recv_sem=sem, device_id=sibling, device_id_type=MESH
            ).wait_recv()
    for part in (0, 1):
        for k in range(1, NB):
            shard = lax.rem(pb + k, NB)
            view = half_of_sibling(part, shard)
            pltpu.make_async_remote_copy(
                src_ref=view, dst_ref=view, send_sem=send.at[0], recv_sem=lent.at[part, shard], device_id=sibling, device_id_type=MESH
            ).wait_recv()
    for copy in sent:
        copy.wait_send()


def exchange(eig, freq, quartets, counts):
    any_space = pl.BlockSpec(memory_space=pl.ANY)
    vmem = pl.BlockSpec(memory_space=pltpu.VMEM)
    return pl.pallas_call(
        exchange_kernel,
        out_shape=(
            pltpu.VMEM((NB, 24, WIDTH), jnp.bfloat16),
            pltpu.VMEM((NB, 2, 4, LANES), jnp.int32),
            pltpu.VMEM((NB, 1, LANES), jnp.int32),
        ),
        in_specs=[any_space, any_space, any_space, pl.BlockSpec(memory_space=pltpu.SMEM)],
        out_specs=(vmem, vmem, vmem),
        scratch_shapes=[
            pltpu.VMEM((1, LANES), jnp.int32),
            pltpu.SemaphoreType.DMA((120,)),
            pltpu.SemaphoreType.DMA((2, NB)),
            pltpu.SemaphoreType.DMA((2, NB)),
            pltpu.SemaphoreType.DMA((NB,)),
            pltpu.SemaphoreType.DMA((NB,)),
            pltpu.SemaphoreType.DMA((5,)),
        ],
        compiler_params=pltpu.CompilerParams(collective_id=0, has_side_effects=True, vmem_limit_bytes=8 << 20),
        name="exchange",
    )(eig, freq, quartets, counts)


def selection(rows, columns, hit):
    r, c = np.meshgrid(np.arange(rows), np.arange(columns), indexing="ij")
    return jnp.asarray(hit(r, c), jnp.bfloat16)


def spread_hit(r, c):
    kind, t = r // 144, r % 144
    phonon = np.array([2, 3, 0, 1])[kind]
    component = np.where(kind % 2 == 0, t // BR, t % BR)
    return c == phonon * 16 + component


def order_hit(r, c):
    group, t = r // 32, r % 32
    lane = np.where(t < 12, t, np.where(t == 12, 24, np.where((t >= 16) & (t < 28), t - 4, -999)))
    return c == group * 32 + lane


def cosine_of(step):
    near = jnp.minimum(step, 16 - step)
    out = jnp.full(step.shape, -1.0, jnp.float32)
    for k in range(8):
        out = jnp.where(near == k, math.cos(math.pi * k / 8) if k != 4 else 0.0, out)
    return out


def floor_div(value, by):
    return jnp.floor((value.astype(jnp.float32) + 0.5) * (1.0 / by)).astype(jnp.int32)


def quartet_kernel(
    tab, blocks, tallies, phi, cells, eye, reorder, spread, out,
    table, wide, rows_v, rows_s, tally_s, live_s, near_a, near_b, sums, sem,
):
    pb, wa = lax.axis_index("pb"), lax.axis_index("wa")

    modes = jnp.maximum(blocks[...], 0)
    first = lax.broadcasted_iota(jnp.int32, modes.shape, 2) == 0
    modes = modes + jnp.where(first, pb * LOCAL, 0)
    unit = floor_div(modes, GROUP)
    rows_v[...] = (unit >> 2) * GROUP + modes - unit * GROUP
    copy_rows = pltpu.make_async_copy(rows_v, rows_s, sem.at[0])
    copy_tally = pltpu.make_async_copy(tallies, tally_s, sem.at[1])
    copy_rows.start()
    copy_tally.start()

    def turn(shard, carry):
        freq = tab[shard, :, FREQ_AT : FREQ_AT + LANES].astype(jnp.float32)
        for j in range(3):
            stack = []
            for g in range(4):
                stack.append(tab[shard, :, GROUP_AT[g] + 256 * j : GROUP_AT[g] + 256 * (j + 1)].astype(jnp.float32))
                at = 6 * g + 2 * j
                stack.append(
                    jnp.concatenate(
                        [jnp.broadcast_to(freq[at + h : at + h + 1, :], (8, LANES)) for h in range(2)], axis=1
                    )
                )
            stack = jnp.concatenate(stack, axis=0).astype(jnp.bfloat16)
            table[pl.ds(pl.multiple_of(shard * GROUP + 256 * j, 256), 256), :] = lax.dot_general(
                eye[...], stack, NT, preferred_element_type=jnp.float32
            )
        return carry

    lax.fori_loop(0, NB, turn, 0)
    copy_tally.wait()
    copy_rows.wait()

    def note(slot, total):
        source = slot >> 1
        held = ((wa - source) & (NB - 1)) + NB * (slot & 1)
        live_s[total] = slot
        return total + (held < tally_s[source, 0, 0]).astype(jnp.int32)

    live_s[0] = 0
    total = lax.fori_loop(0, 2 * NB, note, 0)
    for k in range(3):
        live_s[total + k] = 0

    sums[...] = jnp.zeros_like(sums)
    cell = cells[...].astype(jnp.float32)

    def gather(into, index):
        slot = live_s[index]
        for n in range(LANES):
            for k in range(4):
                into[k, n : n + 1, :] = table[pl.ds(rows_s[slot >> 1, slot & 1, k, n], 1), :]

    def work(held, index):
        slot = live_s[index]
        raw = blocks[slot >> 1, slot & 1]
        modes = jnp.maximum(raw, 0)
        fullmode = modes + jnp.where(lax.broadcasted_iota(jnp.int32, modes.shape, 0) == 0, pb * LOCAL, 0)
        group = floor_div(fullmode, GROUP) & 3
        halves, freqs = [], []
        for k in range(4):
            turned = lax.dot_general(reorder[...], held[k].astype(jnp.bfloat16), NT, preferred_element_type=jnp.float32)
            which = group[k : k + 1, :]
            mine = jnp.where(
                which < 2,
                jnp.where(which == 0, turned[0:32], turned[32:64]),
                jnp.where(which == 2, turned[64:96], turned[96:128]),
            )
            halves.append(jnp.concatenate([mine[0:16], mine[16:32]], axis=1))
            freqs.append(mine[12:13])
        vectors = jnp.concatenate(halves, axis=0).astype(jnp.bfloat16)
        pairs = jnp.dot(spread[...], vectors, preferred_element_type=jnp.float32)
        third, fourth, e1, e2 = (pairs[144 * k : 144 * (k + 1)] for k in range(4))
        far_re = third[:, :LANES] * fourth[:, :LANES] - third[:, LANES:] * fourth[:, LANES:]
        far_im = -(third[:, :LANES] * fourth[:, LANES:] + third[:, LANES:] * fourth[:, :LANES])

        point = floor_div(modes, BR)
        coords = [(point >> 8).astype(jnp.float32), ((point >> 4) & 15).astype(jnp.float32), (point & 15).astype(jnp.float32)]
        shift = jnp.zeros((8, LANES), jnp.float32)
        for which in range(3):
            for axis in range(3):
                column = cell[:, 3 * which + axis : 3 * which + axis + 1]
                term = column * coords[axis][which + 1 : which + 2, :]
                shift = shift + term if which == 0 else shift - term
        step = shift.astype(jnp.int32) & 15
        cosine, sine = cosine_of(step), cosine_of((step - 4) & 15)

        for k in range(8):
            c, s = cosine[k : k + 1, :], sine[k : k + 1, :]
            wide[144 * k : 144 * (k + 1), :LANES] = (c * far_re - s * far_im).astype(jnp.bfloat16)
            wide[144 * k : 144 * (k + 1), LANES:] = (c * far_im + s * far_re).astype(jnp.bfloat16)
        weighted = jnp.dot(phi[...], wide[...], preferred_element_type=jnp.float32)
        w_re, w_im = weighted[:, :LANES], weighted[:, LANES:]
        near_re = e1[:, :LANES] * e2[:, :LANES] - e1[:, LANES:] * e2[:, LANES:]
        near_im = e1[:, :LANES] * e2[:, LANES:] + e1[:, LANES:] * e2[:, :LANES]
        value_re = jnp.sum(near_re * w_re - near_im * w_im, axis=0, keepdims=True)
        value_im = jnp.sum(near_re * w_im + near_im * w_re, axis=0, keepdims=True)

        occupied = [1.0 / (jnp.exp(f) - 1.0) for f in freqs]
        mismatch = freqs[0] + freqs[1] - freqs[2] - freqs[3]
        delta = jnp.exp(-((mismatch / SMEARING) ** 2)) / (SMEARING * math.sqrt(math.pi))
        weight = (1.0 + occupied[1]) * occupied[2] * occupied[3] / occupied[0]
        product = freqs[0] * freqs[1] * freqs[2] * freqs[3]
        valid = (raw[1:2, :] >= 0) & (index < total)
        term = jnp.where(valid, (value_re * value_re + value_im * value_im) * delta * weight / product, 0.0)

        first = modes[0:1, :]
        high = floor_div(first, 192)
        low = first - 192 * high
        placed = jnp.where(lax.broadcasted_iota(jnp.int32, (NB, LANES), 0) == high, term, 0.0)
        one = placed.astype(jnp.bfloat16)
        rest = placed - one.astype(jnp.float32)
        two = rest.astype(jnp.bfloat16)
        three = (rest - two.astype(jnp.float32)).astype(jnp.bfloat16)
        spot = jnp.where(lax.broadcasted_iota(jnp.int32, (256, LANES), 0) == low, 1.0, 0.0).astype(jnp.bfloat16)
        sums[...] += lax.dot_general(
            jnp.concatenate([one, two, three], axis=0), spot, NT, preferred_element_type=jnp.float32
        )

    gather(near_a, 0)

    def two_blocks(it, carry):
        gather(near_b, 2 * it + 1)
        work(near_a, 2 * it)
        gather(near_a, 2 * it + 2)
        work(near_b, 2 * it + 1)
        return carry

    lax.fori_loop(0, (total + 1) // 2, two_blocks, 0)
    result = sums[0:16] + sums[16:32] + sums[32:48]
    for w in range(NB):
        out[w] = result[w : w + 1]


def quartet_sums(tab, blocks, tallies, phi, cells):
    vmem = pl.BlockSpec(memory_space=pltpu.VMEM)
    pinned = [pltpu.with_memory_space_constraint(a, pltpu.VMEM) for a in (tab, blocks, tallies)]
    return pl.pallas_call(
        quartet_kernel,
        out_shape=pltpu.VMEM((NB, 1, 256), jnp.float32),
        in_specs=[vmem] * 8,
        out_specs=vmem,
        scratch_shapes=[
            pltpu.VMEM((NB * GROUP, LANES), jnp.float32),
            pltpu.VMEM((1152, 256), jnp.bfloat16),
            pltpu.VMEM((NB, 2, 4, LANES), jnp.int32),
            pltpu.SMEM((NB, 2, 4, LANES), jnp.int32),
            pltpu.SMEM((NB, 1, LANES), jnp.int32),
            pltpu.SMEM((2 * NB + 4,), jnp.int32),
            pltpu.VMEM((4, LANES, LANES), jnp.float32),
            pltpu.VMEM((4, LANES, LANES), jnp.float32),
            pltpu.VMEM((48, 256), jnp.float32),
            pltpu.SemaphoreType.DMA((2,)),
        ],
        compiler_params=pltpu.CompilerParams(vmem_limit_bytes=32 << 20),
        name="quartets",
    )(
        *pinned, phi, cells,
        selection(256, 256, lambda r, c: r == c), selection(128, 128, order_hit), selection(576, 64, spread_hit),
    )


def reduce_kernel(part, out, arrived, send, recv):
    pb, wa = lax.axis_index("pb"), lax.axis_index("wa")
    barrier = pltpu.get_barrier_semaphore()
    peers = [lax.rem(wa + k, NB) for k in range(1, NB)]
    for peer in peers:
        pl.semaphore_signal(barrier, inc=1, device_id=(pb, peer), device_id_type=MESH)
    pl.semaphore_wait(barrier, NB - 1)
    sent = []
    for k, peer in enumerate(peers):
        copy = pltpu.make_async_remote_copy(
            src_ref=part.at[peer], dst_ref=arrived.at[wa], send_sem=send.at[k], recv_sem=recv.at[wa],
            device_id=(pb, peer), device_id_type=MESH,
        )
        copy.start()
        sent.append(copy)
    total = part[wa]
    for peer in peers:
        pltpu.make_async_remote_copy(
            src_ref=arrived.at[peer], dst_ref=arrived.at[peer], send_sem=send.at[0], recv_sem=recv.at[peer],
            device_id=(pb, peer), device_id_type=MESH,
        ).wait_recv()
        total = total + arrived[peer]
    out[...] = total
    for copy in sent:
        copy.wait_send()


def reduce_over_wa(part):
    vmem = pl.BlockSpec(memory_space=pltpu.VMEM)
    return pl.pallas_call(
        reduce_kernel,
        out_shape=jax.ShapeDtypeStruct((1, 256), jnp.float32),
        in_specs=[vmem],
        out_specs=vmem,
        scratch_shapes=[
            pltpu.VMEM((NB, 1, 256), jnp.float32),
            pltpu.SemaphoreType.DMA((NB,)),
            pltpu.SemaphoreType.DMA((NB,)),
        ],
        compiler_params=pltpu.CompilerParams(collective_id=1, has_side_effects=True, vmem_limit_bytes=1 << 20),
        name="reduce_wa",
    )(pltpu.with_memory_space_constraint(part, pltpu.VMEM))


def body(quartets, counts, eig, freq, phi, cells):
    dealt = quartets.reshape(2, NB, 4, LANES)
    tab, blocks, tallies = exchange(eig, freq.reshape(24, LANES), dealt, counts)
    part = quartet_sums(tab, blocks, tallies, phi, cells)
    return reduce_over_wa(part)[0, :192]


def solution(mesh):
    placed = (P(("pb", "wa"), None, None), P(("pb", "wa")), P(None, "pb"), P("pb"), P(), P())
    return jax.shard_map(body, mesh=mesh, in_specs=placed, out_specs=P(("pb", "wa")), check_vma=False)
```

```python
import functools
import math

import jax
import jax.numpy as jnp
import numpy as np
from jax import lax
from jax.experimental import pallas as pl
from jax.experimental.pallas import tpu as pltpu
from jax.sharding import PartitionSpec as P

QMESH = 16
BR = 12
NB = 16
LOCAL = 3072
GROUP = 768
LANES = 128
GROUP_AT = (0, 768, 1664, 2432)
FREQ_AT = 1536
WIDTH = 3200
SMEARING = 0.5
MESH = pl.DeviceIdType.MESH
NT = (((1,), (1,)), ((), ()))


def exchange_kernel(
    eig, freq, quartets, phi, cells, reorder, spread, eye, counts,
    table, blocks, tallies, rows, phi_v, cells_v, reorder_v, spread_v,
    tab, mine, eye_v, dealt, send, got, lent, got_q, got_c, local,
):
    pb, wa = lax.axis_index("pb"), lax.axis_index("wa")
    x, y, core = pb // 4, pb % 4, wa % 2
    ahead = 1 - 2 * core
    sibling = (pb, wa + ahead)

    def place(dx, dy):
        return lax.rem(x + dx + 4, 4) * 4 + lax.rem(y + dy + 4, 4)

    mine[...] = jnp.full((1, LANES), counts[0], jnp.int32)

    barrier = pltpu.get_barrier_semaphore()
    for step in (1, -1):
        pl.semaphore_signal(barrier, inc=1, device_id=(place(step, 0), wa), device_id_type=MESH)
        pl.semaphore_signal(barrier, inc=1, device_id=(place(0, step), wa), device_id_type=MESH)
    for k in range(1, NB):
        pl.semaphore_signal(barrier, inc=1, device_id=(pb, lax.rem(wa + k, NB)), device_id_type=MESH)

    own = [
        pltpu.make_async_copy(eig.at[:, pl.ds(0, 1536)], tab.at[pb, :, pl.ds(0, 1536)], local.at[0]),
        pltpu.make_async_copy(eig.at[:, pl.ds(1536, 1536)], tab.at[pb, :, pl.ds(1664, 1536)], local.at[1]),
        pltpu.make_async_copy(freq, tab.at[pb, :, pl.ds(FREQ_AT, LANES)], local.at[2]),
        pltpu.make_async_copy(quartets, dealt, local.at[3]),
        pltpu.make_async_copy(eye, eye_v, local.at[4]),
    ]
    later = [
        pltpu.make_async_copy(phi, phi_v, local.at[5]),
        pltpu.make_async_copy(cells, cells_v, local.at[6]),
        pltpu.make_async_copy(reorder, reorder_v, local.at[7]),
        pltpu.make_async_copy(spread, spread_v, local.at[8]),
    ]
    for copy in own + later:
        copy.start()
    for copy in own:
        copy.wait()
    tallies[wa] = mine[...]
    blocks[wa] = dealt[:, 0]

    pl.semaphore_wait(barrier, 4 + NB - 1)

    sent = []

    def push(src, dst, sem, device):
        copy = pltpu.make_async_remote_copy(
            src_ref=src, dst_ref=dst, send_sem=send.at[len(sent)], recv_sem=sem, device_id=device, device_id_type=MESH
        )
        copy.start()
        sent.append(copy)

    def piece(part, shard):
        if part == 0:
            return tab.at[shard, :, pl.ds(pl.multiple_of(core * 2432, LANES), 768)]
        return tab.at[shard, :, pl.ds(pl.multiple_of(768 + core * 768, LANES), 896)]

    def half(part, shard):
        if part == 0:
            return piece(part, shard)
        return tab.at[shard, :, pl.ds(pl.multiple_of(768 + core * 896, LANES), 768)]

    def half_of_sibling(part, shard):
        if part == 0:
            return tab.at[shard, :, pl.ds(pl.multiple_of((1 - core) * 2432, LANES), 768)]
        return tab.at[shard, :, pl.ds(pl.multiple_of(768 + (1 - core) * 896, LANES), 768)]

    def at(part, first, second):
        return place(first, second) if part == 0 else place(second, first)

    def relay(part, shard, first, second):
        view = piece(part, shard)
        push(view, view, got.at[part, shard], (at(part, first, second), wa))

    def lend(part, shard):
        view = half(part, shard)
        push(view, view, lent.at[part, shard], sibling)

    def arrived(part, shard):
        view = piece(part, shard)
        pltpu.make_async_remote_copy(
            src_ref=view, dst_ref=view, send_sem=send.at[0], recv_sem=got.at[part, shard], device_id=sibling, device_id_type=MESH
        ).wait_recv()

    def second_both(part, shard):
        relay(part, shard, 0, ahead)
        relay(part, shard, 0, -ahead)

    for part in (0, 1):
        relay(part, pb, ahead, 0)
        relay(part, pb, -ahead, 0)
    for part in (0, 1):
        second_both(part, pb)
    for k in range(1, NB):
        peer = lax.rem(wa + k, NB)
        push(dealt.at[:, k], blocks.at[wa], got_q.at[wa], (pb, peer))
        push(mine, tallies.at[wa], got_c.at[wa], (pb, peer))

    def first_axis(part, step):
        shard = at(part, step, 0)
        arrived(part, shard)
        if step is back:
            relay(part, shard, ahead, 0)
        second_both(part, shard)
        lend(part, shard)

    def second_axis(part, row, step):
        shard = at(part, row, step)
        arrived(part, shard)
        if step is back:
            relay(part, shard, 0, ahead)
        lend(part, shard)

    back, fore = -ahead, ahead
    order = [
        (first_axis, (back,)),
        (first_axis, (fore,)),
        (second_axis, (0, back)),
        (second_axis, (0, fore)),
        (first_axis, (2,)),
        (second_axis, (back, back)),
        (second_axis, (back, fore)),
        (second_axis, (0, 2)),
        (second_axis, (fore, back)),
        (second_axis, (fore, fore)),
        (second_axis, (back, 2)),
        (second_axis, (2, back)),
        (second_axis, (2, fore)),
        (second_axis, (fore, 2)),
        (second_axis, (2, 2)),
    ]

    def turn(shard):
        values = tab[shard, :, FREQ_AT : FREQ_AT + LANES].astype(jnp.float32)
        for j in range(3):
            stack = []
            for g in range(4):
                stack.append(tab[shard, :, GROUP_AT[g] + 256 * j : GROUP_AT[g] + 256 * (j + 1)].astype(jnp.float32))
                at = 6 * g + 2 * j
                stack.append(
                    jnp.concatenate(
                        [jnp.broadcast_to(values[at + h : at + h + 1, :], (8, LANES)) for h in range(2)], axis=1
                    )
                )
            stack = jnp.concatenate(stack, axis=0).astype(jnp.bfloat16)
            table[pl.ds(pl.multiple_of(shard * GROUP + 256 * j, 256), 256), :] = lax.dot_general(
                eye_v[...], stack, NT, preferred_element_type=jnp.float32
            )

    def borrowed(shard):
        for part in (0, 1):
            view = half_of_sibling(part, shard)
            pltpu.make_async_remote_copy(
                src_ref=view, dst_ref=view, send_sem=send.at[0], recv_sem=lent.at[part, shard], device_id=sibling, device_id_type=MESH
            ).wait_recv()

    turns = {
        5: ((back, 0), (fore, 0), (0, back), (0, fore)),
        9: ((2, 0), (0, 2)),
        10: ((back, fore), (fore, back)),
        12: ((back, back), (fore, fore)),
        14: ((back, 2), (2, back), (2, fore), (fore, 2), (2, 2)),
    }
    turn(pb)
    def blocks_in():
        for k in range(1, NB):
            peer = lax.rem(wa + k, NB)
            for dst, sem in ((blocks.at[peer], got_q.at[peer]), (tallies.at[peer], got_c.at[peer])):
                pltpu.make_async_remote_copy(
                    src_ref=dst, dst_ref=dst, send_sem=send.at[0], recv_sem=sem, device_id=sibling, device_id_type=MESH
                ).wait_recv()
        modes = jnp.maximum(blocks[...], 0)
        first = lax.broadcasted_iota(jnp.int32, modes.shape, 2) == 0
        rows[...] = rows_of(modes + jnp.where(first, pb * LOCAL, 0))
        for copy in later:
            copy.wait()

    for number, (what, where) in enumerate(order):
        for part in (0, 1):
            what(part, *where)
        if number == 7:
            blocks_in()
        for offset in turns.get(number, ()):
            shard = place(*offset)
            borrowed(shard)
            turn(shard)

    for copy in sent:
        copy.wait_send()


def exchange(eig, freq, quartets, phi, cells, counts):
    hbm = pl.BlockSpec(memory_space=pltpu.HBM)
    vmem = pl.BlockSpec(memory_space=pltpu.VMEM)
    return pl.pallas_call(
        exchange_kernel,
        out_shape=(
            pltpu.VMEM((NB * GROUP, LANES), jnp.float32),
            pltpu.VMEM((NB, 2, 4, LANES), jnp.int32),
            pltpu.VMEM((NB, 1, LANES), jnp.int32),
            pltpu.VMEM((NB, 2, 4, LANES), jnp.int32),
            pltpu.VMEM((144, 1152), jnp.bfloat16),
            pltpu.VMEM((8, 9), jnp.int32),
            pltpu.VMEM((128, 128), jnp.bfloat16),
            pltpu.VMEM((576, 64), jnp.bfloat16),
        ),
        in_specs=[hbm] * 8 + [pl.BlockSpec(memory_space=pltpu.SMEM)],
        out_specs=(vmem,) * 8,
        scratch_shapes=[
            pltpu.VMEM((NB, 24, WIDTH), jnp.bfloat16),
            pltpu.VMEM((1, LANES), jnp.int32),
            pltpu.VMEM((256, 256), jnp.bfloat16),
            pltpu.VMEM((2, NB, 4, LANES), jnp.int32),
            pltpu.SemaphoreType.DMA((120,)),
            pltpu.SemaphoreType.DMA((2, NB)),
            pltpu.SemaphoreType.DMA((2, NB)),
            pltpu.SemaphoreType.DMA((NB,)),
            pltpu.SemaphoreType.DMA((NB,)),
            pltpu.SemaphoreType.DMA((9,)),
        ],
        compiler_params=pltpu.CompilerParams(collective_id=0, has_side_effects=True, vmem_limit_bytes=24 << 20),
        name="exchange",
    )(
        *[
            pltpu.with_memory_space_constraint(a, pltpu.HBM)
            for a in (
                eig, freq, quartets, phi, cells, selection(128, 128, order_hit), selection(576, 64, spread_hit),
                selection(256, 256, lambda r, c: r == c),
            )
        ],
        counts,
    )


def selection(rows, columns, hit):
    r, c = np.meshgrid(np.arange(rows), np.arange(columns), indexing="ij")
    return jnp.asarray(hit(r, c), jnp.bfloat16)


def spread_hit(r, c):
    kind, t = r // 144, r % 144
    phonon = np.array([2, 3, 0, 1])[kind]
    component = np.where(kind % 2 == 0, t // BR, t % BR)
    return c == phonon * 16 + component


def order_hit(r, c):
    group, t = r // 32, r % 32
    lane = np.where(t < 12, t, np.where(t == 12, 24, np.where((t >= 16) & (t < 28), t - 4, -999)))
    return c == group * 32 + lane


def cosine_of(step):
    near = jnp.minimum(step, 16 - step)
    out = jnp.full(step.shape, -1.0, jnp.float32)
    for k in range(8):
        out = jnp.where(near == k, math.cos(math.pi * k / 8) if k != 4 else 0.0, out)
    return out


def floor_div(value, by):
    return jnp.floor((value.astype(jnp.float32) + 0.5) * (1.0 / by)).astype(jnp.int32)


def rows_of(modes):
    unit = floor_div(modes, GROUP)
    return (unit >> 2) * GROUP + modes - unit * GROUP


def quartet_kernel(
    table, blocks, tallies, rows, phi, cells, reorder, spread, out,
    wide_a, wide_b, near_a, near_b, scale_a, scale_b, held_a, held_b, rows_a, rows_b, tally_s, live_s, sums, sem,
):
    pb, wa = lax.axis_index("pb"), lax.axis_index("wa")
    copy_tally = pltpu.make_async_copy(tallies, tally_s, sem.at[2])
    copy_tally.start()
    sums[...] = jnp.zeros_like(sums)
    cell = cells[...].astype(jnp.float32)
    copy_tally.wait()

    live_s[0] = 0
    total = jnp.int32(0)
    for source in range(NB):
        held = (wa - source) & (NB - 1)
        tally = tally_s[source, 0, 0]
        for high in range(2):
            live_s[total] = 2 * source + high
            total = total + (held + NB * high < tally).astype(jnp.int32)
    for k in range(6):
        live_s[total + k] = 0

    def fetch(index, into, which):
        slot = live_s[index]
        return pltpu.make_async_copy(rows.at[slot >> 1, slot & 1], into, sem.at[which])

    def gather(into, at):
        for n in range(LANES):
            for k in range(4):
                into[LANES * k + n : LANES * k + n + 1, :] = table[pl.ds(at[k, n], 1), :]

    def products(held, index, wide, near, scale):
        slot = live_s[index]
        raw = blocks[slot >> 1, slot & 1]
        modes = jnp.maximum(raw, 0)
        fullmode = modes + jnp.where(lax.broadcasted_iota(jnp.int32, modes.shape, 0) == 0, pb * LOCAL, 0)
        group = floor_div(fullmode, GROUP) & 3
        turned = lax.dot_general(reorder[...], held[...].astype(jnp.bfloat16), NT, preferred_element_type=jnp.float32)
        halves, freqs = [], []
        for k in range(4):
            which = group[k : k + 1, :]
            part = turned[:, LANES * k : LANES * (k + 1)]
            mine = jnp.where(
                which < 2,
                jnp.where(which == 0, part[0:32], part[32:64]),
                jnp.where(which == 2, part[64:96], part[96:128]),
            )
            halves.append(jnp.concatenate([mine[0:16], mine[16:32]], axis=1))
            freqs.append(mine[12:13])
        vectors = jnp.concatenate(halves, axis=0).astype(jnp.bfloat16)
        pairs = jnp.dot(spread[...], vectors, preferred_element_type=jnp.float32)
        third, fourth, e1, e2 = (pairs[144 * k : 144 * (k + 1)] for k in range(4))
        far_re = third[:, :LANES] * fourth[:, :LANES] - third[:, LANES:] * fourth[:, LANES:]
        far_im = -(third[:, :LANES] * fourth[:, LANES:] + third[:, LANES:] * fourth[:, :LANES])
        near[0:144] = e1[:, :LANES] * e2[:, :LANES] - e1[:, LANES:] * e2[:, LANES:]
        near[144:288] = e1[:, :LANES] * e2[:, LANES:] + e1[:, LANES:] * e2[:, :LANES]

        point = floor_div(modes, BR)
        coords = [(point >> 8).astype(jnp.float32), ((point >> 4) & 15).astype(jnp.float32), (point & 15).astype(jnp.float32)]
        shift = jnp.zeros((8, LANES), jnp.float32)
        for which in range(3):
            for axis in range(3):
                column = cell[:, 3 * which + axis : 3 * which + axis + 1]
                term = column * coords[axis][which + 1 : which + 2, :]
                shift = shift + term if which == 0 else shift - term
        step = shift.astype(jnp.int32) & 15
        cosine, sine = cosine_of(step), cosine_of((step - 4) & 15)
        for k in range(8):
            c, s = cosine[k : k + 1, :], sine[k : k + 1, :]
            wide[144 * k : 144 * (k + 1), :LANES] = (c * far_re - s * far_im).astype(jnp.bfloat16)
            wide[144 * k : 144 * (k + 1), LANES:] = (c * far_im + s * far_re).astype(jnp.bfloat16)

        occupied = [1.0 / (jnp.exp(f) - 1.0) for f in freqs]
        mismatch = freqs[0] + freqs[1] - freqs[2] - freqs[3]
        delta = jnp.exp(-((mismatch / SMEARING) ** 2)) / (SMEARING * math.sqrt(math.pi))
        weight = (1.0 + occupied[1]) * occupied[2] * occupied[3] / occupied[0]
        product = freqs[0] * freqs[1] * freqs[2] * freqs[3]
        valid = (raw[1:2, :] >= 0) & (index < total)
        scale[...] = jnp.where(valid, delta * weight / product, 0.0)

    def contract(index, wide, near, scale):
        slot = live_s[index]
        weighted = jnp.dot(phi[...], wide[...], preferred_element_type=jnp.float32)
        w_re, w_im = weighted[:, :LANES], weighted[:, LANES:]
        near_re, near_im = near[0:144], near[144:288]
        value_re = jnp.sum(near_re * w_re - near_im * w_im, axis=0, keepdims=True)
        value_im = jnp.sum(near_re * w_im + near_im * w_re, axis=0, keepdims=True)
        term = (value_re * value_re + value_im * value_im) * scale[...]

        first = jnp.maximum(blocks[slot >> 1, slot & 1][0:1, :], 0)
        high = floor_div(first, 192)
        low = first - 192 * high
        placed = jnp.where(lax.broadcasted_iota(jnp.int32, (NB, LANES), 0) == high, term, 0.0)
        one = placed.astype(jnp.bfloat16)
        rest = placed - one.astype(jnp.float32)
        two = rest.astype(jnp.bfloat16)
        three = (rest - two.astype(jnp.float32)).astype(jnp.bfloat16)
        spot = jnp.where(lax.broadcasted_iota(jnp.int32, (256, LANES), 0) == low, 1.0, 0.0).astype(jnp.bfloat16)
        sums[...] += lax.dot_general(
            jnp.concatenate([one, two, three], axis=0), spot, NT, preferred_element_type=jnp.float32
        )

    fetch(0, rows_a, 0).start()
    fetch(1, rows_b, 1).start()
    fetch(0, rows_a, 0).wait()
    gather(held_a, rows_a)
    fetch(2, rows_a, 0).start()
    fetch(1, rows_b, 1).wait()
    gather(held_b, rows_b)
    products(held_a, 0, wide_a, near_a, scale_a)
    fetch(3, rows_b, 1).start()

    def two_blocks(it, carry):
        i = 2 * it
        fetch(i + 2, rows_a, 0).wait()
        gather(held_a, rows_a)
        products(held_b, i + 1, wide_b, near_b, scale_b)
        contract(i, wide_a, near_a, scale_a)
        fetch(i + 4, rows_a, 0).start()
        fetch(i + 3, rows_b, 1).wait()
        gather(held_b, rows_b)
        products(held_a, i + 2, wide_a, near_a, scale_a)
        contract(i + 1, wide_b, near_b, scale_b)
        fetch(i + 5, rows_b, 1).start()
        return carry

    trips = (total + 1) // 2
    lax.fori_loop(0, trips, two_blocks, 0)
    fetch(2 * trips + 2, rows_a, 0).wait()
    fetch(2 * trips + 3, rows_b, 1).wait()
    result = sums[0:16] + sums[16:32] + sums[32:48]
    for w in range(NB):
        out[w] = result[w : w + 1]


def quartet_sums(*operands):
    vmem = pl.BlockSpec(memory_space=pltpu.VMEM)
    pinned = [pltpu.with_memory_space_constraint(a, pltpu.VMEM) for a in operands]
    return pl.pallas_call(
        quartet_kernel,
        out_shape=pltpu.VMEM((NB, 1, 256), jnp.float32),
        in_specs=[vmem] * 8,
        out_specs=vmem,
        scratch_shapes=[
            pltpu.VMEM((1152, 256), jnp.bfloat16),
            pltpu.VMEM((1152, 256), jnp.bfloat16),
            pltpu.VMEM((288, LANES), jnp.float32),
            pltpu.VMEM((288, LANES), jnp.float32),
            pltpu.VMEM((1, LANES), jnp.float32),
            pltpu.VMEM((1, LANES), jnp.float32),
            pltpu.VMEM((4 * LANES, LANES), jnp.float32),
            pltpu.VMEM((4 * LANES, LANES), jnp.float32),
            pltpu.SMEM((4, LANES), jnp.int32),
            pltpu.SMEM((4, LANES), jnp.int32),
            pltpu.SMEM((NB, 1, LANES), jnp.int32),
            pltpu.SMEM((2 * NB + 8,), jnp.int32),
            pltpu.VMEM((48, 256), jnp.float32),
            pltpu.SemaphoreType.DMA((3,)),
        ],
        compiler_params=pltpu.CompilerParams(vmem_limit_bytes=16 << 20),
        name="quartets",
    )(*pinned)


def reduce_kernel(part, out, arrived, send, recv):
    pb, wa = lax.axis_index("pb"), lax.axis_index("wa")
    barrier = pltpu.get_barrier_semaphore()
    peers = [lax.rem(wa + k, NB) for k in range(1, NB)]
    for peer in peers:
        pl.semaphore_signal(barrier, inc=1, device_id=(pb, peer), device_id_type=MESH)
    pl.semaphore_wait(barrier, NB - 1)
    sent = []
    for k, peer in enumerate(peers):
        copy = pltpu.make_async_remote_copy(
            src_ref=part.at[peer], dst_ref=arrived.at[wa], send_sem=send.at[k], recv_sem=recv.at[wa],
            device_id=(pb, peer), device_id_type=MESH,
        )
        copy.start()
        sent.append(copy)
    total = part[wa]
    for peer in peers:
        pltpu.make_async_remote_copy(
            src_ref=arrived.at[peer], dst_ref=arrived.at[peer], send_sem=send.at[0], recv_sem=recv.at[peer],
            device_id=(pb, peer), device_id_type=MESH,
        ).wait_recv()
        total = total + arrived[peer]
    out[...] = total
    for copy in sent:
        copy.wait_send()


def reduce_over_wa(part):
    vmem = pl.BlockSpec(memory_space=pltpu.VMEM)
    return pl.pallas_call(
        reduce_kernel,
        out_shape=jax.ShapeDtypeStruct((1, 256), jnp.float32),
        in_specs=[vmem],
        out_specs=vmem,
        scratch_shapes=[
            pltpu.VMEM((NB, 1, 256), jnp.float32),
            pltpu.SemaphoreType.DMA((NB,)),
            pltpu.SemaphoreType.DMA((NB,)),
        ],
        compiler_params=pltpu.CompilerParams(collective_id=1, has_side_effects=True, vmem_limit_bytes=1 << 20),
        name="reduce_wa",
    )(pltpu.with_memory_space_constraint(part, pltpu.VMEM))


def body(quartets, counts, eig, freq, phi, cells):
    dealt = quartets.reshape(2, NB, 4, LANES)
    held = exchange(eig, freq.reshape(24, LANES), dealt, phi, cells, counts)
    part = quartet_sums(*held)
    return reduce_over_wa(part)[0, :192]


def solution(mesh):
    placed = (P(("pb", "wa"), None, None), P(("pb", "wa")), P(None, "pb"), P("pb"), P(), P())
    return jax.shard_map(body, mesh=mesh, in_specs=placed, out_specs=P(("pb", "wa")), check_vma=False)
```

```python
import functools
import math

import jax
import jax.numpy as jnp
from jax import lax
from jax.experimental import pallas as pl
from jax.experimental.pallas import tpu as pltpu
from jax.sharding import PartitionSpec as P

QMESH = 16
BR = 12
NB = 16
LOCAL = 3072
GROUP = 768
LANES = 128
GROUP_AT = (0, 768, 1664, 2432)
FREQ_AT = 1536
WIDTH = 3200
SMEARING = 0.5
MESH = pl.DeviceIdType.MESH
NT = (((1,), (1,)), ((), ()))


ORDER = (
    (-1, 0), (1, 0), (0, -1), (0, 1), (2, 0), (-1, -1), (-1, 1), (0, 2), (1, -1), (1, 1), (-1, 2), (2, -1), (2, 1), (1, 2), (2, 2),
)
WAVES = (
    ((-1, 0), (1, 0), (0, -1), (0, 1)),
    ((2, 0), (0, 2)),
    ((-1, 1), (1, -1)),
    ((-1, -1), (1, 1)),
    ((-1, 2), (2, -1), (2, 1), (1, 2)),
    ((2, 2),),
)
WAVE_AFTER = {5: (0,), 9: (1,), 10: (2,), 12: (3,), 14: (4, 5)}


def wrapped(offset):
    return (offset + 1) % 4 - 1


def hit(rows, columns, where):
    r = lax.broadcasted_iota(jnp.int32, (rows, columns), 0)
    c = lax.broadcasted_iota(jnp.int32, (rows, columns), 1)
    return jnp.where(where(r) == c, 1.0, 0.0).astype(jnp.bfloat16)


def spread_column(r):
    kind = floor_div(r, 144)
    t = r - 144 * kind
    first = floor_div(t, BR)
    return ((kind + 2) & 3) * 16 + jnp.where((kind & 1) == 0, first, t - BR * first)


def order_column(r):
    t = r & 31
    lane = jnp.where(t < 12, t, jnp.where(t == 12, 24, jnp.where((t >= 16) & (t < 28), t - 4, -999)))
    return lane + (r - t)


def exchange_kernel(
    eig, freq, quartets, phi, cells, counts,
    table, blocks, tallies, rows, phi_v, cells_v, reorder, spread,
    tab, mine, eye, dealt, send, got, lent, local,
):
    pb, wa = lax.axis_index("pb"), lax.axis_index("wa")
    x, y, core = pb // 4, pb % 4, wa % 2
    ahead = 1 - 2 * core
    sibling = (pb, wa + ahead)

    def place(dx, dy):
        return lax.rem(x + ahead * dx + 4, 4) * 4 + lax.rem(y + ahead * dy + 4, 4)

    barrier = pltpu.get_barrier_semaphore()
    for step in (1, -1):
        pl.semaphore_signal(barrier, inc=1, device_id=(place(step, 0), wa), device_id_type=MESH)
        pl.semaphore_signal(barrier, inc=1, device_id=(place(0, step), wa), device_id_type=MESH)
    for k in range(1, NB):
        pl.semaphore_signal(barrier, inc=1, device_id=(pb, lax.rem(wa + k, NB)), device_id_type=MESH)

    left = pltpu.make_async_copy(eig.at[:, pl.ds(0, 1536)], tab.at[pb, :, pl.ds(0, 1536)], local.at[0])
    right = pltpu.make_async_copy(eig.at[:, pl.ds(1536, 1536)], tab.at[pb, :, pl.ds(1664, 1536)], local.at[1])
    copy_freq = pltpu.make_async_copy(freq, tab.at[pb, :, pl.ds(FREQ_AT, LANES)], local.at[2])
    copy_dealt = pltpu.make_async_copy(quartets, dealt, local.at[3])
    copy_phi = pltpu.make_async_copy(phi, phi_v, local.at[4])
    copy_cells = pltpu.make_async_copy(cells, cells_v, local.at[5])
    own = (left, right, copy_freq, copy_dealt)
    for copy in own + (copy_phi, copy_cells):
        copy.start()
    mine[...] = jnp.full((1, LANES), counts[0], jnp.int32)
    tallies[wa] = mine[...]
    eye[...] = hit(256, 256, lambda r: r)
    reorder[...] = hit(LANES, LANES, order_column)
    spread[...] = hit(576, 64, spread_column)
    for copy in own:
        copy.wait()
    blocks[wa] = dealt[:, 0]

    pl.semaphore_wait(barrier, 4 + NB - 1)

    def push(src, dst, sent, arrival, device):
        pltpu.make_async_remote_copy(
            src_ref=src, dst_ref=dst, send_sem=send.at[sent], recv_sem=arrival, device_id=device, device_id_type=MESH
        ).start()

    def bytes_in(view, sem):
        pltpu.make_async_remote_copy(
            src_ref=view, dst_ref=view, send_sem=send.at[0], recv_sem=sem, device_id=sibling, device_id_type=MESH
        ).wait_recv()

    def bytes_out(view, sent):
        pltpu.make_async_remote_copy(
            src_ref=view, dst_ref=view, send_sem=send.at[sent], recv_sem=got.at[0], device_id=sibling, device_id_type=MESH
        ).wait_send()

    def at(part, first, second):
        return place(first, second) if part == 0 else place(second, first)

    def relay(part, first, second, axis, step):
        shard = at(part, first, second)
        if part == 0:
            view = tab.at[shard, :, pl.ds(pl.multiple_of(core * 2432, LANES), 768)]
        else:
            view = tab.at[shard, :, pl.ds(pl.multiple_of(768 + core * 768, LANES), 896)]
        key = (wrapped(first - step), second) if axis == 0 else (first, wrapped(second - step))
        target = at(part, step, 0) if axis == 0 else at(part, 0, step)
        push(view, view, part, got.at[ORDER.index(key)], (target, wa))

    def lend(part, first, second):
        shard = at(part, first, second)
        if part == 0:
            view = tab.at[shard, :, pl.ds(pl.multiple_of(core * 2432, LANES), 768)]
        else:
            view = tab.at[shard, :, pl.ds(pl.multiple_of(768 + core * 896, LANES), 768)]
        offset = (first, second) if part == 0 else (second, first)
        wave = [w for w, members in enumerate(WAVES) if offset in members][0]
        push(view, view, 2, lent.at[wave], sibling)

    def turn(shard):
        values = tab[shard, :, FREQ_AT : FREQ_AT + LANES].astype(jnp.float32)
        for j in range(3):
            stack = []
            for g in range(4):
                stack.append(tab[shard, :, GROUP_AT[g] + 256 * j : GROUP_AT[g] + 256 * (j + 1)].astype(jnp.float32))
                at_row = 6 * g + 2 * j
                stack.append(
                    jnp.concatenate(
                        [jnp.broadcast_to(values[at_row + h : at_row + h + 1, :], (8, LANES)) for h in range(2)], axis=1
                    )
                )
            stack = jnp.concatenate(stack, axis=0).astype(jnp.bfloat16)
            table[pl.ds(pl.multiple_of(shard * GROUP + 256 * j, 256), 256), :] = lax.dot_general(
                eye[...], stack, NT, preferred_element_type=jnp.float32
            )

    for axis in (0, 1):
        for part in (0, 1):
            relay(part, 0, 0, axis, 1)
            relay(part, 0, 0, axis, -1)
    for k in range(1, NB):
        peer = lax.rem(wa + k, NB)
        push(dealt.at[:, k], blocks.at[wa], 3, lent.at[len(WAVES)], (pb, peer))
        push(mine, tallies.at[wa], 4, lent.at[len(WAVES) + 1], (pb, peer))
    turn(pb)

    for number, (first, second) in enumerate(ORDER):
        bytes_in(tab.at[0, :, pl.ds(0, 1664)], got.at[number])
        for part in (0, 1):
            if second == 0:
                if first == -1:
                    relay(part, first, 0, 0, 1)
                relay(part, first, 0, 1, 1)
                relay(part, first, 0, 1, -1)
            elif second == -1:
                relay(part, first, second, 1, 1)
            lend(part, first, second)
        if number == 7:
            bytes_in(blocks.at[pl.ds(0, NB - 1)], lent.at[len(WAVES)])
            bytes_in(tallies.at[pl.ds(0, NB - 1)], lent.at[len(WAVES) + 1])
            modes = jnp.maximum(blocks[...], 0)
            local_mode = lax.broadcasted_iota(jnp.int32, modes.shape, 2) == 0
            rows[...] = rows_of(modes + jnp.where(local_mode, pb * LOCAL, 0))
        for wave in WAVE_AFTER.get(number, ()):
            members = WAVES[wave]
            bytes_in(tab.at[pl.ds(0, len(members)), :, pl.ds(0, 1536)], lent.at[wave])
            for offset in members:
                turn(place(*offset))

    copy_phi.wait()
    copy_cells.wait()
    bytes_out(tab.at[pl.ds(0, 15), :, pl.ds(0, 768)], 0)
    bytes_out(tab.at[pl.ds(0, 15), :, pl.ds(0, 896)], 1)
    bytes_out(tab.at[pl.ds(0, 15), :, pl.ds(0, 1536)], 2)
    bytes_out(blocks.at[pl.ds(0, NB - 1)], 3)
    bytes_out(tallies.at[pl.ds(0, NB - 1)], 4)


def exchange(eig, freq, quartets, phi, cells, counts):
    hbm = pl.BlockSpec(memory_space=pltpu.HBM)
    vmem = pl.BlockSpec(memory_space=pltpu.VMEM)
    return pl.pallas_call(
        exchange_kernel,
        out_shape=(
            pltpu.VMEM((NB * GROUP, LANES), jnp.float32),
            pltpu.VMEM((NB, 2, 4, LANES), jnp.int32),
            pltpu.VMEM((NB, 1, LANES), jnp.int32),
            pltpu.VMEM((NB, 2, 4, LANES), jnp.int32),
            pltpu.VMEM((144, 1152), jnp.bfloat16),
            pltpu.VMEM((8, 9), jnp.int32),
            pltpu.VMEM((128, 128), jnp.bfloat16),
            pltpu.VMEM((576, 64), jnp.bfloat16),
        ),
        in_specs=[hbm] * 5 + [pl.BlockSpec(memory_space=pltpu.SMEM)],
        out_specs=(vmem,) * 8,
        scratch_shapes=[
            pltpu.VMEM((NB, 24, WIDTH), jnp.bfloat16),
            pltpu.VMEM((1, LANES), jnp.int32),
            pltpu.VMEM((256, 256), jnp.bfloat16),
            pltpu.VMEM((2, NB, 4, LANES), jnp.int32),
            pltpu.SemaphoreType.DMA((5,)),
            pltpu.SemaphoreType.DMA((len(ORDER),)),
            pltpu.SemaphoreType.DMA((len(WAVES) + 2,)),
            pltpu.SemaphoreType.DMA((6,)),
        ],
        compiler_params=pltpu.CompilerParams(collective_id=0, has_side_effects=True, vmem_limit_bytes=24 << 20),
        name="exchange",
    )(*[pltpu.with_memory_space_constraint(a, pltpu.HBM) for a in (eig, freq, quartets, phi, cells)], counts)


def cosine_of(step):
    near = jnp.minimum(step, 16 - step)
    out = jnp.full(step.shape, -1.0, jnp.float32)
    for k in range(8):
        out = jnp.where(near == k, math.cos(math.pi * k / 8) if k != 4 else 0.0, out)
    return out


def floor_div(value, by):
    return jnp.floor((value.astype(jnp.float32) + 0.5) * (1.0 / by)).astype(jnp.int32)


def rows_of(modes):
    unit = floor_div(modes, GROUP)
    return (unit >> 2) * GROUP + modes - unit * GROUP


def quartet_kernel(
    table, blocks, tallies, rows, phi, cells, reorder, spread, out,
    wide_a, wide_b, near_a, near_b, scale_a, scale_b, held_a, held_b, rows_a, rows_b, tally_s, live_s, sums, sem,
):
    pb, wa = lax.axis_index("pb"), lax.axis_index("wa")
    copy_tally = pltpu.make_async_copy(tallies, tally_s, sem.at[2])
    copy_tally.start()
    sums[...] = jnp.zeros_like(sums)
    cell = cells[...].astype(jnp.float32)
    copy_tally.wait()

    live_s[0] = 0
    total = jnp.int32(0)
    for source in range(NB):
        held = (wa - source) & (NB - 1)
        tally = tally_s[source, 0, 0]
        for high in range(2):
            live_s[total] = 2 * source + high
            total = total + (held + NB * high < tally).astype(jnp.int32)
    for k in range(6):
        live_s[total + k] = 0

    def fetch(index, into, which):
        slot = live_s[index]
        return pltpu.make_async_copy(rows.at[slot >> 1, slot & 1], into, sem.at[which])

    def gather(into, at):
        for n in range(LANES):
            for k in range(4):
                into[LANES * k + n : LANES * k + n + 1, :] = table[pl.ds(at[k, n], 1), :]

    def products(held, index, wide, near, scale):
        slot = live_s[index]
        raw = blocks[slot >> 1, slot & 1]
        modes = jnp.maximum(raw, 0)
        fullmode = modes + jnp.where(lax.broadcasted_iota(jnp.int32, modes.shape, 0) == 0, pb * LOCAL, 0)
        group = floor_div(fullmode, GROUP) & 3
        turned = lax.dot_general(reorder[...], held[...].astype(jnp.bfloat16), NT, preferred_element_type=jnp.float32)
        halves, freqs = [], []
        for k in range(4):
            which = group[k : k + 1, :]
            part = turned[:, LANES * k : LANES * (k + 1)]
            mine = jnp.where(
                which < 2,
                jnp.where(which == 0, part[0:32], part[32:64]),
                jnp.where(which == 2, part[64:96], part[96:128]),
            )
            halves.append(jnp.concatenate([mine[0:16], mine[16:32]], axis=1))
            freqs.append(mine[12:13])
        vectors = jnp.concatenate(halves, axis=0).astype(jnp.bfloat16)
        pairs = jnp.dot(spread[...], vectors, preferred_element_type=jnp.float32)
        third, fourth, e1, e2 = (pairs[144 * k : 144 * (k + 1)] for k in range(4))
        far_re = third[:, :LANES] * fourth[:, :LANES] - third[:, LANES:] * fourth[:, LANES:]
        far_im = -(third[:, :LANES] * fourth[:, LANES:] + third[:, LANES:] * fourth[:, :LANES])
        near[0:144] = e1[:, :LANES] * e2[:, :LANES] - e1[:, LANES:] * e2[:, LANES:]
        near[144:288] = e1[:, :LANES] * e2[:, LANES:] + e1[:, LANES:] * e2[:, :LANES]

        point = floor_div(modes, BR)
        coords = [(point >> 8).astype(jnp.float32), ((point >> 4) & 15).astype(jnp.float32), (point & 15).astype(jnp.float32)]
        shift = jnp.zeros((8, LANES), jnp.float32)
        for which in range(3):
            for axis in range(3):
                column = cell[:, 3 * which + axis : 3 * which + axis + 1]
                term = column * coords[axis][which + 1 : which + 2, :]
                shift = shift + term if which == 0 else shift - term
        step = shift.astype(jnp.int32) & 15
        cosine, sine = cosine_of(step), cosine_of((step - 4) & 15)
        for k in range(8):
            c, s = cosine[k : k + 1, :], sine[k : k + 1, :]
            wide[144 * k : 144 * (k + 1), :LANES] = (c * far_re - s * far_im).astype(jnp.bfloat16)
            wide[144 * k : 144 * (k + 1), LANES:] = (c * far_im + s * far_re).astype(jnp.bfloat16)

        occupied = [1.0 / (jnp.exp(f) - 1.0) for f in freqs]
        mismatch = freqs[0] + freqs[1] - freqs[2] - freqs[3]
        delta = jnp.exp(-((mismatch / SMEARING) ** 2)) / (SMEARING * math.sqrt(math.pi))
        weight = (1.0 + occupied[1]) * occupied[2] * occupied[3] / occupied[0]
        product = freqs[0] * freqs[1] * freqs[2] * freqs[3]
        valid = (raw[1:2, :] >= 0) & (index < total)
        scale[...] = jnp.where(valid, delta * weight / product, 0.0)

    def contract(index, wide, near, scale):
        slot = live_s[index]
        weighted = jnp.dot(phi[...], wide[...], preferred_element_type=jnp.float32)
        w_re, w_im = weighted[:, :LANES], weighted[:, LANES:]
        near_re, near_im = near[0:144], near[144:288]
        value_re = jnp.sum(near_re * w_re - near_im * w_im, axis=0, keepdims=True)
        value_im = jnp.sum(near_re * w_im + near_im * w_re, axis=0, keepdims=True)
        term = (value_re * value_re + value_im * value_im) * scale[...]

        first = jnp.maximum(blocks[slot >> 1, slot & 1][0:1, :], 0)
        high = floor_div(first, 192)
        low = first - 192 * high
        placed = jnp.where(lax.broadcasted_iota(jnp.int32, (NB, LANES), 0) == high, term, 0.0)
        one = placed.astype(jnp.bfloat16)
        rest = placed - one.astype(jnp.float32)
        two = rest.astype(jnp.bfloat16)
        three = (rest - two.astype(jnp.float32)).astype(jnp.bfloat16)
        spot = jnp.where(lax.broadcasted_iota(jnp.int32, (256, LANES), 0) == low, 1.0, 0.0).astype(jnp.bfloat16)
        sums[...] += lax.dot_general(
            jnp.concatenate([one, two, three], axis=0), spot, NT, preferred_element_type=jnp.float32
        )

    fetch(0, rows_a, 0).start()
    fetch(1, rows_b, 1).start()
    fetch(0, rows_a, 0).wait()
    gather(held_a, rows_a)
    fetch(2, rows_a, 0).start()
    fetch(1, rows_b, 1).wait()
    gather(held_b, rows_b)
    products(held_a, 0, wide_a, near_a, scale_a)
    fetch(3, rows_b, 1).start()

    def two_blocks(it, carry):
        i = 2 * it
        fetch(i + 2, rows_a, 0).wait()
        gather(held_a, rows_a)
        products(held_b, i + 1, wide_b, near_b, scale_b)
        contract(i, wide_a, near_a, scale_a)
        fetch(i + 4, rows_a, 0).start()
        fetch(i + 3, rows_b, 1).wait()
        gather(held_b, rows_b)
        products(held_a, i + 2, wide_a, near_a, scale_a)
        contract(i + 1, wide_b, near_b, scale_b)
        fetch(i + 5, rows_b, 1).start()
        return carry

    trips = (total + 1) // 2
    lax.fori_loop(0, trips, two_blocks, 0)
    fetch(2 * trips + 2, rows_a, 0).wait()
    fetch(2 * trips + 3, rows_b, 1).wait()
    result = sums[0:16] + sums[16:32] + sums[32:48]
    for w in range(NB):
        out[w] = result[w : w + 1]


def quartet_sums(*operands):
    vmem = pl.BlockSpec(memory_space=pltpu.VMEM)
    pinned = [pltpu.with_memory_space_constraint(a, pltpu.VMEM) for a in operands]
    return pl.pallas_call(
        quartet_kernel,
        out_shape=pltpu.VMEM((NB, 1, 256), jnp.float32),
        in_specs=[vmem] * 8,
        out_specs=vmem,
        scratch_shapes=[
            pltpu.VMEM((1152, 256), jnp.bfloat16),
            pltpu.VMEM((1152, 256), jnp.bfloat16),
            pltpu.VMEM((288, LANES), jnp.float32),
            pltpu.VMEM((288, LANES), jnp.float32),
            pltpu.VMEM((1, LANES), jnp.float32),
            pltpu.VMEM((1, LANES), jnp.float32),
            pltpu.VMEM((4 * LANES, LANES), jnp.float32),
            pltpu.VMEM((4 * LANES, LANES), jnp.float32),
            pltpu.SMEM((4, LANES), jnp.int32),
            pltpu.SMEM((4, LANES), jnp.int32),
            pltpu.SMEM((NB, 1, LANES), jnp.int32),
            pltpu.SMEM((2 * NB + 8,), jnp.int32),
            pltpu.VMEM((48, 256), jnp.float32),
            pltpu.SemaphoreType.DMA((3,)),
        ],
        compiler_params=pltpu.CompilerParams(vmem_limit_bytes=16 << 20),
        name="quartets",
    )(*pinned)


def reduce_kernel(part, out, arrived, send, recv):
    pb, wa = lax.axis_index("pb"), lax.axis_index("wa")
    barrier = pltpu.get_barrier_semaphore()
    peers = [lax.rem(wa + k, NB) for k in range(1, NB)]
    for peer in peers:
        pl.semaphore_signal(barrier, inc=1, device_id=(pb, peer), device_id_type=MESH)
    pl.semaphore_wait(barrier, NB - 1)
    for k, peer in enumerate(peers):
        pltpu.make_async_remote_copy(
            src_ref=part.at[peer], dst_ref=arrived.at[k], send_sem=send.at[0], recv_sem=recv.at[0],
            device_id=(pb, peer), device_id_type=MESH,
        ).start()
    everything = pltpu.make_async_remote_copy(
        src_ref=part.at[pl.ds(0, NB - 1)], dst_ref=arrived, send_sem=send.at[0], recv_sem=recv.at[0],
        device_id=(pb, peers[0]), device_id_type=MESH,
    )
    everything.wait_recv()
    total = part[wa]
    for k in range(NB - 1):
        total = total + arrived[k]
    out[...] = total
    everything.wait_send()


def reduce_over_wa(part):
    vmem = pl.BlockSpec(memory_space=pltpu.VMEM)
    return pl.pallas_call(
        reduce_kernel,
        out_shape=jax.ShapeDtypeStruct((1, 256), jnp.float32),
        in_specs=[vmem],
        out_specs=vmem,
        scratch_shapes=[
            pltpu.VMEM((NB - 1, 1, 256), jnp.float32),
            pltpu.SemaphoreType.DMA((1,)),
            pltpu.SemaphoreType.DMA((1,)),
        ],
        compiler_params=pltpu.CompilerParams(collective_id=1, has_side_effects=True, vmem_limit_bytes=1 << 20),
        name="reduce_wa",
    )(pltpu.with_memory_space_constraint(part, pltpu.VMEM))


def body(quartets, counts, eig, freq, phi, cells):
    dealt = quartets.reshape(2, NB, 4, LANES)
    held = exchange(eig, freq.reshape(24, LANES), dealt, phi, cells, counts)
    part = quartet_sums(*held)
    return reduce_over_wa(part)[0, :192]


def solution(mesh):
    placed = (P(("pb", "wa"), None, None), P(("pb", "wa")), P(None, "pb"), P("pb"), P(), P())
    return jax.shard_map(body, mesh=mesh, in_specs=placed, out_specs=P(("pb", "wa")), check_vma=False)
```

```python
import functools
import math

import jax
import jax.numpy as jnp
from jax import lax
from jax.experimental import pallas as pl
from jax.experimental.pallas import tpu as pltpu
from jax.sharding import PartitionSpec as P

QMESH = 16
BR = 12
NB = 16
LOCAL = 3072
GROUP = 768
LANES = 128
GROUP_AT = (0, 768, 1664, 2432)
FREQ_AT = 1536
WIDTH = 3200
SMEARING = 0.5
MESH = pl.DeviceIdType.MESH
NT = (((1,), (1,)), ((), ()))


ORDER = (
    (-1, 0), (1, 0), (0, -1), (0, 1), (2, 0), (-1, -1), (-1, 1), (0, 2), (1, -1), (1, 1), (-1, 2), (2, -1), (2, 1), (1, 2), (2, 2),
)
WAVES = (
    ((-1, 0), (1, 0), (0, -1), (0, 1)),
    ((2, 0), (0, 2)),
    ((-1, 1), (1, -1)),
    ((-1, -1), (1, 1)),
    ((-1, 2), (2, -1), (2, 1), (1, 2)),
    ((2, 2),),
)
WAVE_AFTER = {5: (0,), 9: (1,), 10: (2,), 12: (3,), 14: (4, 5)}


def wrapped(offset):
    return (offset + 1) % 4 - 1


def hit(rows, columns, where):
    r = lax.broadcasted_iota(jnp.int32, (rows, columns), 0)
    c = lax.broadcasted_iota(jnp.int32, (rows, columns), 1)
    return jnp.where(where(r) == c, 1.0, 0.0).astype(jnp.bfloat16)


def spread_column(r):
    kind = floor_div(r, 144)
    t = r - 144 * kind
    first = floor_div(t, BR)
    return ((kind + 2) & 3) * 16 + jnp.where((kind & 1) == 0, first, t - BR * first)


def order_column(r):
    t = r & 31
    lane = jnp.where(t < 12, t, jnp.where(t == 12, 24, jnp.where((t >= 16) & (t < 28), t - 4, -999)))
    return lane + (r - t)


def exchange_kernel(
    eig, freq, quartets, phi, cells, counts,
    table, blocks, tallies, rows, phi_v, cells_v, reorder, spread,
    tab, mine, eye, dealt, send, got, lent, local,
):
    pb, wa = lax.axis_index("pb"), lax.axis_index("wa")
    x, y, core = pb // 4, pb % 4, wa % 2
    ahead = 1 - 2 * core
    sibling = (pb, wa + ahead)

    def place(dx, dy):
        return lax.rem(x + ahead * dx + 4, 4) * 4 + lax.rem(y + ahead * dy + 4, 4)

    barrier = pltpu.get_barrier_semaphore()
    for step in (1, -1):
        pl.semaphore_signal(barrier, inc=1, device_id=(place(step, 0), wa), device_id_type=MESH)
        pl.semaphore_signal(barrier, inc=1, device_id=(place(0, step), wa), device_id_type=MESH)
    for k in range(1, NB):
        pl.semaphore_signal(barrier, inc=1, device_id=(pb, lax.rem(wa + k, NB)), device_id_type=MESH)

    left = pltpu.make_async_copy(eig.at[:, pl.ds(0, 1536)], tab.at[pb, :, pl.ds(0, 1536)], local.at[0])
    right = pltpu.make_async_copy(eig.at[:, pl.ds(1536, 1536)], tab.at[pb, :, pl.ds(1664, 1536)], local.at[1])
    copy_freq = pltpu.make_async_copy(freq, tab.at[pb, :, pl.ds(FREQ_AT, LANES)], local.at[2])
    copy_dealt = pltpu.make_async_copy(quartets, dealt, local.at[3])
    copy_phi = pltpu.make_async_copy(phi, phi_v, local.at[4])
    copy_cells = pltpu.make_async_copy(cells, cells_v, local.at[5])
    own = (left, right, copy_freq, copy_dealt)
    for copy in own + (copy_phi, copy_cells):
        copy.start()
    mine[...] = jnp.full((1, LANES), counts[0], jnp.int32)
    tallies[wa] = mine[...]
    eye[...] = hit(256, 256, lambda r: r)
    reorder[...] = hit(LANES, LANES, order_column)
    spread[...] = hit(576, 64, spread_column)
    for copy in own:
        copy.wait()
    blocks[wa] = dealt[:, 0]

    pl.semaphore_wait(barrier, 4 + NB - 1)

    def push(src, dst, sent, arrival, device):
        pltpu.make_async_remote_copy(
            src_ref=src, dst_ref=dst, send_sem=send.at[sent], recv_sem=arrival, device_id=device, device_id_type=MESH
        ).start()

    def bytes_in(view, sem):
        pltpu.make_async_remote_copy(
            src_ref=view, dst_ref=view, send_sem=send.at[0], recv_sem=sem, device_id=sibling, device_id_type=MESH
        ).wait_recv()

    def bytes_out(view, sent):
        pltpu.make_async_remote_copy(
            src_ref=view, dst_ref=view, send_sem=send.at[sent], recv_sem=got.at[0], device_id=sibling, device_id_type=MESH
        ).wait_send()

    def at(part, first, second):
        return place(first, second) if part == 0 else place(second, first)

    def relay(part, first, second, axis, step):
        shard = at(part, first, second)
        if part == 0:
            view = tab.at[shard, :, pl.ds(pl.multiple_of(core * 2432, LANES), 768)]
        else:
            view = tab.at[shard, :, pl.ds(pl.multiple_of(768 + core * 768, LANES), 896)]
        key = (wrapped(first - step), second) if axis == 0 else (first, wrapped(second - step))
        target = at(part, step, 0) if axis == 0 else at(part, 0, step)
        push(view, view, part, got.at[ORDER.index(key)], (target, wa))

    def lend(part, first, second):
        shard = at(part, first, second)
        if part == 0:
            view = tab.at[shard, :, pl.ds(pl.multiple_of(core * 2432, LANES), 768)]
        else:
            view = tab.at[shard, :, pl.ds(pl.multiple_of(768 + core * 896, LANES), 768)]
        offset = (first, second) if part == 0 else (second, first)
        wave = [w for w, members in enumerate(WAVES) if offset in members][0]
        push(view, view, 2, lent.at[wave], sibling)

    def turn(shard):
        values = tab[shard, :, FREQ_AT : FREQ_AT + LANES].astype(jnp.float32)
        for j in range(3):
            stack = []
            for g in range(4):
                stack.append(tab[shard, :, GROUP_AT[g] + 256 * j : GROUP_AT[g] + 256 * (j + 1)].astype(jnp.float32))
                at_row = 6 * g + 2 * j
                stack.append(
                    jnp.concatenate(
                        [jnp.broadcast_to(values[at_row + h : at_row + h + 1, :], (8, LANES)) for h in range(2)], axis=1
                    )
                )
            stack = jnp.concatenate(stack, axis=0).astype(jnp.bfloat16)
            table[pl.ds(pl.multiple_of(shard * GROUP + 256 * j, 256), 256), :] = lax.dot_general(
                eye[...], stack, NT, preferred_element_type=jnp.float32
            )

    for axis in (0, 1):
        for part in (0, 1):
            relay(part, 0, 0, axis, 1)
            relay(part, 0, 0, axis, -1)
    for k in range(1, NB):
        peer = lax.rem(wa + k, NB)
        push(dealt.at[:, k], blocks.at[wa], 3, lent.at[len(WAVES)], (pb, peer))
        push(mine, tallies.at[wa], 4, lent.at[len(WAVES) + 1], (pb, peer))
    turn(pb)

    for number, (first, second) in enumerate(ORDER):
        bytes_in(tab.at[0, :, pl.ds(0, 1664)], got.at[number])
        for part in (0, 1):
            if second == 0:
                if first == -1:
                    relay(part, first, 0, 0, 1)
                relay(part, first, 0, 1, 1)
                relay(part, first, 0, 1, -1)
            elif second == -1:
                relay(part, first, second, 1, 1)
            lend(part, first, second)
        if number == 7:
            bytes_in(blocks.at[pl.ds(0, NB - 1)], lent.at[len(WAVES)])
            bytes_in(tallies.at[pl.ds(0, NB - 1)], lent.at[len(WAVES) + 1])
            modes = jnp.maximum(blocks[...], 0)
            local_mode = lax.broadcasted_iota(jnp.int32, modes.shape, 2) == 0
            rows[...] = rows_of(modes + jnp.where(local_mode, pb * LOCAL, 0))
        for wave in WAVE_AFTER.get(number, ()):
            members = WAVES[wave]
            bytes_in(tab.at[pl.ds(0, len(members)), :, pl.ds(0, 1536)], lent.at[wave])
            for offset in members:
                turn(place(*offset))

    copy_phi.wait()
    copy_cells.wait()
    bytes_out(tab.at[pl.ds(0, 15), :, pl.ds(0, 768)], 0)
    bytes_out(tab.at[pl.ds(0, 15), :, pl.ds(0, 896)], 1)
    bytes_out(tab.at[pl.ds(0, 15), :, pl.ds(0, 1536)], 2)
    bytes_out(blocks.at[pl.ds(0, NB - 1)], 3)
    bytes_out(tallies.at[pl.ds(0, NB - 1)], 4)


def exchange(eig, freq, quartets, phi, cells, counts):
    hbm = pl.BlockSpec(memory_space=pltpu.HBM)
    vmem = pl.BlockSpec(memory_space=pltpu.VMEM)
    return pl.pallas_call(
        exchange_kernel,
        out_shape=(
            pltpu.VMEM((NB * GROUP, LANES), jnp.float32),
            pltpu.VMEM((NB, 2, 4, LANES), jnp.int32),
            pltpu.VMEM((NB, 1, LANES), jnp.int32),
            pltpu.VMEM((NB, 2, 4, LANES), jnp.int32),
            pltpu.VMEM((144, 1152), jnp.bfloat16),
            pltpu.VMEM((8, 9), jnp.int32),
            pltpu.VMEM((128, 128), jnp.bfloat16),
            pltpu.VMEM((576, 64), jnp.bfloat16),
        ),
        in_specs=[hbm] * 5 + [pl.BlockSpec(memory_space=pltpu.SMEM)],
        out_specs=(vmem,) * 8,
        scratch_shapes=[
            pltpu.VMEM((NB, 24, WIDTH), jnp.bfloat16),
            pltpu.VMEM((1, LANES), jnp.int32),
            pltpu.VMEM((256, 256), jnp.bfloat16),
            pltpu.VMEM((2, NB, 4, LANES), jnp.int32),
            pltpu.SemaphoreType.DMA((5,)),
            pltpu.SemaphoreType.DMA((len(ORDER),)),
            pltpu.SemaphoreType.DMA((len(WAVES) + 2,)),
            pltpu.SemaphoreType.DMA((6,)),
        ],
        compiler_params=pltpu.CompilerParams(collective_id=0, has_side_effects=True, vmem_limit_bytes=24 << 20),
        name="exchange",
    )(*[pltpu.with_memory_space_constraint(a, pltpu.HBM) for a in (eig, freq, quartets, phi, cells)], counts)


def cosine_of(step):
    near = jnp.minimum(step, 16 - step)
    out = jnp.full(step.shape, -1.0, jnp.float32)
    for k in range(8):
        out = jnp.where(near == k, math.cos(math.pi * k / 8) if k != 4 else 0.0, out)
    return out


def floor_div(value, by):
    return jnp.floor((value.astype(jnp.float32) + 0.5) * (1.0 / by)).astype(jnp.int32)


def rows_of(modes):
    unit = floor_div(modes, GROUP)
    return (unit >> 2) * GROUP + modes - unit * GROUP


def quartet_kernel(
    table, blocks, tallies, rows, phi, cells, reorder, spread, out,
    wide_a, wide_b, near_a, near_b, scale_a, scale_b, term_a, term_b, vectors_a, vectors_b, held_a, held_b,
    rows_a, rows_b, tally_s, live_s, sums, sem,
):
    pb, wa = lax.axis_index("pb"), lax.axis_index("wa")
    copy_tally = pltpu.make_async_copy(tallies, tally_s, sem.at[2])
    copy_tally.start()
    sums[...] = jnp.zeros_like(sums)
    cell = cells[...].astype(jnp.float32)
    copy_tally.wait()

    live_s[0] = 0
    total = jnp.int32(0)
    for source in range(NB):
        held = (wa - source) & (NB - 1)
        tally = tally_s[source, 0, 0]
        for high in range(2):
            live_s[total] = 2 * source + high
            total = total + (held + NB * high < tally).astype(jnp.int32)
    for k in range(6):
        live_s[total + k] = 0

    def fetch(index, into, which):
        slot = live_s[index]
        return pltpu.make_async_copy(rows.at[slot >> 1, slot & 1], into, sem.at[which])

    sublane = lax.broadcasted_iota(jnp.int32, (8, LANES), 0)
    odd = [(sublane & (1 << bit)) != 0 for bit in range(3)]

    def gather(into, at):
        for k in range(4):
            for n in range(0, LANES, 16):
                pair = []
                for half in (n, n + 8):
                    level = [table[pl.ds(at[k, half + j], 8, stride=0), :] for j in range(8)]
                    for bit in range(3):
                        level = [jnp.where(odd[bit], high, low) for low, high in zip(level[::2], level[1::2])]
                    pair.append(level[0])
                into[LANES * k + n : LANES * k + n + 16, :] = jnp.concatenate(pair, axis=0).astype(jnp.bfloat16)

    def vectors_of(at, index, held, vectors, scale):
        gather(held, at)
        slot = live_s[index]
        raw = blocks[slot >> 1, slot & 1]
        modes = jnp.maximum(raw, 0)
        fullmode = modes + jnp.where(lax.broadcasted_iota(jnp.int32, modes.shape, 0) == 0, pb * LOCAL, 0)
        group = floor_div(fullmode, GROUP) & 3
        turned = lax.dot_general(reorder[...], held[...], NT, preferred_element_type=jnp.float32)
        halves, freqs = [], []
        for k in range(4):
            which = group[k : k + 1, :]
            part = turned[:, LANES * k : LANES * (k + 1)]
            mine = jnp.where(
                which < 2,
                jnp.where(which == 0, part[0:32], part[32:64]),
                jnp.where(which == 2, part[64:96], part[96:128]),
            )
            halves.append(jnp.concatenate([mine[0:16], mine[16:32]], axis=1))
            freqs.append(mine[12:13])
        vectors[...] = jnp.concatenate(halves, axis=0).astype(jnp.bfloat16)
        occupied = [1.0 / (jnp.exp(f) - 1.0) for f in freqs]
        mismatch = freqs[0] + freqs[1] - freqs[2] - freqs[3]
        delta = jnp.exp(-((mismatch / SMEARING) ** 2)) / (SMEARING * math.sqrt(math.pi))
        weight = (1.0 + occupied[1]) * occupied[2] * occupied[3] / occupied[0]
        product = freqs[0] * freqs[1] * freqs[2] * freqs[3]
        valid = (raw[1:2, :] >= 0) & (index < total)
        scale[...] = jnp.where(valid, delta * weight / product, 0.0)

    def products(index, vectors, wide, near):
        slot = live_s[index]
        modes = jnp.maximum(blocks[slot >> 1, slot & 1], 0)
        pairs = jnp.dot(spread[...], vectors[...], preferred_element_type=jnp.float32)
        third, fourth, e1, e2 = (pairs[144 * k : 144 * (k + 1)] for k in range(4))
        far_re = third[:, :LANES] * fourth[:, :LANES] - third[:, LANES:] * fourth[:, LANES:]
        far_im = -(third[:, :LANES] * fourth[:, LANES:] + third[:, LANES:] * fourth[:, :LANES])
        near[0:144] = e1[:, :LANES] * e2[:, :LANES] - e1[:, LANES:] * e2[:, LANES:]
        near[144:288] = e1[:, :LANES] * e2[:, LANES:] + e1[:, LANES:] * e2[:, :LANES]

        point = floor_div(modes, BR)
        coords = [(point >> 8).astype(jnp.float32), ((point >> 4) & 15).astype(jnp.float32), (point & 15).astype(jnp.float32)]
        shift = jnp.zeros((8, LANES), jnp.float32)
        for which in range(3):
            for axis in range(3):
                column = cell[:, 3 * which + axis : 3 * which + axis + 1]
                term = column * coords[axis][which + 1 : which + 2, :]
                shift = shift + term if which == 0 else shift - term
        step = shift.astype(jnp.int32) & 15
        cosine, sine = cosine_of(step), cosine_of((step - 4) & 15)
        for k in range(8):
            c, s = cosine[k : k + 1, :], sine[k : k + 1, :]
            wide[144 * k : 144 * (k + 1), :LANES] = (c * far_re - s * far_im).astype(jnp.bfloat16)
            wide[144 * k : 144 * (k + 1), LANES:] = (c * far_im + s * far_re).astype(jnp.bfloat16)

    def contract(wide, near, scale, term):
        weighted = jnp.dot(phi[...], wide[...], preferred_element_type=jnp.float32)
        w_re, w_im = weighted[:, :LANES], weighted[:, LANES:]
        near_re, near_im = near[0:144], near[144:288]
        value_re = jnp.sum(near_re * w_re - near_im * w_im, axis=0, keepdims=True)
        value_im = jnp.sum(near_re * w_im + near_im * w_re, axis=0, keepdims=True)
        term[...] = (value_re * value_re + value_im * value_im) * scale[...]

    def scatter(index, term):
        slot = live_s[index]
        first = jnp.maximum(blocks[slot >> 1, slot & 1][0:1, :], 0)
        high = floor_div(first, 192)
        low = first - 192 * high
        placed = jnp.where(lax.broadcasted_iota(jnp.int32, (NB, LANES), 0) == high, term, 0.0)
        one = placed.astype(jnp.bfloat16)
        rest = placed - one.astype(jnp.float32)
        two = rest.astype(jnp.bfloat16)
        three = (rest - two.astype(jnp.float32)).astype(jnp.bfloat16)
        spot = jnp.where(lax.broadcasted_iota(jnp.int32, (256, LANES), 0) == low, 1.0, 0.0).astype(jnp.bfloat16)
        sums[...] += lax.dot_general(
            jnp.concatenate([one, two, three], axis=0), spot, NT, preferred_element_type=jnp.float32
        )

    sides = (
        (rows_a, held_a, vectors_a, scale_a, wide_a, near_a, term_a, 0),
        (rows_b, held_b, vectors_b, scale_b, wide_b, near_b, term_b, 1),
    )

    def step_of(i, side):
        at, held, vectors, scale, wide, near, term, which = sides[side]
        _, _, next_vectors, _, next_wide, next_near, last_term, _ = sides[1 - side]
        fetch(i + 2, at, which).wait()
        scatter(jnp.maximum(i - 1, 0), last_term[...])
        contract(wide, near, scale, term)
        products(i + 1, next_vectors, next_wide, next_near)
        vectors_of(at, i + 2, held, vectors, scale)
        fetch(i + 4, at, which).start()

    term_b[...] = jnp.zeros_like(term_b)
    fetch(0, rows_a, 0).start()
    fetch(1, rows_b, 1).start()
    fetch(0, rows_a, 0).wait()
    vectors_of(rows_a, 0, held_a, vectors_a, scale_a)
    fetch(2, rows_a, 0).start()
    fetch(1, rows_b, 1).wait()
    products(0, vectors_a, wide_a, near_a)
    vectors_of(rows_b, 1, held_b, vectors_b, scale_b)
    fetch(3, rows_b, 1).start()

    def two_blocks(it, carry):
        step_of(2 * it, 0)

        @pl.when(2 * it + 1 < total)
        def _():
            step_of(2 * it + 1, 1)

        return carry

    lax.fori_loop(0, (total + 1) // 2, two_blocks, 0)
    scatter(total - 1, jnp.where(total % 2 == 1, term_a[...], term_b[...]))
    fetch(0, rows_a, 0).wait()
    fetch(0, rows_b, 1).wait()
    result = sums[0:16] + sums[16:32] + sums[32:48]
    for w in range(NB):
        out[w] = result[w : w + 1]


def quartet_sums(*operands):
    vmem = pl.BlockSpec(memory_space=pltpu.VMEM)
    pinned = [pltpu.with_memory_space_constraint(a, pltpu.VMEM) for a in operands]
    return pl.pallas_call(
        quartet_kernel,
        out_shape=pltpu.VMEM((NB, 1, 256), jnp.float32),
        in_specs=[vmem] * 8,
        out_specs=vmem,
        scratch_shapes=[
            pltpu.VMEM((1152, 256), jnp.bfloat16),
            pltpu.VMEM((1152, 256), jnp.bfloat16),
            pltpu.VMEM((288, LANES), jnp.float32),
            pltpu.VMEM((288, LANES), jnp.float32),
            pltpu.VMEM((1, LANES), jnp.float32),
            pltpu.VMEM((1, LANES), jnp.float32),
            pltpu.VMEM((1, LANES), jnp.float32),
            pltpu.VMEM((1, LANES), jnp.float32),
            pltpu.VMEM((64, 256), jnp.bfloat16),
            pltpu.VMEM((64, 256), jnp.bfloat16),
            pltpu.VMEM((4 * LANES, LANES), jnp.bfloat16),
            pltpu.VMEM((4 * LANES, LANES), jnp.bfloat16),
            pltpu.SMEM((4, LANES), jnp.int32),
            pltpu.SMEM((4, LANES), jnp.int32),
            pltpu.SMEM((NB, 1, LANES), jnp.int32),
            pltpu.SMEM((2 * NB + 8,), jnp.int32),
            pltpu.VMEM((48, 256), jnp.float32),
            pltpu.SemaphoreType.DMA((3,)),
        ],
        compiler_params=pltpu.CompilerParams(vmem_limit_bytes=16 << 20),
        name="quartets",
    )(*pinned)


def reduce_kernel(part, out, arrived, send, recv):
    pb, wa = lax.axis_index("pb"), lax.axis_index("wa")
    barrier = pltpu.get_barrier_semaphore()
    peers = [lax.rem(wa + k, NB) for k in range(1, NB)]
    for peer in peers:
        pl.semaphore_signal(barrier, inc=1, device_id=(pb, peer), device_id_type=MESH)
    pl.semaphore_wait(barrier, NB - 1)
    for k, peer in enumerate(peers):
        pltpu.make_async_remote_copy(
            src_ref=part.at[peer], dst_ref=arrived.at[k], send_sem=send.at[0], recv_sem=recv.at[0],
            device_id=(pb, peer), device_id_type=MESH,
        ).start()
    everything = pltpu.make_async_remote_copy(
        src_ref=part.at[pl.ds(0, NB - 1)], dst_ref=arrived, send_sem=send.at[0], recv_sem=recv.at[0],
        device_id=(pb, peers[0]), device_id_type=MESH,
    )
    everything.wait_recv()
    total = part[wa]
    for k in range(NB - 1):
        total = total + arrived[k]
    out[...] = total
    everything.wait_send()


def reduce_over_wa(part):
    vmem = pl.BlockSpec(memory_space=pltpu.VMEM)
    return pl.pallas_call(
        reduce_kernel,
        out_shape=jax.ShapeDtypeStruct((1, 256), jnp.float32),
        in_specs=[vmem],
        out_specs=vmem,
        scratch_shapes=[
            pltpu.VMEM((NB - 1, 1, 256), jnp.float32),
            pltpu.SemaphoreType.DMA((1,)),
            pltpu.SemaphoreType.DMA((1,)),
        ],
        compiler_params=pltpu.CompilerParams(collective_id=1, has_side_effects=True, vmem_limit_bytes=1 << 20),
        name="reduce_wa",
    )(pltpu.with_memory_space_constraint(part, pltpu.VMEM))


def body(quartets, counts, eig, freq, phi, cells):
    dealt = quartets.reshape(2, NB, 4, LANES)
    held = exchange(eig, freq.reshape(24, LANES), dealt, phi, cells, counts)
    part = quartet_sums(*held)
    return reduce_over_wa(part)[0, :192]


def solution(mesh):
    placed = (P(("pb", "wa"), None, None), P(("pb", "wa")), P(None, "pb"), P("pb"), P(), P())
    return jax.shard_map(body, mesh=mesh, in_specs=placed, out_specs=P(("pb", "wa")), check_vma=False)
```

```python
import functools
import math

import jax
import jax.numpy as jnp
from jax import lax
from jax.experimental import pallas as pl
from jax.experimental.pallas import tpu as pltpu
from jax.sharding import PartitionSpec as P

QMESH = 16
BR = 12
NB = 16
LOCAL = 3072
GROUP = 768
LANES = 128
GROUP_AT = (0, 768, 1664, 2432)
FREQ_AT = 1536
WIDTH = 3200
SMEARING = 0.5
MESH = pl.DeviceIdType.MESH
NT = (((1,), (1,)), ((), ()))


PIECES = {(1, 0): (0, 768), (1, 1): (768, 896), (-1, 1): (1664, 768), (-1, 0): (2432, 768)}
RELAY_CORE = 1
ORDER = (
    (-1, 0), (1, 0), (0, -1), (0, 1), (2, 0), (-1, -1), (-1, 1), (0, 2), (1, -1), (1, 1), (-1, 2), (2, -1), (2, 1), (1, 2), (2, 2),
)
WAVES = (
    ((-1, 0), (1, 0), (0, -1), (0, 1)),
    ((2, 0), (0, 2)),
    ((-1, 1), (1, -1)),
    ((-1, -1), (1, 1)),
    ((-1, 2), (2, -1), (2, 1), (1, 2)),
    ((2, 2),),
)
WAVE_AFTER = {5: (0,), 9: (1,), 10: (2,), 12: (3,), 14: (4, 5)}


def wrapped(offset):
    return (offset + 1) % 4 - 1


def hit(rows, columns, where):
    r = lax.broadcasted_iota(jnp.int32, (rows, columns), 0)
    c = lax.broadcasted_iota(jnp.int32, (rows, columns), 1)
    return jnp.where(where(r) == c, 1.0, 0.0).astype(jnp.bfloat16)


def spread_column(r):
    kind = floor_div(r, 144)
    t = r - 144 * kind
    first = floor_div(t, BR)
    return ((kind + 2) & 3) * 16 + jnp.where((kind & 1) == 0, first, t - BR * first)


def order_column(r):
    t = r & 31
    lane = jnp.where(t < 12, t, jnp.where(t == 12, 24, jnp.where((t >= 16) & (t < 28), t - 4, -999)))
    return lane + (r - t)


def exchange_kernel(
    eig, freq, quartets, phi, cells, counts,
    table, blocks, tallies, rows, phi_v, cells_v, reorder, spread,
    tab, mine, eye, dealt, send, got, lent, local,
):
    pb, wa = lax.axis_index("pb"), lax.axis_index("wa")
    x, y, core = pb // 4, pb % 4, wa % 2
    relays = core == RELAY_CORE
    sibling = (pb, wa + 1 - 2 * core)

    def place(dx, dy):
        return lax.rem(x + dx + 4, 4) * 4 + lax.rem(y + dy + 4, 4)

    barrier = pltpu.get_barrier_semaphore()

    @pl.when(relays)
    def _():
        for step in (1, -1):
            pl.semaphore_signal(barrier, inc=1, device_id=(place(step, 0), wa), device_id_type=MESH)
            pl.semaphore_signal(barrier, inc=1, device_id=(place(0, step), wa), device_id_type=MESH)

    for k in range(1, NB):
        pl.semaphore_signal(barrier, inc=1, device_id=(pb, lax.rem(wa + k, NB)), device_id_type=MESH)

    left = pltpu.make_async_copy(eig.at[:, pl.ds(0, 1536)], tab.at[pb, :, pl.ds(0, 1536)], local.at[0])
    right = pltpu.make_async_copy(eig.at[:, pl.ds(1536, 1536)], tab.at[pb, :, pl.ds(1664, 1536)], local.at[1])
    copy_freq = pltpu.make_async_copy(freq, tab.at[pb, :, pl.ds(FREQ_AT, LANES)], local.at[2])
    copy_dealt = pltpu.make_async_copy(quartets, dealt, local.at[3])
    copy_phi = pltpu.make_async_copy(phi, phi_v, local.at[4])
    copy_cells = pltpu.make_async_copy(cells, cells_v, local.at[5])
    own = (left, right, copy_freq, copy_dealt)
    for copy in own + (copy_phi, copy_cells):
        copy.start()
    mine[...] = jnp.full((1, LANES), counts[0], jnp.int32)
    tallies[wa] = mine[...]
    eye[...] = hit(256, 256, lambda r: r)
    reorder[...] = hit(LANES, LANES, order_column)
    spread[...] = hit(576, 64, spread_column)
    for copy in own:
        copy.wait()
    blocks[wa] = dealt[:, 0]

    pl.semaphore_wait(barrier, NB - 1 + jnp.where(relays, 4, 0))

    def push(src, dst, sent, arrival, device):
        pltpu.make_async_remote_copy(
            src_ref=src, dst_ref=dst, send_sem=send.at[sent], recv_sem=arrival, device_id=device, device_id_type=MESH
        ).start()

    def bytes_in(view, sem):
        pltpu.make_async_remote_copy(
            src_ref=view, dst_ref=view, send_sem=send.at[0], recv_sem=sem, device_id=sibling, device_id_type=MESH
        ).wait_recv()

    def bytes_out(view, sent):
        pltpu.make_async_remote_copy(
            src_ref=view, dst_ref=view, send_sem=send.at[sent], recv_sem=got.at[0], device_id=sibling, device_id_type=MESH
        ).wait_send()

    def at(way, part, first, second):
        return place(way * first, way * second) if part == 0 else place(way * second, way * first)

    def relay(way, part, first, second, axis, step):
        start, width = PIECES[way, part]
        view = tab.at[at(way, part, first, second), :, pl.ds(start, width)]
        key = (wrapped(first - step), second) if axis == 0 else (first, wrapped(second - step))
        target = at(way, part, step, 0) if axis == 0 else at(way, part, 0, step)
        push(view, view, 0, got.at[ORDER.index(key)], (target, wa))

    def lend(way, part, first, second):
        start, width = PIECES[way, part]
        view = tab.at[at(way, part, first, second), :, pl.ds(start, width)]
        offset = (way * first, way * second) if part == 0 else (way * second, way * first)
        offset = tuple(wrapped(o) for o in offset)
        wave = [w for w, members in enumerate(WAVES) if offset in members][0]
        push(view, view, 1, lent.at[wave], sibling)

    def turn(shard):
        values = tab[shard, :, FREQ_AT : FREQ_AT + LANES].astype(jnp.float32)
        for j in range(3):
            stack = []
            for g in range(4):
                stack.append(tab[shard, :, GROUP_AT[g] + 256 * j : GROUP_AT[g] + 256 * (j + 1)].astype(jnp.float32))
                at_row = 6 * g + 2 * j
                stack.append(
                    jnp.concatenate(
                        [jnp.broadcast_to(values[at_row + h : at_row + h + 1, :], (8, LANES)) for h in range(2)], axis=1
                    )
                )
            stack = jnp.concatenate(stack, axis=0).astype(jnp.bfloat16)
            table[pl.ds(pl.multiple_of(shard * GROUP + 256 * j, 256), 256), :] = lax.dot_general(
                eye[...], stack, NT, preferred_element_type=jnp.float32
            )

    @pl.when(relays)
    def _():
        for axis in (0, 1):
            for way in (1, -1):
                for part in (0, 1):
                    relay(way, part, 0, 0, axis, 1)
                    relay(way, part, 0, 0, axis, -1)

    for k in range(1, NB):
        peer = lax.rem(wa + k, NB)
        push(dealt.at[:, k], blocks.at[wa], 2, lent.at[len(WAVES)], (pb, peer))
        push(mine, tallies.at[wa], 3, lent.at[len(WAVES) + 1], (pb, peer))
    turn(pb)

    def blocks_in():
        bytes_in(blocks.at[pl.ds(0, NB - 1)], lent.at[len(WAVES)])
        bytes_in(tallies.at[pl.ds(0, NB - 1)], lent.at[len(WAVES) + 1])
        modes = jnp.maximum(blocks[...], 0)
        local_mode = lax.broadcasted_iota(jnp.int32, modes.shape, 2) == 0
        rows[...] = rows_of(modes + jnp.where(local_mode, pb * LOCAL, 0))

    @pl.when(relays)
    def _():
        for number, (first, second) in enumerate(ORDER):
            bytes_in(tab.at[0], got.at[number])
            for way in (1, -1):
                for part in (0, 1):
                    if second == 0:
                        if first == -1:
                            relay(way, part, first, 0, 0, 1)
                        relay(way, part, first, 0, 1, 1)
                        relay(way, part, first, 0, 1, -1)
                    elif second == -1:
                        relay(way, part, first, second, 1, 1)
                    lend(way, part, first, second)
            if number == 7:
                blocks_in()
            for wave in WAVE_AFTER.get(number, ()):
                for offset in WAVES[wave]:
                    turn(place(*offset))
        bytes_out(tab.at[pl.ds(0, 15)], 0)
        bytes_out(tab.at[pl.ds(0, 15)], 1)

    @pl.when(jnp.logical_not(relays))
    def _():
        for wave, members in enumerate(WAVES):
            if wave == 1:
                blocks_in()
            bytes_in(tab.at[pl.ds(0, len(members))], lent.at[wave])
            for offset in members:
                turn(place(*offset))

    copy_phi.wait()
    copy_cells.wait()
    bytes_out(blocks.at[pl.ds(0, NB - 1)], 2)
    bytes_out(tallies.at[pl.ds(0, NB - 1)], 3)


def exchange(eig, freq, quartets, phi, cells, counts):
    hbm = pl.BlockSpec(memory_space=pltpu.HBM)
    vmem = pl.BlockSpec(memory_space=pltpu.VMEM)
    return pl.pallas_call(
        exchange_kernel,
        out_shape=(
            pltpu.VMEM((NB * GROUP, LANES), jnp.float32),
            pltpu.VMEM((NB, 2, 4, LANES), jnp.int32),
            pltpu.VMEM((NB, 1, LANES), jnp.int32),
            pltpu.VMEM((NB, 2, 4, LANES), jnp.int32),
            pltpu.VMEM((144, 1152), jnp.bfloat16),
            pltpu.VMEM((8, 9), jnp.int32),
            pltpu.VMEM((128, 128), jnp.bfloat16),
            pltpu.VMEM((576, 64), jnp.bfloat16),
        ),
        in_specs=[hbm] * 5 + [pl.BlockSpec(memory_space=pltpu.SMEM)],
        out_specs=(vmem,) * 8,
        scratch_shapes=[
            pltpu.VMEM((NB, 24, WIDTH), jnp.bfloat16),
            pltpu.VMEM((1, LANES), jnp.int32),
            pltpu.VMEM((256, 256), jnp.bfloat16),
            pltpu.VMEM((2, NB, 4, LANES), jnp.int32),
            pltpu.SemaphoreType.DMA((4,)),
            pltpu.SemaphoreType.DMA((len(ORDER),)),
            pltpu.SemaphoreType.DMA((len(WAVES) + 2,)),
            pltpu.SemaphoreType.DMA((6,)),
        ],
        compiler_params=pltpu.CompilerParams(collective_id=0, has_side_effects=True, vmem_limit_bytes=24 << 20),
        name="exchange",
    )(*[pltpu.with_memory_space_constraint(a, pltpu.HBM) for a in (eig, freq, quartets, phi, cells)], counts)


def cosine_of(step):
    near = jnp.minimum(step, 16 - step)
    out = jnp.full(step.shape, -1.0, jnp.float32)
    for k in range(8):
        out = jnp.where(near == k, math.cos(math.pi * k / 8) if k != 4 else 0.0, out)
    return out


def floor_div(value, by):
    return jnp.floor((value.astype(jnp.float32) + 0.5) * (1.0 / by)).astype(jnp.int32)


def rows_of(modes):
    unit = floor_div(modes, GROUP)
    return (unit >> 2) * GROUP + modes - unit * GROUP


def quartet_kernel(
    table, blocks, tallies, rows, phi, cells, reorder, spread, out,
    wide_a, wide_b, near_a, near_b, scale_a, scale_b, term_a, term_b, freqs_a, freqs_b, vectors_a, vectors_b, held_a, held_b,
    rows_a, rows_b, tally_s, live_s, sums, sem,
):
    pb, wa = lax.axis_index("pb"), lax.axis_index("wa")
    copy_tally = pltpu.make_async_copy(tallies, tally_s, sem.at[2])
    copy_tally.start()
    first_rows = pltpu.make_async_copy(rows.at[wa, 0], rows_a, sem.at[0])
    first_rows.start()
    sums[...] = jnp.zeros_like(sums)
    cell = cells[...].astype(jnp.float32)
    copy_tally.wait()

    live_s[0] = 0
    total = jnp.int32(0)
    for held in range(NB):
        source = (wa - held) & (NB - 1)
        tally = tally_s[source, 0, 0]
        for high in range(2):
            live_s[total] = 2 * source + high
            total = total + (held + NB * high < tally).astype(jnp.int32)
    for k in range(6):
        live_s[total + k] = 0

    def fetch(index, into, which):
        slot = live_s[index]
        return pltpu.make_async_copy(rows.at[slot >> 1, slot & 1], into, sem.at[which])

    sublane = lax.broadcasted_iota(jnp.int32, (8, LANES), 0)
    odd = [(sublane & (1 << bit)) != 0 for bit in range(3)]

    def gather(into, at):
        for k in range(4):
            for n in range(0, LANES, 16):
                pair = []
                for half in (n, n + 8):
                    level = [table[pl.ds(at[k, half + j], 8, stride=0), :] for j in range(8)]
                    for bit in range(3):
                        level = [jnp.where(odd[bit], high, low) for low, high in zip(level[::2], level[1::2])]
                    pair.append(level[0])
                into[LANES * k + n : LANES * k + n + 16, :] = jnp.concatenate(pair, axis=0).astype(jnp.bfloat16)

    def vectors_of(at, index, held, vectors, freqs_of):
        gather(held, at)
        slot = live_s[index]
        raw = blocks[slot >> 1, slot & 1]
        modes = jnp.maximum(raw, 0)
        fullmode = modes + jnp.where(lax.broadcasted_iota(jnp.int32, modes.shape, 0) == 0, pb * LOCAL, 0)
        group = floor_div(fullmode, GROUP) & 3
        turned = lax.dot_general(reorder[...], held[...], NT, preferred_element_type=jnp.float32)
        halves, freqs = [], []
        for k in range(4):
            which = group[k : k + 1, :]
            part = turned[:, LANES * k : LANES * (k + 1)]
            mine = jnp.where(
                which < 2,
                jnp.where(which == 0, part[0:32], part[32:64]),
                jnp.where(which == 2, part[64:96], part[96:128]),
            )
            halves.append(jnp.concatenate([mine[0:16], mine[16:32]], axis=1))
            freqs.append(mine[12:13])
        vectors[...] = jnp.concatenate(halves, axis=0).astype(jnp.bfloat16)
        freqs_of[...] = jnp.concatenate(freqs, axis=0)

    def products(index, vectors, freqs_of, wide, near, scale):
        slot = live_s[index]
        raw = blocks[slot >> 1, slot & 1]
        modes = jnp.maximum(raw, 0)
        pairs = jnp.dot(spread[...], vectors[...], preferred_element_type=jnp.float32)
        third, fourth, e1, e2 = (pairs[144 * k : 144 * (k + 1)] for k in range(4))
        far_re = third[:, :LANES] * fourth[:, :LANES] - third[:, LANES:] * fourth[:, LANES:]
        far_im = -(third[:, :LANES] * fourth[:, LANES:] + third[:, LANES:] * fourth[:, :LANES])
        near[0:144] = e1[:, :LANES] * e2[:, :LANES] - e1[:, LANES:] * e2[:, LANES:]
        near[144:288] = e1[:, :LANES] * e2[:, LANES:] + e1[:, LANES:] * e2[:, :LANES]

        point = floor_div(modes, BR)
        coords = [(point >> 8).astype(jnp.float32), ((point >> 4) & 15).astype(jnp.float32), (point & 15).astype(jnp.float32)]
        shift = jnp.zeros((8, LANES), jnp.float32)
        for which in range(3):
            for axis in range(3):
                column = cell[:, 3 * which + axis : 3 * which + axis + 1]
                term = column * coords[axis][which + 1 : which + 2, :]
                shift = shift + term if which == 0 else shift - term
        step = shift.astype(jnp.int32) & 15
        cosine, sine = cosine_of(step), cosine_of((step - 4) & 15)
        for k in range(8):
            c, s = cosine[k : k + 1, :], sine[k : k + 1, :]
            wide[144 * k : 144 * (k + 1), :LANES] = (c * far_re - s * far_im).astype(jnp.bfloat16)
            wide[144 * k : 144 * (k + 1), LANES:] = (c * far_im + s * far_re).astype(jnp.bfloat16)

        freqs = [freqs_of[k : k + 1] for k in range(4)]
        occupied = [1.0 / (jnp.exp(f) - 1.0) for f in freqs]
        mismatch = freqs[0] + freqs[1] - freqs[2] - freqs[3]
        delta = jnp.exp(-((mismatch / SMEARING) ** 2)) / (SMEARING * math.sqrt(math.pi))
        weight = (1.0 + occupied[1]) * occupied[2] * occupied[3] / occupied[0]
        product = freqs[0] * freqs[1] * freqs[2] * freqs[3]
        valid = (raw[1:2, :] >= 0) & (index < total)
        scale[...] = jnp.where(valid, delta * weight / product, 0.0)

    def contract(wide, near, scale, term):
        weighted = jnp.dot(phi[...], wide[...], preferred_element_type=jnp.float32)
        w_re, w_im = weighted[:, :LANES], weighted[:, LANES:]
        near_re, near_im = near[0:144], near[144:288]
        value_re = jnp.sum(near_re * w_re - near_im * w_im, axis=0, keepdims=True)
        value_im = jnp.sum(near_re * w_im + near_im * w_re, axis=0, keepdims=True)
        term[...] = (value_re * value_re + value_im * value_im) * scale[...]

    def scatter(index, term):
        slot = live_s[index]
        first = jnp.maximum(blocks[slot >> 1, slot & 1][0:1, :], 0)
        high = floor_div(first, 192)
        low = first - 192 * high
        placed = jnp.where(lax.broadcasted_iota(jnp.int32, (NB, LANES), 0) == high, term, 0.0)
        one = placed.astype(jnp.bfloat16)
        rest = placed - one.astype(jnp.float32)
        two = rest.astype(jnp.bfloat16)
        three = (rest - two.astype(jnp.float32)).astype(jnp.bfloat16)
        spot = jnp.where(lax.broadcasted_iota(jnp.int32, (256, LANES), 0) == low, 1.0, 0.0).astype(jnp.bfloat16)
        sums[...] += lax.dot_general(
            jnp.concatenate([one, two, three], axis=0), spot, NT, preferred_element_type=jnp.float32
        )

    sides = (
        (rows_a, held_a, vectors_a, freqs_a, scale_a, wide_a, near_a, term_a, 0),
        (rows_b, held_b, vectors_b, freqs_b, scale_b, wide_b, near_b, term_b, 1),
    )

    def step_of(i, side):
        at, held, vectors, freqs_of, scale, wide, near, term, which = sides[side]
        _, _, next_vectors, next_freqs, next_scale, next_wide, next_near, last_term, _ = sides[1 - side]
        fetch(i + 2, at, which).wait()
        scatter(jnp.maximum(i - 1, 0), last_term[...])
        contract(wide, near, scale, term)
        products(i + 1, next_vectors, next_freqs, next_wide, next_near, next_scale)
        vectors_of(at, i + 2, held, vectors, freqs_of)
        fetch(i + 4, at, which).start()

    term_b[...] = jnp.zeros_like(term_b)
    fetch(1, rows_b, 1).start()
    first_rows.wait()
    vectors_of(rows_a, 0, held_a, vectors_a, freqs_a)
    fetch(2, rows_a, 0).start()
    fetch(1, rows_b, 1).wait()
    products(0, vectors_a, freqs_a, wide_a, near_a, scale_a)
    vectors_of(rows_b, 1, held_b, vectors_b, freqs_b)
    fetch(3, rows_b, 1).start()

    def two_blocks(it, carry):
        step_of(2 * it, 0)

        @pl.when(2 * it + 1 < total)
        def _():
            step_of(2 * it + 1, 1)

        return carry

    lax.fori_loop(0, (total + 1) // 2, two_blocks, 0)
    scatter(total - 1, jnp.where(total % 2 == 1, term_a[...], term_b[...]))
    fetch(0, rows_a, 0).wait()
    fetch(0, rows_b, 1).wait()
    result = sums[0:16] + sums[16:32] + sums[32:48]
    for w in range(NB):
        out[w] = result[w : w + 1]


def quartet_sums(*operands):
    vmem = pl.BlockSpec(memory_space=pltpu.VMEM)
    pinned = [pltpu.with_memory_space_constraint(a, pltpu.VMEM) for a in operands]
    return pl.pallas_call(
        quartet_kernel,
        out_shape=pltpu.VMEM((NB, 1, 256), jnp.float32),
        in_specs=[vmem] * 8,
        out_specs=vmem,
        scratch_shapes=[
            pltpu.VMEM((1152, 256), jnp.bfloat16),
            pltpu.VMEM((1152, 256), jnp.bfloat16),
            pltpu.VMEM((288, LANES), jnp.float32),
            pltpu.VMEM((288, LANES), jnp.float32),
            pltpu.VMEM((1, LANES), jnp.float32),
            pltpu.VMEM((1, LANES), jnp.float32),
            pltpu.VMEM((1, LANES), jnp.float32),
            pltpu.VMEM((1, LANES), jnp.float32),
            pltpu.VMEM((4, LANES), jnp.float32),
            pltpu.VMEM((4, LANES), jnp.float32),
            pltpu.VMEM((64, 256), jnp.bfloat16),
            pltpu.VMEM((64, 256), jnp.bfloat16),
            pltpu.VMEM((4 * LANES, LANES), jnp.bfloat16),
            pltpu.VMEM((4 * LANES, LANES), jnp.bfloat16),
            pltpu.SMEM((4, LANES), jnp.int32),
            pltpu.SMEM((4, LANES), jnp.int32),
            pltpu.SMEM((NB, 1, LANES), jnp.int32),
            pltpu.SMEM((2 * NB + 8,), jnp.int32),
            pltpu.VMEM((48, 256), jnp.float32),
            pltpu.SemaphoreType.DMA((3,)),
        ],
        compiler_params=pltpu.CompilerParams(
            vmem_limit_bytes=16 << 20
        ),
        name="quartets",
    )(*pinned)


def reduce_kernel(part, out, arrived, send, recv):
    pb, wa = lax.axis_index("pb"), lax.axis_index("wa")
    barrier = pltpu.get_barrier_semaphore()
    peers = [lax.rem(wa + k, NB) for k in range(1, NB)]
    for peer in peers:
        pl.semaphore_signal(barrier, inc=1, device_id=(pb, peer), device_id_type=MESH)
    pl.semaphore_wait(barrier, NB - 1)
    for k, peer in enumerate(peers):
        pltpu.make_async_remote_copy(
            src_ref=part.at[peer], dst_ref=arrived.at[k], send_sem=send.at[0], recv_sem=recv.at[0],
            device_id=(pb, peer), device_id_type=MESH,
        ).start()
    everything = pltpu.make_async_remote_copy(
        src_ref=part.at[pl.ds(0, NB - 1)], dst_ref=arrived, send_sem=send.at[0], recv_sem=recv.at[0],
        device_id=(pb, peers[0]), device_id_type=MESH,
    )
    everything.wait_recv()
    total = part[wa]
    for k in range(NB - 1):
        total = total + arrived[k]
    out[...] = total
    everything.wait_send()


def reduce_over_wa(part):
    vmem = pl.BlockSpec(memory_space=pltpu.VMEM)
    return pl.pallas_call(
        reduce_kernel,
        out_shape=jax.ShapeDtypeStruct((1, 256), jnp.float32),
        in_specs=[vmem],
        out_specs=vmem,
        scratch_shapes=[
            pltpu.VMEM((NB - 1, 1, 256), jnp.float32),
            pltpu.SemaphoreType.DMA((1,)),
            pltpu.SemaphoreType.DMA((1,)),
        ],
        compiler_params=pltpu.CompilerParams(collective_id=1, has_side_effects=True, vmem_limit_bytes=1 << 20),
        name="reduce_wa",
    )(pltpu.with_memory_space_constraint(part, pltpu.VMEM))


def body(quartets, counts, eig, freq, phi, cells):
    dealt = quartets.reshape(2, NB, 4, LANES)
    held = exchange(eig, freq.reshape(24, LANES), dealt, phi, cells, counts)
    part = quartet_sums(*held)
    return reduce_over_wa(part)[0, :192]


def solution(mesh):
    placed = (P(("pb", "wa"), None, None), P(("pb", "wa")), P(None, "pb"), P("pb"), P(), P())
    return jax.shard_map(body, mesh=mesh, in_specs=placed, out_specs=P(("pb", "wa")), check_vma=False)
```

```python
import functools
import math

import jax
import jax.numpy as jnp
from jax import lax
from jax.experimental import pallas as pl
from jax.experimental.pallas import tpu as pltpu
from jax.sharding import PartitionSpec as P

QMESH = 16
BR = 12
NB = 16
LOCAL = 3072
GROUP = 768
LANES = 128
GROUP_AT = (0, 768, 1664, 2432)
FREQ_AT = 1536
WIDTH = 3200
SMEARING = 0.5
MESH = pl.DeviceIdType.MESH
NT = (((1,), (1,)), ((), ()))


PIECES = {(1, 0): (0, 768), (1, 1): (768, 896), (-1, 1): (1664, 768), (-1, 0): (2432, 768)}
RELAY_CORE = 1
ORDER = (
    (-1, 0), (1, 0), (0, -1), (0, 1), (2, 0), (-1, -1), (-1, 1), (0, 2), (1, -1), (1, 1), (-1, 2), (2, -1), (2, 1), (1, 2), (2, 2),
)
WAVES = (
    ((-1, 0), (1, 0), (0, -1), (0, 1)),
    ((2, 0), (0, 2)),
    ((-1, 1), (1, -1)),
    ((-1, -1), (1, 1)),
    ((-1, 2), (2, -1), (2, 1), (1, 2)),
    ((2, 2),),
)
WAVE_AFTER = {5: (0,), 9: (1,), 10: (2,), 12: (3,), 14: (4, 5)}


def wrapped(offset):
    return (offset + 1) % 4 - 1


def hit(rows, columns, where):
    r = lax.broadcasted_iota(jnp.int32, (rows, columns), 0)
    c = lax.broadcasted_iota(jnp.int32, (rows, columns), 1)
    return jnp.where(where(r) == c, 1.0, 0.0).astype(jnp.bfloat16)


def spread_column(r):
    kind = floor_div(r, 144)
    t = r - 144 * kind
    first = floor_div(t, BR)
    return ((kind + 2) & 3) * 16 + jnp.where((kind & 1) == 0, first, t - BR * first)


def order_column(r):
    t = r & 31
    lane = jnp.where(t < 12, t, jnp.where(t == 12, 24, jnp.where((t >= 16) & (t < 28), t - 4, -999)))
    return lane + (r - t)


def exchange_kernel(
    eig, freq, quartets, phi, cells, counts,
    table, packed, lengths, phi_v, cells_v, reorder, spread,
    blocks, tallies, lengths_v, tab, mine, eye, dealt, send, got, lent, local,
):
    pb, wa = lax.axis_index("pb"), lax.axis_index("wa")
    x, y, core = pb // 4, pb % 4, wa % 2
    relays = core == RELAY_CORE
    sibling = (pb, wa + 1 - 2 * core)

    def place(dx, dy):
        return lax.rem(x + dx + 4, 4) * 4 + lax.rem(y + dy + 4, 4)

    barrier = pltpu.get_barrier_semaphore()

    @pl.when(relays)
    def _():
        for step in (1, -1):
            pl.semaphore_signal(barrier, inc=1, device_id=(place(step, 0), wa), device_id_type=MESH)
            pl.semaphore_signal(barrier, inc=1, device_id=(place(0, step), wa), device_id_type=MESH)

    for k in range(1, NB):
        pl.semaphore_signal(barrier, inc=1, device_id=(pb, lax.rem(wa + k, NB)), device_id_type=MESH)

    left = pltpu.make_async_copy(eig.at[:, pl.ds(0, 1536)], tab.at[pb, :, pl.ds(0, 1536)], local.at[0])
    right = pltpu.make_async_copy(eig.at[:, pl.ds(1536, 1536)], tab.at[pb, :, pl.ds(1664, 1536)], local.at[1])
    copy_freq = pltpu.make_async_copy(freq, tab.at[pb, :, pl.ds(FREQ_AT, LANES)], local.at[2])
    copy_dealt = pltpu.make_async_copy(quartets, dealt, local.at[3])
    copy_phi = pltpu.make_async_copy(phi, phi_v, local.at[4])
    copy_cells = pltpu.make_async_copy(cells, cells_v, local.at[5])
    own = (left, right, copy_freq, copy_dealt)
    for copy in own + (copy_phi, copy_cells):
        copy.start()
    mine[...] = jnp.full((1, LANES), counts[0], jnp.int32)
    tallies[wa] = mine[...]
    eye[...] = hit(256, 256, lambda r: r)
    reorder[...] = hit(LANES, LANES, order_column)
    spread[...] = hit(576, 64, spread_column)
    for copy in own:
        copy.wait()
    blocks[wa] = dealt[:, 0]

    pl.semaphore_wait(barrier, NB - 1 + jnp.where(relays, 4, 0))

    def push(src, dst, sent, arrival, device):
        pltpu.make_async_remote_copy(
            src_ref=src, dst_ref=dst, send_sem=send.at[sent], recv_sem=arrival, device_id=device, device_id_type=MESH
        ).start()

    def bytes_in(view, sem):
        pltpu.make_async_remote_copy(
            src_ref=view, dst_ref=view, send_sem=send.at[0], recv_sem=sem, device_id=sibling, device_id_type=MESH
        ).wait_recv()

    def bytes_out(view, sent):
        pltpu.make_async_remote_copy(
            src_ref=view, dst_ref=view, send_sem=send.at[sent], recv_sem=got.at[0], device_id=sibling, device_id_type=MESH
        ).wait_send()

    def at(way, part, first, second):
        return place(way * first, way * second) if part == 0 else place(way * second, way * first)

    def relay(way, part, first, second, axis, step):
        start, width = PIECES[way, part]
        view = tab.at[at(way, part, first, second), :, pl.ds(start, width)]
        key = (wrapped(first - step), second) if axis == 0 else (first, wrapped(second - step))
        target = at(way, part, step, 0) if axis == 0 else at(way, part, 0, step)
        push(view, view, 0, got.at[ORDER.index(key)], (target, wa))

    def lend(way, part, first, second):
        start, width = PIECES[way, part]
        view = tab.at[at(way, part, first, second), :, pl.ds(start, width)]
        offset = (way * first, way * second) if part == 0 else (way * second, way * first)
        offset = tuple(wrapped(o) for o in offset)
        wave = [w for w, members in enumerate(WAVES) if offset in members][0]
        push(view, view, 1, lent.at[wave], sibling)

    def turn(shard):
        values = tab[shard, :, FREQ_AT : FREQ_AT + LANES].astype(jnp.float32)
        for j in range(3):
            stack = []
            for g in range(4):
                stack.append(tab[shard, :, GROUP_AT[g] + 256 * j : GROUP_AT[g] + 256 * (j + 1)].astype(jnp.float32))
                at_row = 6 * g + 2 * j
                stack.append(
                    jnp.concatenate(
                        [jnp.broadcast_to(values[at_row + h : at_row + h + 1, :], (8, LANES)) for h in range(2)], axis=1
                    )
                )
            stack = jnp.concatenate(stack, axis=0).astype(jnp.bfloat16)
            table[pl.ds(pl.multiple_of(shard * GROUP + 256 * j, 256), 256), :] = lax.dot_general(
                eye[...], stack, NT, preferred_element_type=jnp.float32
            )

    @pl.when(relays)
    def _():
        for axis in (0, 1):
            for way in (1, -1):
                for part in (0, 1):
                    relay(way, part, 0, 0, axis, 1)
                    relay(way, part, 0, 0, axis, -1)

    for k in range(1, NB):
        peer = lax.rem(wa + k, NB)
        push(dealt.at[:, k], blocks.at[wa], 2, lent.at[len(WAVES)], (pb, peer))
        push(mine, tallies.at[wa], 3, lent.at[len(WAVES) + 1], (pb, peer))
    turn(pb)

    def blocks_in():
        bytes_in(blocks.at[pl.ds(0, NB - 1)], lent.at[len(WAVES)])
        bytes_in(tallies.at[pl.ds(0, NB - 1)], lent.at[len(WAVES) + 1])
        held = blocks[...]
        modes = jnp.maximum(held, 0)
        local_mode = lax.broadcasted_iota(jnp.int32, modes.shape, 2) == 0
        packed[:, :, 0:4] = held
        packed[:, :, 4:8] = rows_of(modes + jnp.where(local_mode, pb * LOCAL, 0))
        lane = lax.broadcasted_iota(jnp.int32, (NB, 1, LANES), 2)
        source = lax.broadcasted_iota(jnp.int32, (NB, 1, LANES), 0)
        length = jnp.zeros((NB, 1, LANES), jnp.int32)
        for high in range(2):
            last = jnp.max(jnp.where(held[:, high, 1:2] >= 0, lane + 1, 0), axis=2, keepdims=True)
            used = ((wa - source) & (NB - 1)) + NB * high < tallies[...]
            length = jnp.where((lane == high) & used, last, length)
        lengths_v[...] = length

    @pl.when(relays)
    def _():
        for number, (first, second) in enumerate(ORDER):
            bytes_in(tab.at[0], got.at[number])
            for way in (1, -1):
                for part in (0, 1):
                    if second == 0:
                        if first == -1:
                            relay(way, part, first, 0, 0, 1)
                        relay(way, part, first, 0, 1, 1)
                        relay(way, part, first, 0, 1, -1)
                    elif second == -1:
                        relay(way, part, first, second, 1, 1)
                    lend(way, part, first, second)
            if number == 7:
                blocks_in()
            for wave in WAVE_AFTER.get(number, ()):
                for offset in WAVES[wave]:
                    turn(place(*offset))
        bytes_out(tab.at[pl.ds(0, 15)], 0)
        bytes_out(tab.at[pl.ds(0, 15)], 1)

    @pl.when(jnp.logical_not(relays))
    def _():
        for wave, members in enumerate(WAVES):
            if wave == 1:
                blocks_in()
            bytes_in(tab.at[pl.ds(0, len(members))], lent.at[wave])
            for offset in members:
                turn(place(*offset))

    copy_lengths = pltpu.make_async_copy(lengths_v, lengths, local.at[0])
    copy_lengths.start()
    copy_phi.wait()
    copy_cells.wait()
    copy_lengths.wait()
    bytes_out(blocks.at[pl.ds(0, NB - 1)], 2)
    bytes_out(tallies.at[pl.ds(0, NB - 1)], 3)


def exchange(eig, freq, quartets, phi, cells, counts):
    hbm = pl.BlockSpec(memory_space=pltpu.HBM)
    vmem = pl.BlockSpec(memory_space=pltpu.VMEM)
    return pl.pallas_call(
        exchange_kernel,
        out_shape=(
            pltpu.VMEM((NB * GROUP, LANES), jnp.float32),
            pltpu.VMEM((NB, 2, 8, LANES), jnp.int32),
            pltpu.SMEM((NB, 1, LANES), jnp.int32),
            pltpu.VMEM((144, 1152), jnp.bfloat16),
            pltpu.VMEM((8, 9), jnp.int32),
            pltpu.VMEM((128, 128), jnp.bfloat16),
            pltpu.VMEM((576, 64), jnp.bfloat16),
        ),
        in_specs=[hbm] * 5 + [pl.BlockSpec(memory_space=pltpu.SMEM)],
        out_specs=(vmem, vmem, pl.BlockSpec(memory_space=pltpu.SMEM), vmem, vmem, vmem, vmem),
        scratch_shapes=[
            pltpu.VMEM((NB, 2, 4, LANES), jnp.int32),
            pltpu.VMEM((NB, 1, LANES), jnp.int32),
            pltpu.VMEM((NB, 1, LANES), jnp.int32),
            pltpu.VMEM((NB, 24, WIDTH), jnp.bfloat16),
            pltpu.VMEM((1, LANES), jnp.int32),
            pltpu.VMEM((256, 256), jnp.bfloat16),
            pltpu.VMEM((2, NB, 4, LANES), jnp.int32),
            pltpu.SemaphoreType.DMA((4,)),
            pltpu.SemaphoreType.DMA((len(ORDER),)),
            pltpu.SemaphoreType.DMA((len(WAVES) + 2,)),
            pltpu.SemaphoreType.DMA((6,)),
        ],
        compiler_params=pltpu.CompilerParams(collective_id=0, has_side_effects=True, vmem_limit_bytes=24 << 20),
        name="exchange",
    )(*[pltpu.with_memory_space_constraint(a, pltpu.HBM) for a in (eig, freq, quartets, phi, cells)], counts)


def cosine_of(step):
    near = jnp.minimum(step, 16 - step)
    out = jnp.full(step.shape, -1.0, jnp.float32)
    for k in range(8):
        out = jnp.where(near == k, math.cos(math.pi * k / 8) if k != 4 else 0.0, out)
    return out


def floor_div(value, by):
    return jnp.floor((value.astype(jnp.float32) + 0.5) * (1.0 / by)).astype(jnp.int32)


def rows_of(modes):
    unit = floor_div(modes, GROUP)
    return (unit >> 2) * GROUP + modes - unit * GROUP


def quartet_kernel(
    table, packed, lengths, phi, cells, reorder, spread, out,
    wide_a, wide_b, near_a, near_b, scale_a, scale_b, term_a, term_b, freqs_a, freqs_b, vectors_a, vectors_b, held_a, held_b,
    rows_a, rows_b, dense, sums, sem,
):
    pb, wa = lax.axis_index("pb"), lax.axis_index("wa")

    lane8 = lax.broadcasted_iota(jnp.int32, (8, LANES), 1)
    count = jnp.int32(0)
    current = jnp.zeros((8, LANES), jnp.int32)
    for held in range(NB):
        source = (wa - held) & (NB - 1)
        for high in range(2):
            length = lengths[source, 0, high]
            offset = count & (LANES - 1)
            rolled = pltpu.roll(packed[source, high], offset, 1)
            current = jnp.where(lane8 >= offset, rolled, current)
            dense[count >> 7] = current
            current = jnp.where(offset + length >= LANES, rolled, current)
            count = count + length
    total = (count + LANES - 1) >> 7
    dense[count >> 7] = current
    for k in range(6):
        dense[total + k] = jnp.zeros((8, LANES), jnp.int32)

    sums[...] = jnp.zeros_like(sums)
    cell = cells[...].astype(jnp.float32)

    def fetch(index, into, which):
        return pltpu.make_async_copy(dense.at[index, pl.ds(4, 4)], into, sem.at[which])

    sublane = lax.broadcasted_iota(jnp.int32, (8, LANES), 0)
    odd = [(sublane & (1 << bit)) != 0 for bit in range(3)]

    def gather(into, at):
        for k in range(4):
            for n in range(0, LANES, 16):
                pair = []
                for half in (n, n + 8):
                    level = [table[pl.ds(at[k, half + j], 8, stride=0), :] for j in range(8)]
                    for bit in range(3):
                        level = [jnp.where(odd[bit], high, low) for low, high in zip(level[::2], level[1::2])]
                    pair.append(level[0])
                into[LANES * k + n : LANES * k + n + 16, :] = jnp.concatenate(pair, axis=0).astype(jnp.bfloat16)

    def vectors_of(at, index, held, vectors, freqs_of):
        gather(held, at)
        raw = dense[index][0:4]
        modes = jnp.maximum(raw, 0)
        fullmode = modes + jnp.where(lax.broadcasted_iota(jnp.int32, modes.shape, 0) == 0, pb * LOCAL, 0)
        group = floor_div(fullmode, GROUP) & 3
        turned = lax.dot_general(reorder[...], held[...], NT, preferred_element_type=jnp.float32)
        halves, freqs = [], []
        for k in range(4):
            which = group[k : k + 1, :]
            part = turned[:, LANES * k : LANES * (k + 1)]
            mine = jnp.where(
                which < 2,
                jnp.where(which == 0, part[0:32], part[32:64]),
                jnp.where(which == 2, part[64:96], part[96:128]),
            )
            halves.append(jnp.concatenate([mine[0:16], mine[16:32]], axis=1))
            freqs.append(mine[12:13])
        vectors[...] = jnp.concatenate(halves, axis=0).astype(jnp.bfloat16)
        freqs_of[...] = jnp.concatenate(freqs, axis=0)

    def products(index, vectors, freqs_of, wide, near, scale):
        raw = dense[index][0:4]
        modes = jnp.maximum(raw, 0)
        pairs = jnp.dot(spread[...], vectors[...], preferred_element_type=jnp.float32)
        third, fourth, e1, e2 = (pairs[144 * k : 144 * (k + 1)] for k in range(4))
        far_re = third[:, :LANES] * fourth[:, :LANES] - third[:, LANES:] * fourth[:, LANES:]
        far_im = -(third[:, :LANES] * fourth[:, LANES:] + third[:, LANES:] * fourth[:, :LANES])
        near[0:144] = e1[:, :LANES] * e2[:, :LANES] - e1[:, LANES:] * e2[:, LANES:]
        near[144:288] = e1[:, :LANES] * e2[:, LANES:] + e1[:, LANES:] * e2[:, :LANES]

        point = floor_div(modes, BR)
        coords = [(point >> 8).astype(jnp.float32), ((point >> 4) & 15).astype(jnp.float32), (point & 15).astype(jnp.float32)]
        shift = jnp.zeros((8, LANES), jnp.float32)
        for which in range(3):
            for axis in range(3):
                column = cell[:, 3 * which + axis : 3 * which + axis + 1]
                term = column * coords[axis][which + 1 : which + 2, :]
                shift = shift + term if which == 0 else shift - term
        step = shift.astype(jnp.int32) & 15
        cosine, sine = cosine_of(step), cosine_of((step - 4) & 15)
        for k in range(8):
            c, s = cosine[k : k + 1, :], sine[k : k + 1, :]
            wide[144 * k : 144 * (k + 1), :LANES] = (c * far_re - s * far_im).astype(jnp.bfloat16)
            wide[144 * k : 144 * (k + 1), LANES:] = (c * far_im + s * far_re).astype(jnp.bfloat16)

        freqs = [freqs_of[k : k + 1] for k in range(4)]
        occupied = [1.0 / (jnp.exp(f) - 1.0) for f in freqs]
        mismatch = freqs[0] + freqs[1] - freqs[2] - freqs[3]
        delta = jnp.exp(-((mismatch / SMEARING) ** 2)) / (SMEARING * math.sqrt(math.pi))
        weight = (1.0 + occupied[1]) * occupied[2] * occupied[3] / occupied[0]
        product = freqs[0] * freqs[1] * freqs[2] * freqs[3]
        number = LANES * index + lax.broadcasted_iota(jnp.int32, (1, LANES), 1)
        valid = (raw[1:2, :] >= 0) & (number < count)
        scale[...] = jnp.where(valid, delta * weight / product, 0.0)

    def contract(wide, near, scale, term):
        weighted = jnp.dot(phi[...], wide[...], preferred_element_type=jnp.float32)
        w_re, w_im = weighted[:, :LANES], weighted[:, LANES:]
        near_re, near_im = near[0:144], near[144:288]
        value_re = jnp.sum(near_re * w_re - near_im * w_im, axis=0, keepdims=True)
        value_im = jnp.sum(near_re * w_im + near_im * w_re, axis=0, keepdims=True)
        term[...] = (value_re * value_re + value_im * value_im) * scale[...]

    def scatter(index, term):
        first = jnp.maximum(dense[index][0:1, :], 0)
        high = floor_div(first, 192)
        low = first - 192 * high
        placed = jnp.where(lax.broadcasted_iota(jnp.int32, (NB, LANES), 0) == high, term, 0.0)
        one = placed.astype(jnp.bfloat16)
        rest = placed - one.astype(jnp.float32)
        two = rest.astype(jnp.bfloat16)
        three = (rest - two.astype(jnp.float32)).astype(jnp.bfloat16)
        spot = jnp.where(lax.broadcasted_iota(jnp.int32, (256, LANES), 0) == low, 1.0, 0.0).astype(jnp.bfloat16)
        sums[...] += lax.dot_general(
            jnp.concatenate([one, two, three], axis=0), spot, NT, preferred_element_type=jnp.float32
        )

    sides = (
        (rows_a, held_a, vectors_a, freqs_a, scale_a, wide_a, near_a, term_a, 0),
        (rows_b, held_b, vectors_b, freqs_b, scale_b, wide_b, near_b, term_b, 1),
    )

    def step_of(i, side):
        at, held, vectors, freqs_of, scale, wide, near, term, which = sides[side]
        _, _, next_vectors, next_freqs, next_scale, next_wide, next_near, last_term, _ = sides[1 - side]
        fetch(i + 2, at, which).wait()
        scatter(jnp.maximum(i - 1, 0), last_term[...])
        contract(wide, near, scale, term)
        products(i + 1, next_vectors, next_freqs, next_wide, next_near, next_scale)
        vectors_of(at, i + 2, held, vectors, freqs_of)
        fetch(i + 4, at, which).start()

    term_b[...] = jnp.zeros_like(term_b)
    fetch(0, rows_a, 0).start()
    fetch(1, rows_b, 1).start()
    fetch(0, rows_a, 0).wait()
    vectors_of(rows_a, 0, held_a, vectors_a, freqs_a)
    fetch(2, rows_a, 0).start()
    fetch(1, rows_b, 1).wait()
    products(0, vectors_a, freqs_a, wide_a, near_a, scale_a)
    vectors_of(rows_b, 1, held_b, vectors_b, freqs_b)
    fetch(3, rows_b, 1).start()

    def two_blocks(it, carry):
        step_of(2 * it, 0)

        @pl.when(2 * it + 1 < total)
        def _():
            step_of(2 * it + 1, 1)

        return carry

    lax.fori_loop(0, (total + 1) // 2, two_blocks, 0)
    scatter(jnp.maximum(total - 1, 0), jnp.where(total % 2 == 1, term_a[...], term_b[...]))
    fetch(0, rows_a, 0).wait()
    fetch(0, rows_b, 1).wait()
    result = sums[0:16] + sums[16:32] + sums[32:48]
    for w in range(NB):
        out[w] = result[w : w + 1]


def quartet_sums(*operands):
    vmem = pl.BlockSpec(memory_space=pltpu.VMEM)
    smem = pl.BlockSpec(memory_space=pltpu.SMEM)
    pinned = [pltpu.with_memory_space_constraint(a, pltpu.SMEM if k == 2 else pltpu.VMEM) for k, a in enumerate(operands)]
    return pl.pallas_call(
        quartet_kernel,
        out_shape=pltpu.VMEM((NB, 1, 256), jnp.float32),
        in_specs=[vmem, vmem, smem, vmem, vmem, vmem, vmem],
        out_specs=vmem,
        scratch_shapes=[
            pltpu.VMEM((1152, 256), jnp.bfloat16),
            pltpu.VMEM((1152, 256), jnp.bfloat16),
            pltpu.VMEM((288, LANES), jnp.float32),
            pltpu.VMEM((288, LANES), jnp.float32),
            pltpu.VMEM((1, LANES), jnp.float32),
            pltpu.VMEM((1, LANES), jnp.float32),
            pltpu.VMEM((1, LANES), jnp.float32),
            pltpu.VMEM((1, LANES), jnp.float32),
            pltpu.VMEM((4, LANES), jnp.float32),
            pltpu.VMEM((4, LANES), jnp.float32),
            pltpu.VMEM((64, 256), jnp.bfloat16),
            pltpu.VMEM((64, 256), jnp.bfloat16),
            pltpu.VMEM((4 * LANES, LANES), jnp.bfloat16),
            pltpu.VMEM((4 * LANES, LANES), jnp.bfloat16),
            pltpu.SMEM((4, LANES), jnp.int32),
            pltpu.SMEM((4, LANES), jnp.int32),
            pltpu.VMEM((2 * NB + 8, 8, LANES), jnp.int32),
            pltpu.VMEM((48, 256), jnp.float32),
            pltpu.SemaphoreType.DMA((2,)),
        ],
        compiler_params=pltpu.CompilerParams(
            vmem_limit_bytes=16 << 20
        ),
        name="quartets",
    )(*pinned)


def reduce_kernel(part, out, arrived, send, recv):
    pb, wa = lax.axis_index("pb"), lax.axis_index("wa")
    barrier = pltpu.get_barrier_semaphore()
    peers = [lax.rem(wa + k, NB) for k in range(1, NB)]
    for peer in peers:
        pl.semaphore_signal(barrier, inc=1, device_id=(pb, peer), device_id_type=MESH)
    pl.semaphore_wait(barrier, NB - 1)
    for k, peer in enumerate(peers):
        pltpu.make_async_remote_copy(
            src_ref=part.at[peer], dst_ref=arrived.at[k], send_sem=send.at[0], recv_sem=recv.at[0],
            device_id=(pb, peer), device_id_type=MESH,
        ).start()
    everything = pltpu.make_async_remote_copy(
        src_ref=part.at[pl.ds(0, NB - 1)], dst_ref=arrived, send_sem=send.at[0], recv_sem=recv.at[0],
        device_id=(pb, peers[0]), device_id_type=MESH,
    )
    everything.wait_recv()
    total = part[wa]
    for k in range(NB - 1):
        total = total + arrived[k]
    out[...] = total
    everything.wait_send()


def reduce_over_wa(part):
    vmem = pl.BlockSpec(memory_space=pltpu.VMEM)
    return pl.pallas_call(
        reduce_kernel,
        out_shape=jax.ShapeDtypeStruct((1, 256), jnp.float32),
        in_specs=[vmem],
        out_specs=vmem,
        scratch_shapes=[
            pltpu.VMEM((NB - 1, 1, 256), jnp.float32),
            pltpu.SemaphoreType.DMA((1,)),
            pltpu.SemaphoreType.DMA((1,)),
        ],
        compiler_params=pltpu.CompilerParams(collective_id=1, has_side_effects=True, vmem_limit_bytes=1 << 20),
        name="reduce_wa",
    )(pltpu.with_memory_space_constraint(part, pltpu.VMEM))


def body(quartets, counts, eig, freq, phi, cells):
    dealt = quartets.reshape(2, NB, 4, LANES)
    held = exchange(eig, freq.reshape(24, LANES), dealt, phi, cells, counts)
    part = quartet_sums(*held)
    return reduce_over_wa(part)[0, :192]


def solution(mesh):
    placed = (P(("pb", "wa"), None, None), P(("pb", "wa")), P(None, "pb"), P("pb"), P(), P())
    return jax.shard_map(body, mesh=mesh, in_specs=placed, out_specs=P(("pb", "wa")), check_vma=False)
```

```python
import functools
import math

import jax
import jax.numpy as jnp
from jax import lax
from jax.experimental import pallas as pl
from jax.experimental.pallas import tpu as pltpu
from jax.sharding import PartitionSpec as P

QMESH = 16
BR = 12
NB = 16
LOCAL = 3072
GROUP = 768
LANES = 128
GROUP_AT = (0, 768, 1664, 2432)
FREQ_AT = 1536
WIDTH = 3200
SMEARING = 0.5
MESH = pl.DeviceIdType.MESH
NT = (((1,), (1,)), ((), ()))


PIECES = {(1, 0): (0, 768), (1, 1): (768, 896), (-1, 1): (1664, 768), (-1, 0): (2432, 768)}
RELAY_CORE = 1
CHIPS = 8
ORDER = (
    (-1, 0), (1, 0), (0, -1), (0, 1), (2, 0), (-1, -1), (-1, 1), (0, 2), (1, -1), (1, 1), (-1, 2), (2, -1), (2, 1), (1, 2), (2, 2),
)
WAVES = (
    ((-1, 0), (1, 0), (0, -1), (0, 1)),
    ((2, 0), (0, 2)),
    ((-1, 1), (1, -1)),
    ((-1, -1), (1, 1)),
    ((-1, 2), (2, -1), (2, 1), (1, 2)),
    ((2, 2),),
)
WAVE_AFTER = {5: (0,), 9: (1,), 10: (2,), 12: (3,), 14: (4, 5)}


def wrapped(offset):
    return (offset + 1) % 4 - 1


def hit(rows, columns, where):
    r = lax.broadcasted_iota(jnp.int32, (rows, columns), 0)
    c = lax.broadcasted_iota(jnp.int32, (rows, columns), 1)
    return jnp.where(where(r) == c, 1.0, 0.0).astype(jnp.bfloat16)


def spread_column(r):
    kind = floor_div(r, 144)
    t = r - 144 * kind
    first = floor_div(t, BR)
    return ((kind + 2) & 3) * 16 + jnp.where((kind & 1) == 0, first, t - BR * first)


def order_column(r):
    t = r & 31
    lane = jnp.where(t < 12, t, jnp.where(t == 12, 24, jnp.where((t >= 16) & (t < 28), t - 4, -999)))
    return lane + (r - t)


def exchange_kernel(
    eig, freq, quartets, phi, cells, counts,
    table, packed, lengths, phi_v, cells_v, reorder, spread,
    blocks, tallies, lengths_v, tab, mine, eye, dealt, send, got, lent, dealt_sem, local,
):
    pb, wa = lax.axis_index("pb"), lax.axis_index("wa")
    x, y, z, core = pb // 4, pb % 4, wa // 2, wa % 2
    relays = core == RELAY_CORE
    sibling = (pb, wa + 1 - 2 * core)
    dealers = [(pb, 2 * lax.rem(z + k, CHIPS)) for k in range(1, CHIPS)]

    def place(dx, dy):
        return lax.rem(x + dx + 4, 4) * 4 + lax.rem(y + dy + 4, 4)

    barrier = pltpu.get_barrier_semaphore()
    pl.semaphore_signal(barrier, inc=1, device_id=sibling, device_id_type=MESH)

    @pl.when(relays)
    def _():
        for step in (1, -1):
            pl.semaphore_signal(barrier, inc=1, device_id=(place(step, 0), wa), device_id_type=MESH)
            pl.semaphore_signal(barrier, inc=1, device_id=(place(0, step), wa), device_id_type=MESH)

    @pl.when(jnp.logical_not(relays))
    def _():
        for dealer in dealers:
            pl.semaphore_signal(barrier, inc=1, device_id=dealer, device_id_type=MESH)

    left = pltpu.make_async_copy(eig.at[:, pl.ds(0, 1536)], tab.at[pb, :, pl.ds(0, 1536)], local.at[0])
    right = pltpu.make_async_copy(eig.at[:, pl.ds(1536, 1536)], tab.at[pb, :, pl.ds(1664, 1536)], local.at[1])
    copy_freq = pltpu.make_async_copy(freq, tab.at[pb, :, pl.ds(FREQ_AT, LANES)], local.at[2])
    copy_dealt = pltpu.make_async_copy(quartets, dealt.at[core], local.at[3])
    copy_phi = pltpu.make_async_copy(phi, phi_v, local.at[4])
    copy_cells = pltpu.make_async_copy(cells, cells_v, local.at[5])
    first_copies = (left, right, copy_freq, copy_dealt)
    for copy in first_copies + (copy_phi, copy_cells):
        copy.start()
    mine[core] = jnp.full((1, LANES), counts[0], jnp.int32)
    eye[...] = hit(256, 256, lambda r: r)
    reorder[...] = hit(LANES, LANES, order_column)
    spread[...] = hit(576, 64, spread_column)
    for copy in first_copies:
        copy.wait()

    pl.semaphore_wait(barrier, jnp.where(relays, 5, CHIPS))

    def push(src, dst, sent, arrival, device):
        pltpu.make_async_remote_copy(
            src_ref=src, dst_ref=dst, send_sem=send.at[sent], recv_sem=arrival, device_id=device, device_id_type=MESH
        ).start()

    def bytes_in(view, sem):
        pltpu.make_async_remote_copy(
            src_ref=view, dst_ref=view, send_sem=send.at[0], recv_sem=sem, device_id=sibling, device_id_type=MESH
        ).wait_recv()

    def bytes_out(view, sent):
        pltpu.make_async_remote_copy(
            src_ref=view, dst_ref=view, send_sem=send.at[sent], recv_sem=got.at[0], device_id=sibling, device_id_type=MESH
        ).wait_send()

    def at(way, part, first, second):
        return place(way * first, way * second) if part == 0 else place(way * second, way * first)

    def relay(way, part, first, second, axis, step):
        start, width = PIECES[way, part]
        view = tab.at[at(way, part, first, second), :, pl.ds(start, width)]
        key = (wrapped(first - step), second) if axis == 0 else (first, wrapped(second - step))
        target = at(way, part, step, 0) if axis == 0 else at(way, part, 0, step)
        push(view, view, 0, got.at[ORDER.index(key)], (target, wa))

    def lend(way, part, first, second):
        start, width = PIECES[way, part]
        view = tab.at[at(way, part, first, second), :, pl.ds(start, width)]
        offset = (way * first, way * second) if part == 0 else (way * second, way * first)
        offset = tuple(wrapped(o) for o in offset)
        wave = [w for w, members in enumerate(WAVES) if offset in members][0]
        push(view, view, 1, lent.at[wave], sibling)

    def turn(shard):
        values = tab[shard, :, FREQ_AT : FREQ_AT + LANES].astype(jnp.float32)
        for j in range(3):
            stack = []
            for g in range(4):
                stack.append(tab[shard, :, GROUP_AT[g] + 256 * j : GROUP_AT[g] + 256 * (j + 1)].astype(jnp.float32))
                at_row = 6 * g + 2 * j
                stack.append(
                    jnp.concatenate(
                        [jnp.broadcast_to(values[at_row + h : at_row + h + 1, :], (8, LANES)) for h in range(2)], axis=1
                    )
                )
            stack = jnp.concatenate(stack, axis=0).astype(jnp.bfloat16)
            table[pl.ds(pl.multiple_of(shard * GROUP + 256 * j, 256), 256), :] = lax.dot_general(
                eye[...], stack, NT, preferred_element_type=jnp.float32
            )

    @pl.when(relays)
    def _():
        for axis in (0, 1):
            for way in (1, -1):
                for part in (0, 1):
                    relay(way, part, 0, 0, axis, 1)
                    relay(way, part, 0, 0, axis, -1)
        push(dealt.at[1], dealt.at[1], 2, dealt_sem.at[0], sibling)
        push(mine.at[1], mine.at[1], 3, dealt_sem.at[1], sibling)

    turn(pb)

    def position(chip, source):
        return ((chip + source) & 3) + (chip & 4)

    def blocks_in():
        held = blocks[...]
        modes = jnp.maximum(held, 0)
        local_mode = lax.broadcasted_iota(jnp.int32, modes.shape, 3) == 0
        packed[:, :, :, 0:4] = held
        packed[:, :, :, 4:8] = rows_of(modes + jnp.where(local_mode, pb * LOCAL, 0))
        lane = lax.broadcasted_iota(jnp.int32, (CHIPS, 2, 1, LANES), 3)
        source = lax.broadcasted_iota(jnp.int32, (CHIPS, 2, 1, LANES), 0)
        length = jnp.zeros((CHIPS, 2, 1, LANES), jnp.int32)
        for high in range(4):
            last = jnp.max(jnp.where(held[:, :, high, 1:2] >= 0, lane + 1, 0), axis=3, keepdims=True)
            used = position(z, source) + 8 * high < tallies[...]
            length = jnp.where((lane == high) & used, last, length)
        lengths_v[...] = length

    @pl.when(relays)
    def _():
        for number, (first, second) in enumerate(ORDER):
            bytes_in(tab.at[0], got.at[number])
            for way in (1, -1):
                for part in (0, 1):
                    if second == 0:
                        if first == -1:
                            relay(way, part, first, 0, 0, 1)
                        relay(way, part, first, 0, 1, 1)
                        relay(way, part, first, 0, 1, -1)
                    elif second == -1:
                        relay(way, part, first, second, 1, 1)
                    lend(way, part, first, second)
            if number == len(ORDER) - 1:
                bytes_in(blocks, dealt_sem.at[2])
                bytes_in(tallies, dealt_sem.at[3])
                blocks_in()
            for wave in WAVE_AFTER.get(number, ()):
                for offset in WAVES[wave]:
                    turn(place(*offset))
        bytes_out(tab.at[pl.ds(0, 15)], 0)
        bytes_out(tab.at[pl.ds(0, 15)], 1)
        bytes_out(dealt.at[1], 2)
        bytes_out(mine.at[1], 3)

    @pl.when(jnp.logical_not(relays))
    def _():
        bytes_in(dealt.at[1], dealt_sem.at[0])
        bytes_in(mine.at[1], dealt_sem.at[1])
        for k, dealer in enumerate(dealers):
            push(dealt.at[:, :, position(lax.rem(z + k + 1, CHIPS), z)], blocks.at[z], 2, dealt_sem.at[2], dealer)
            push(mine, tallies.at[z], 3, dealt_sem.at[3], dealer)
        blocks[z] = dealt[:, :, position(z, z)]
        tallies[z] = mine[...]
        for wave, members in enumerate(WAVES):
            if wave == 1:
                bytes_in(blocks.at[pl.ds(0, CHIPS - 1)], dealt_sem.at[2])
                bytes_in(tallies.at[pl.ds(0, CHIPS - 1)], dealt_sem.at[3])
                push(blocks, blocks, 0, dealt_sem.at[2], sibling)
                push(tallies, tallies, 1, dealt_sem.at[3], sibling)
                blocks_in()
            bytes_in(tab.at[pl.ds(0, len(members))], lent.at[wave])
            for offset in members:
                turn(place(*offset))
        bytes_out(blocks.at[pl.ds(0, CHIPS - 1)], 2)
        bytes_out(tallies.at[pl.ds(0, CHIPS - 1)], 3)
        bytes_out(blocks, 0)
        bytes_out(tallies, 1)

    copy_lengths = pltpu.make_async_copy(lengths_v, lengths, local.at[0])
    copy_lengths.start()
    copy_phi.wait()
    copy_cells.wait()
    copy_lengths.wait()

def exchange(eig, freq, quartets, phi, cells, counts):
    hbm = pl.BlockSpec(memory_space=pltpu.HBM)
    vmem = pl.BlockSpec(memory_space=pltpu.VMEM)
    return pl.pallas_call(
        exchange_kernel,
        out_shape=(
            pltpu.VMEM((NB * GROUP, LANES), jnp.float32),
            pltpu.VMEM((CHIPS, 2, 4, 8, LANES), jnp.int32),
            pltpu.SMEM((CHIPS, 2, 1, LANES), jnp.int32),
            pltpu.VMEM((144, 1152), jnp.bfloat16),
            pltpu.VMEM((8, 9), jnp.int32),
            pltpu.VMEM((128, 128), jnp.bfloat16),
            pltpu.VMEM((576, 64), jnp.bfloat16),
        ),
        in_specs=[hbm] * 5 + [pl.BlockSpec(memory_space=pltpu.SMEM)],
        out_specs=(vmem, vmem, pl.BlockSpec(memory_space=pltpu.SMEM), vmem, vmem, vmem, vmem),
        scratch_shapes=[
            pltpu.VMEM((CHIPS, 2, 4, 4, LANES), jnp.int32),
            pltpu.VMEM((CHIPS, 2, 1, LANES), jnp.int32),
            pltpu.VMEM((CHIPS, 2, 1, LANES), jnp.int32),
            pltpu.VMEM((NB, 24, WIDTH), jnp.bfloat16),
            pltpu.VMEM((2, 1, LANES), jnp.int32),
            pltpu.VMEM((256, 256), jnp.bfloat16),
            pltpu.VMEM((2, 4, 8, 4, LANES), jnp.int32),
            pltpu.SemaphoreType.DMA((4,)),
            pltpu.SemaphoreType.DMA((len(ORDER),)),
            pltpu.SemaphoreType.DMA((len(WAVES),)),
            pltpu.SemaphoreType.DMA((4,)),
            pltpu.SemaphoreType.DMA((6,)),
        ],
        compiler_params=pltpu.CompilerParams(collective_id=0, has_side_effects=True, vmem_limit_bytes=24 << 20),
        name="exchange",
    )(*[pltpu.with_memory_space_constraint(a, pltpu.HBM) for a in (eig, freq, quartets, phi, cells)], counts)


def cosine_of(step):
    near = jnp.minimum(step, 16 - step)
    out = jnp.full(step.shape, -1.0, jnp.float32)
    for k in range(8):
        out = jnp.where(near == k, math.cos(math.pi * k / 8) if k != 4 else 0.0, out)
    return out


def floor_div(value, by):
    return jnp.floor((value.astype(jnp.float32) + 0.5) * (1.0 / by)).astype(jnp.int32)


def rows_of(modes):
    unit = floor_div(modes, GROUP)
    return (unit >> 2) * GROUP + modes - unit * GROUP


def quartet_kernel(
    table, packed, lengths, phi, cells, reorder, spread, out,
    wide_a, wide_b, near_a, near_b, scale_a, scale_b, term_a, term_b, freqs_a, freqs_b, vectors_a, vectors_b, held_a, held_b,
    rows_a, rows_b, dense, sums, sem,
):
    pb, wa = lax.axis_index("pb"), lax.axis_index("wa")

    lane8 = lax.broadcasted_iota(jnp.int32, (8, LANES), 1)
    count = jnp.int32(0)
    current = jnp.zeros((8, LANES), jnp.int32)
    for source in range(CHIPS):
        for slot in range(8):
            length = lengths[source, slot // 4, 0, slot % 4]
            offset = count & (LANES - 1)
            rolled = pltpu.roll(packed[source, slot // 4, slot % 4], offset, 1)
            current = jnp.where(lane8 >= offset, rolled, current)
            dense[count >> 7] = current
            current = jnp.where(offset + length >= LANES, rolled, current)
            count = count + length
    filled = (count + LANES - 1) >> 7
    dense[count >> 7] = current
    for k in range(6):
        dense[filled + k] = jnp.zeros((8, LANES), jnp.int32)
    half = (filled + 1) >> 1
    begin = (wa & 1) * half
    total = jnp.where((wa & 1) == 0, half, filled - half)

    sums[...] = jnp.zeros_like(sums)
    cell = cells[...].astype(jnp.float32)

    def fetch(index, into, which):
        return pltpu.make_async_copy(dense.at[begin + index, pl.ds(4, 4)], into, sem.at[which])

    sublane = lax.broadcasted_iota(jnp.int32, (8, LANES), 0)
    odd = [(sublane & (1 << bit)) != 0 for bit in range(3)]

    def gather(into, at):
        for k in range(4):
            for n in range(0, LANES, 16):
                pair = []
                for half in (n, n + 8):
                    level = [table[pl.ds(at[k, half + j], 8, stride=0), :] for j in range(8)]
                    for bit in range(3):
                        level = [jnp.where(odd[bit], high, low) for low, high in zip(level[::2], level[1::2])]
                    pair.append(level[0])
                into[LANES * k + n : LANES * k + n + 16, :] = jnp.concatenate(pair, axis=0).astype(jnp.bfloat16)

    def vectors_of(at, index, held, vectors, freqs_of):
        gather(held, at)
        raw = dense[begin + index][0:4]
        modes = jnp.maximum(raw, 0)
        fullmode = modes + jnp.where(lax.broadcasted_iota(jnp.int32, modes.shape, 0) == 0, pb * LOCAL, 0)
        group = floor_div(fullmode, GROUP) & 3
        turned = lax.dot_general(reorder[...], held[...], NT, preferred_element_type=jnp.float32)
        halves, freqs = [], []
        for k in range(4):
            which = group[k : k + 1, :]
            part = turned[:, LANES * k : LANES * (k + 1)]
            mine = jnp.where(
                which < 2,
                jnp.where(which == 0, part[0:32], part[32:64]),
                jnp.where(which == 2, part[64:96], part[96:128]),
            )
            halves.append(jnp.concatenate([mine[0:16], mine[16:32]], axis=1))
            freqs.append(mine[12:13])
        vectors[...] = jnp.concatenate(halves, axis=0).astype(jnp.bfloat16)
        freqs_of[...] = jnp.concatenate(freqs, axis=0)

    def products(index, vectors, freqs_of, wide, near, scale):
        raw = dense[begin + index][0:4]
        modes = jnp.maximum(raw, 0)
        pairs = jnp.dot(spread[...], vectors[...], preferred_element_type=jnp.float32)
        third, fourth, e1, e2 = (pairs[144 * k : 144 * (k + 1)] for k in range(4))
        far_re = third[:, :LANES] * fourth[:, :LANES] - third[:, LANES:] * fourth[:, LANES:]
        far_im = -(third[:, :LANES] * fourth[:, LANES:] + third[:, LANES:] * fourth[:, :LANES])
        near[0:144] = e1[:, :LANES] * e2[:, :LANES] - e1[:, LANES:] * e2[:, LANES:]
        near[144:288] = e1[:, :LANES] * e2[:, LANES:] + e1[:, LANES:] * e2[:, :LANES]

        point = floor_div(modes, BR)
        coords = [(point >> 8).astype(jnp.float32), ((point >> 4) & 15).astype(jnp.float32), (point & 15).astype(jnp.float32)]
        shift = jnp.zeros((8, LANES), jnp.float32)
        for which in range(3):
            for axis in range(3):
                column = cell[:, 3 * which + axis : 3 * which + axis + 1]
                term = column * coords[axis][which + 1 : which + 2, :]
                shift = shift + term if which == 0 else shift - term
        step = shift.astype(jnp.int32) & 15
        cosine, sine = cosine_of(step), cosine_of((step - 4) & 15)
        for k in range(8):
            c, s = cosine[k : k + 1, :], sine[k : k + 1, :]
            wide[144 * k : 144 * (k + 1), :LANES] = (c * far_re - s * far_im).astype(jnp.bfloat16)
            wide[144 * k : 144 * (k + 1), LANES:] = (c * far_im + s * far_re).astype(jnp.bfloat16)

        freqs = [freqs_of[k : k + 1] for k in range(4)]
        occupied = [1.0 / (jnp.exp(f) - 1.0) for f in freqs]
        mismatch = freqs[0] + freqs[1] - freqs[2] - freqs[3]
        delta = jnp.exp(-((mismatch / SMEARING) ** 2)) / (SMEARING * math.sqrt(math.pi))
        weight = (1.0 + occupied[1]) * occupied[2] * occupied[3] / occupied[0]
        product = freqs[0] * freqs[1] * freqs[2] * freqs[3]
        number = LANES * (begin + index) + lax.broadcasted_iota(jnp.int32, (1, LANES), 1)
        valid = (raw[1:2, :] >= 0) & (number < count)
        scale[...] = jnp.where(valid, delta * weight / product, 0.0)

    def contract(wide, near, scale, term):
        weighted = jnp.dot(phi[...], wide[...], preferred_element_type=jnp.float32)
        w_re, w_im = weighted[:, :LANES], weighted[:, LANES:]
        near_re, near_im = near[0:144], near[144:288]
        value_re = jnp.sum(near_re * w_re - near_im * w_im, axis=0, keepdims=True)
        value_im = jnp.sum(near_re * w_im + near_im * w_re, axis=0, keepdims=True)
        term[...] = (value_re * value_re + value_im * value_im) * scale[...]

    def scatter(index, term):
        first = jnp.maximum(dense[begin + index][0:1, :], 0)
        high = floor_div(first, 192)
        low = first - 192 * high
        placed = jnp.where(lax.broadcasted_iota(jnp.int32, (NB, LANES), 0) == high, term, 0.0)
        one = placed.astype(jnp.bfloat16)
        rest = placed - one.astype(jnp.float32)
        two = rest.astype(jnp.bfloat16)
        three = (rest - two.astype(jnp.float32)).astype(jnp.bfloat16)
        spot = jnp.where(lax.broadcasted_iota(jnp.int32, (256, LANES), 0) == low, 1.0, 0.0).astype(jnp.bfloat16)
        sums[...] += lax.dot_general(
            jnp.concatenate([one, two, three], axis=0), spot, NT, preferred_element_type=jnp.float32
        )

    sides = (
        (rows_a, held_a, vectors_a, freqs_a, scale_a, wide_a, near_a, term_a, 0),
        (rows_b, held_b, vectors_b, freqs_b, scale_b, wide_b, near_b, term_b, 1),
    )

    def step_of(i, side):
        at, held, vectors, freqs_of, scale, wide, near, term, which = sides[side]
        _, _, next_vectors, next_freqs, next_scale, next_wide, next_near, last_term, _ = sides[1 - side]
        fetch(i + 2, at, which).wait()
        scatter(jnp.maximum(i - 1, 0), last_term[...])
        contract(wide, near, scale, term)
        products(i + 1, next_vectors, next_freqs, next_wide, next_near, next_scale)
        vectors_of(at, i + 2, held, vectors, freqs_of)
        fetch(i + 4, at, which).start()

    term_b[...] = jnp.zeros_like(term_b)
    fetch(0, rows_a, 0).start()
    fetch(1, rows_b, 1).start()
    fetch(0, rows_a, 0).wait()
    vectors_of(rows_a, 0, held_a, vectors_a, freqs_a)
    fetch(2, rows_a, 0).start()
    fetch(1, rows_b, 1).wait()
    products(0, vectors_a, freqs_a, wide_a, near_a, scale_a)
    vectors_of(rows_b, 1, held_b, vectors_b, freqs_b)
    fetch(3, rows_b, 1).start()

    def two_blocks(it, carry):
        step_of(2 * it, 0)

        @pl.when(2 * it + 1 < total)
        def _():
            step_of(2 * it + 1, 1)

        return carry

    lax.fori_loop(0, (total + 1) // 2, two_blocks, 0)
    scatter(jnp.maximum(total - 1, 0), jnp.where(total % 2 == 1, term_a[...], term_b[...]))
    fetch(0, rows_a, 0).wait()
    fetch(0, rows_b, 1).wait()
    result = sums[0:16] + sums[16:32] + sums[32:48]
    for w in range(NB):
        out[w] = result[w : w + 1]


def quartet_sums(*operands):
    vmem = pl.BlockSpec(memory_space=pltpu.VMEM)
    smem = pl.BlockSpec(memory_space=pltpu.SMEM)
    pinned = [pltpu.with_memory_space_constraint(a, pltpu.SMEM if k == 2 else pltpu.VMEM) for k, a in enumerate(operands)]
    return pl.pallas_call(
        quartet_kernel,
        out_shape=pltpu.VMEM((NB, 1, 256), jnp.float32),
        in_specs=[vmem, vmem, smem, vmem, vmem, vmem, vmem],
        out_specs=vmem,
        scratch_shapes=[
            pltpu.VMEM((1152, 256), jnp.bfloat16),
            pltpu.VMEM((1152, 256), jnp.bfloat16),
            pltpu.VMEM((288, LANES), jnp.float32),
            pltpu.VMEM((288, LANES), jnp.float32),
            pltpu.VMEM((1, LANES), jnp.float32),
            pltpu.VMEM((1, LANES), jnp.float32),
            pltpu.VMEM((1, LANES), jnp.float32),
            pltpu.VMEM((1, LANES), jnp.float32),
            pltpu.VMEM((4, LANES), jnp.float32),
            pltpu.VMEM((4, LANES), jnp.float32),
            pltpu.VMEM((64, 256), jnp.bfloat16),
            pltpu.VMEM((64, 256), jnp.bfloat16),
            pltpu.VMEM((4 * LANES, LANES), jnp.bfloat16),
            pltpu.VMEM((4 * LANES, LANES), jnp.bfloat16),
            pltpu.SMEM((4, LANES), jnp.int32),
            pltpu.SMEM((4, LANES), jnp.int32),
            pltpu.VMEM((4 * NB + 8, 8, LANES), jnp.int32),
            pltpu.VMEM((48, 256), jnp.float32),
            pltpu.SemaphoreType.DMA((2,)),
        ],
        compiler_params=pltpu.CompilerParams(
            vmem_limit_bytes=16 << 20
        ),
        name="quartets",
    )(*pinned)


def reduce_kernel(part, out, arrived, send, recv):
    pb, wa = lax.axis_index("pb"), lax.axis_index("wa")
    barrier = pltpu.get_barrier_semaphore()
    peers = [lax.rem(wa + k, NB) for k in range(1, NB)]
    for peer in peers:
        pl.semaphore_signal(barrier, inc=1, device_id=(pb, peer), device_id_type=MESH)
    pl.semaphore_wait(barrier, NB - 1)
    for k, peer in enumerate(peers):
        pltpu.make_async_remote_copy(
            src_ref=part.at[peer], dst_ref=arrived.at[k], send_sem=send.at[0], recv_sem=recv.at[0],
            device_id=(pb, peer), device_id_type=MESH,
        ).start()
    everything = pltpu.make_async_remote_copy(
        src_ref=part.at[pl.ds(0, NB - 1)], dst_ref=arrived, send_sem=send.at[0], recv_sem=recv.at[0],
        device_id=(pb, peers[0]), device_id_type=MESH,
    )
    everything.wait_recv()
    total = part[wa]
    for k in range(NB - 1):
        total = total + arrived[k]
    out[...] = total
    everything.wait_send()


def reduce_over_wa(part):
    vmem = pl.BlockSpec(memory_space=pltpu.VMEM)
    return pl.pallas_call(
        reduce_kernel,
        out_shape=jax.ShapeDtypeStruct((1, 256), jnp.float32),
        in_specs=[vmem],
        out_specs=vmem,
        scratch_shapes=[
            pltpu.VMEM((NB - 1, 1, 256), jnp.float32),
            pltpu.SemaphoreType.DMA((1,)),
            pltpu.SemaphoreType.DMA((1,)),
        ],
        compiler_params=pltpu.CompilerParams(collective_id=1, has_side_effects=True, vmem_limit_bytes=1 << 20),
        name="reduce_wa",
    )(pltpu.with_memory_space_constraint(part, pltpu.VMEM))


def body(quartets, counts, eig, freq, phi, cells):
    dealt = quartets.reshape(4, 8, 4, LANES)
    held = exchange(eig, freq.reshape(24, LANES), dealt, phi, cells, counts)
    part = quartet_sums(*held)
    return reduce_over_wa(part)[0, :192]


def solution(mesh):
    placed = (P(("pb", "wa"), None, None), P(("pb", "wa")), P(None, "pb"), P("pb"), P(), P())
    return jax.shard_map(body, mesh=mesh, in_specs=placed, out_specs=P(("pb", "wa")), check_vma=False)
```

```python
import functools
import math

import jax
import jax.numpy as jnp
from jax import lax
from jax.experimental import pallas as pl
from jax.experimental.pallas import tpu as pltpu
from jax.sharding import PartitionSpec as P

QMESH = 16
BR = 12
NB = 16
LOCAL = 3072
GROUP = 768
LANES = 128
GROUP_AT = (0, 768, 1664, 2432)
FREQ_AT = 1536
WIDTH = 3200
SMEARING = 0.5
MESH = pl.DeviceIdType.MESH
NT = (((1,), (1,)), ((), ()))


PIECES = {(1, 0): (0, 768), (1, 1): (768, 896), (-1, 1): (1664, 768), (-1, 0): (2432, 768)}
RELAY_CORE = 1
CHIPS = 8
ORDER = (
    (-1, 0), (1, 0), (0, -1), (0, 1), (2, 0), (-1, -1), (-1, 1), (0, 2), (1, -1), (1, 1), (-1, 2), (2, -1), (2, 1), (1, 2), (2, 2),
)
WAVES = (
    ((-1, 0), (1, 0), (0, -1), (0, 1)),
    ((2, 0), (0, 2)),
    ((-1, 1), (1, -1)),
    ((-1, -1), (1, 1)),
    ((-1, 2), (2, -1), (2, 1), (1, 2)),
    ((2, 2),),
)
LEND_AFTER = {3: (0,), 7: (1,), 8: (2,), 9: (3,), 13: (4,), 14: (5,)}
TURN_AFTER = {
    4: ((-1, 0),), 5: ((1, 0),), 6: ((0, -1),), 7: ((0, 1),), 8: ((2, 0),), 9: ((0, 2),), 10: ((-1, 1),),
    11: ((1, -1), (-1, -1), (1, 1)), 13: ((-1, 2), (2, -1), (2, 1), (1, 2)), 14: ((2, 2),),
}


def wrapped(offset):
    return (offset + 1) % 4 - 1


def hit(rows, columns, where):
    r = lax.broadcasted_iota(jnp.int32, (rows, columns), 0)
    c = lax.broadcasted_iota(jnp.int32, (rows, columns), 1)
    return jnp.where(where(r) == c, 1.0, 0.0).astype(jnp.bfloat16)


def spread_column(r):
    kind = floor_div(r, 144)
    t = r - 144 * kind
    first = floor_div(t, BR)
    return ((kind + 2) & 3) * 16 + jnp.where((kind & 1) == 0, first, t - BR * first)


def order_column(r):
    t = r & 31
    lane = jnp.where(t < 12, t, jnp.where(t == 12, 24, jnp.where((t >= 16) & (t < 28), t - 4, -999)))
    return lane + (r - t)


def exchange_kernel(
    eig, freq, quartets, phi, cells, counts,
    table, packed, lengths, phi_v, cells_v, reorder, spread,
    blocks, tallies, lengths_v, tab, mine, eye, dealt, send, got, lent, dealt_sem, local,
):
    pb, wa = lax.axis_index("pb"), lax.axis_index("wa")
    x, y, z, core = pb // 4, pb % 4, wa // 2, wa % 2
    relays = core == RELAY_CORE
    sibling = (pb, wa + 1 - 2 * core)
    dealers = [(pb, 2 * lax.rem(z + k, CHIPS)) for k in range(1, CHIPS)]

    def place(dx, dy):
        return lax.rem(x + dx + 4, 4) * 4 + lax.rem(y + dy + 4, 4)

    left = pltpu.make_async_copy(eig.at[:, pl.ds(0, 1536)], tab.at[pb, :, pl.ds(0, 1536)], local.at[0])
    right = pltpu.make_async_copy(eig.at[:, pl.ds(1536, 1536)], tab.at[pb, :, pl.ds(1664, 1536)], local.at[1])
    copy_freq = pltpu.make_async_copy(freq, tab.at[pb, :, pl.ds(FREQ_AT, LANES)], local.at[2])
    copy_dealt = pltpu.make_async_copy(quartets, dealt.at[core], local.at[3])
    copy_phi = pltpu.make_async_copy(phi, phi_v, local.at[4])
    copy_cells = pltpu.make_async_copy(cells, cells_v, local.at[5])
    first_copies = (left, right, copy_freq, copy_dealt)
    for copy in first_copies + (copy_phi, copy_cells):
        copy.start()
    barrier = pltpu.get_barrier_semaphore()
    pl.semaphore_signal(barrier, inc=1, device_id=sibling, device_id_type=MESH)

    @pl.when(relays)
    def _():
        for step in (1, -1):
            pl.semaphore_signal(barrier, inc=1, device_id=(place(step, 0), wa), device_id_type=MESH)
            pl.semaphore_signal(barrier, inc=1, device_id=(place(0, step), wa), device_id_type=MESH)

    @pl.when(jnp.logical_not(relays))
    def _():
        for dealer in dealers:
            pl.semaphore_signal(barrier, inc=1, device_id=dealer, device_id_type=MESH)

    mine[core] = jnp.full((1, LANES), counts[0], jnp.int32)
    eye[...] = hit(256, 256, lambda r: r)
    reorder[...] = hit(LANES, LANES, order_column)
    spread[...] = hit(576, 64, spread_column)
    for copy in first_copies:
        copy.wait()

    pl.semaphore_wait(barrier, jnp.where(relays, 5, CHIPS))

    def push(src, dst, sent, arrival, device):
        pltpu.make_async_remote_copy(
            src_ref=src, dst_ref=dst, send_sem=send.at[sent], recv_sem=arrival, device_id=device, device_id_type=MESH
        ).start()

    def bytes_in(view, sem):
        pltpu.make_async_remote_copy(
            src_ref=view, dst_ref=view, send_sem=send.at[0], recv_sem=sem, device_id=sibling, device_id_type=MESH
        ).wait_recv()

    def bytes_out(view, sent):
        pltpu.make_async_remote_copy(
            src_ref=view, dst_ref=view, send_sem=send.at[sent], recv_sem=got.at[0], device_id=sibling, device_id_type=MESH
        ).wait_send()

    def at(way, part, first, second):
        return place(way * first, way * second) if part == 0 else place(way * second, way * first)

    def relay(way, part, first, second, axis, step):
        start, width = PIECES[way, part]
        view = tab.at[at(way, part, first, second), :, pl.ds(start, width)]
        key = (wrapped(first - step), second) if axis == 0 else (first, wrapped(second - step))
        target = at(way, part, step, 0) if axis == 0 else at(way, part, 0, step)
        push(view, view, 0, got.at[ORDER.index(key)], (target, wa))

    def lend(shard, wave):
        push(tab.at[shard], tab.at[shard], 1, lent.at[wave], sibling)

    def turn(shard):
        values = tab[shard, :, FREQ_AT : FREQ_AT + LANES].astype(jnp.float32)
        for j in range(3):
            stack = []
            for g in range(4):
                stack.append(tab[shard, :, GROUP_AT[g] + 256 * j : GROUP_AT[g] + 256 * (j + 1)].astype(jnp.float32))
                at_row = 6 * g + 2 * j
                stack.append(
                    jnp.concatenate(
                        [jnp.broadcast_to(values[at_row + h : at_row + h + 1, :], (8, LANES)) for h in range(2)], axis=1
                    )
                )
            stack = jnp.concatenate(stack, axis=0).astype(jnp.bfloat16)
            table[pl.ds(pl.multiple_of(shard * GROUP + 256 * j, 256), 256), :] = lax.dot_general(
                eye[...], stack, NT, preferred_element_type=jnp.float32
            )

    @pl.when(relays)
    def _():
        for axis in (0, 1):
            for way in (1, -1):
                for part in (0, 1):
                    relay(way, part, 0, 0, axis, 1)
                    relay(way, part, 0, 0, axis, -1)
        push(dealt.at[1], dealt.at[1], 2, dealt_sem.at[0], sibling)
        push(mine.at[1], mine.at[1], 3, dealt_sem.at[1], sibling)

    turn(pb)

    def position(chip, source):
        return ((chip + source) & 3) + (chip & 4)

    def blocks_in():
        held = blocks[...]
        modes = jnp.maximum(held, 0)
        local_mode = lax.broadcasted_iota(jnp.int32, modes.shape, 3) == 0
        packed[:, :, :, 0:4] = held
        packed[:, :, :, 4:8] = rows_of(modes + jnp.where(local_mode, pb * LOCAL, 0))
        lane = lax.broadcasted_iota(jnp.int32, (CHIPS, 2, 1, LANES), 3)
        source = lax.broadcasted_iota(jnp.int32, (CHIPS, 2, 1, LANES), 0)
        length = jnp.zeros((CHIPS, 2, 1, LANES), jnp.int32)
        for high in range(4):
            last = jnp.max(jnp.where(held[:, :, high, 1:2] >= 0, lane + 1, 0), axis=3, keepdims=True)
            used = position(z, source) + 8 * high < tallies[...]
            length = jnp.where((lane == high) & used, last, length)
        lengths_v[...] = length

    @pl.when(relays)
    def _():
        for number, (first, second) in enumerate(ORDER):
            bytes_in(tab.at[0], got.at[number])
            if second == 0 and first == -1:
                for way in (1, -1):
                    for part in (0, 1):
                        relay(way, part, first, 0, 0, 1)
            if second in (0, -1):
                for way in (1, -1):
                    for part in (0, 1):
                        relay(way, part, first, second, 1, 1)
                        if second == 0:
                            relay(way, part, first, second, 1, -1)
            for wave in LEND_AFTER.get(number, ()):
                for offset in WAVES[wave]:
                    lend(place(*offset), wave)
            for offset in TURN_AFTER.get(number, ()):
                turn(place(*offset))
            if number == 13:
                bytes_in(blocks, dealt_sem.at[2])
                bytes_in(tallies, dealt_sem.at[3])
                blocks_in()
        bytes_out(tab.at[pl.ds(0, 15)], 0)
        bytes_out(tab.at[pl.ds(0, 15)], 1)
        bytes_out(dealt.at[1], 2)
        bytes_out(mine.at[1], 3)

    @pl.when(jnp.logical_not(relays))
    def _():
        bytes_in(dealt.at[1], dealt_sem.at[0])
        bytes_in(mine.at[1], dealt_sem.at[1])
        for k, dealer in enumerate(dealers):
            push(dealt.at[:, :, position(lax.rem(z + k + 1, CHIPS), z)], blocks.at[z], 2, dealt_sem.at[2], dealer)
            push(mine, tallies.at[z], 3, dealt_sem.at[3], dealer)
        blocks[z] = dealt[:, :, position(z, z)]
        tallies[z] = mine[...]
        for wave, members in enumerate(WAVES):
            if wave == 1:
                bytes_in(blocks.at[pl.ds(0, CHIPS - 1)], dealt_sem.at[2])
                bytes_in(tallies.at[pl.ds(0, CHIPS - 1)], dealt_sem.at[3])
                push(blocks, blocks, 0, dealt_sem.at[2], sibling)
                push(tallies, tallies, 1, dealt_sem.at[3], sibling)
                blocks_in()
            bytes_in(tab.at[pl.ds(0, len(members))], lent.at[wave])
            for offset in members:
                turn(place(*offset))
        bytes_out(blocks.at[pl.ds(0, CHIPS - 1)], 2)
        bytes_out(tallies.at[pl.ds(0, CHIPS - 1)], 3)
        bytes_out(blocks, 0)
        bytes_out(tallies, 1)

    copy_lengths = pltpu.make_async_copy(lengths_v, lengths, local.at[0])
    copy_lengths.start()
    copy_phi.wait()
    copy_cells.wait()
    copy_lengths.wait()

def exchange(eig, freq, quartets, phi, cells, counts):
    hbm = pl.BlockSpec(memory_space=pltpu.HBM)
    vmem = pl.BlockSpec(memory_space=pltpu.VMEM)
    return pl.pallas_call(
        exchange_kernel,
        out_shape=(
            pltpu.VMEM((NB * GROUP, LANES), jnp.float32),
            pltpu.VMEM((CHIPS, 2, 4, 8, LANES), jnp.int32),
            pltpu.SMEM((CHIPS, 2, 1, LANES), jnp.int32),
            pltpu.VMEM((144, 1152), jnp.bfloat16),
            pltpu.VMEM((8, 9), jnp.int32),
            pltpu.VMEM((128, 128), jnp.bfloat16),
            pltpu.VMEM((576, 64), jnp.bfloat16),
        ),
        in_specs=[hbm] * 5 + [pl.BlockSpec(memory_space=pltpu.SMEM)],
        out_specs=(vmem, vmem, pl.BlockSpec(memory_space=pltpu.SMEM), vmem, vmem, vmem, vmem),
        scratch_shapes=[
            pltpu.VMEM((CHIPS, 2, 4, 4, LANES), jnp.int32),
            pltpu.VMEM((CHIPS, 2, 1, LANES), jnp.int32),
            pltpu.VMEM((CHIPS, 2, 1, LANES), jnp.int32),
            pltpu.VMEM((NB, 24, WIDTH), jnp.bfloat16),
            pltpu.VMEM((2, 1, LANES), jnp.int32),
            pltpu.VMEM((256, 256), jnp.bfloat16),
            pltpu.VMEM((2, 4, 8, 4, LANES), jnp.int32),
            pltpu.SemaphoreType.DMA((4,)),
            pltpu.SemaphoreType.DMA((len(ORDER),)),
            pltpu.SemaphoreType.DMA((len(WAVES),)),
            pltpu.SemaphoreType.DMA((4,)),
            pltpu.SemaphoreType.DMA((6,)),
        ],
        compiler_params=pltpu.CompilerParams(collective_id=0, has_side_effects=True, vmem_limit_bytes=24 << 20),
        name="exchange",
    )(*[pltpu.with_memory_space_constraint(a, pltpu.HBM) for a in (eig, freq, quartets, phi, cells)], counts)


def cosine_of(step):
    near = jnp.minimum(step, 16 - step)
    out = jnp.full(step.shape, -1.0, jnp.float32)
    for k in range(8):
        out = jnp.where(near == k, math.cos(math.pi * k / 8) if k != 4 else 0.0, out)
    return out


def floor_div(value, by):
    return jnp.floor((value.astype(jnp.float32) + 0.5) * (1.0 / by)).astype(jnp.int32)


def rows_of(modes):
    unit = floor_div(modes, GROUP)
    return (unit >> 2) * GROUP + modes - unit * GROUP


def quartet_kernel(
    table, packed, lengths, phi, cells, reorder, spread, out,
    wide_a, wide_b, near_a, near_b, scale_a, scale_b, term_a, term_b, freqs_a, freqs_b, vectors_a, vectors_b, held_a, held_b,
    rows_a, rows_b, dense, sums, sem,
):
    pb, wa = lax.axis_index("pb"), lax.axis_index("wa")

    lane8 = lax.broadcasted_iota(jnp.int32, (8, LANES), 1)
    count = jnp.int32(0)
    current = jnp.zeros((8, LANES), jnp.int32)
    for source in range(CHIPS):
        for slot in range(8):
            length = lengths[source, slot // 4, 0, slot % 4]
            offset = count & (LANES - 1)
            rolled = pltpu.roll(packed[source, slot // 4, slot % 4], offset, 1)
            current = jnp.where(lane8 >= offset, rolled, current)
            dense[count >> 7] = current
            current = jnp.where(offset + length >= LANES, rolled, current)
            count = count + length
    filled = (count + LANES - 1) >> 7
    dense[count >> 7] = current
    for k in range(6):
        dense[filled + k] = jnp.zeros((8, LANES), jnp.int32)
    half = (filled + 1) >> 1
    begin = (wa & 1) * half
    total = jnp.where((wa & 1) == 0, half, filled - half)

    sums[...] = jnp.zeros_like(sums)
    cell = cells[...].astype(jnp.float32)

    def fetch(index, into, which):
        return pltpu.make_async_copy(dense.at[begin + index, pl.ds(4, 4)], into, sem.at[which])

    sublane = lax.broadcasted_iota(jnp.int32, (8, LANES), 0)
    odd = [(sublane & (1 << bit)) != 0 for bit in range(3)]

    def gather(into, at):
        for k in range(4):
            for n in range(0, LANES, 16):
                pair = []
                for half in (n, n + 8):
                    level = [table[pl.ds(at[k, half + j], 8, stride=0), :] for j in range(8)]
                    for bit in range(3):
                        level = [jnp.where(odd[bit], high, low) for low, high in zip(level[::2], level[1::2])]
                    pair.append(level[0])
                into[LANES * k + n : LANES * k + n + 16, :] = jnp.concatenate(pair, axis=0).astype(jnp.bfloat16)

    def vectors_of(at, index, held, vectors, freqs_of):
        gather(held, at)
        raw = dense[begin + index][0:4]
        modes = jnp.maximum(raw, 0)
        fullmode = modes + jnp.where(lax.broadcasted_iota(jnp.int32, modes.shape, 0) == 0, pb * LOCAL, 0)
        group = floor_div(fullmode, GROUP) & 3
        turned = lax.dot_general(reorder[...], held[...], NT, preferred_element_type=jnp.float32)
        halves, freqs = [], []
        for k in range(4):
            which = group[k : k + 1, :]
            part = turned[:, LANES * k : LANES * (k + 1)]
            mine = jnp.where(
                which < 2,
                jnp.where(which == 0, part[0:32], part[32:64]),
                jnp.where(which == 2, part[64:96], part[96:128]),
            )
            halves.append(jnp.concatenate([mine[0:16], mine[16:32]], axis=1))
            freqs.append(mine[12:13])
        vectors[...] = jnp.concatenate(halves, axis=0).astype(jnp.bfloat16)
        freqs_of[...] = jnp.concatenate(freqs, axis=0)

    def products(index, vectors, freqs_of, wide, near, scale):
        raw = dense[begin + index][0:4]
        modes = jnp.maximum(raw, 0)
        pairs = jnp.dot(spread[...], vectors[...], preferred_element_type=jnp.float32)
        third, fourth, e1, e2 = (pairs[144 * k : 144 * (k + 1)] for k in range(4))
        far_re = third[:, :LANES] * fourth[:, :LANES] - third[:, LANES:] * fourth[:, LANES:]
        far_im = -(third[:, :LANES] * fourth[:, LANES:] + third[:, LANES:] * fourth[:, :LANES])
        near[0:144] = e1[:, :LANES] * e2[:, :LANES] - e1[:, LANES:] * e2[:, LANES:]
        near[144:288] = e1[:, :LANES] * e2[:, LANES:] + e1[:, LANES:] * e2[:, :LANES]

        point = floor_div(modes, BR)
        coords = [(point >> 8).astype(jnp.float32), ((point >> 4) & 15).astype(jnp.float32), (point & 15).astype(jnp.float32)]
        shift = jnp.zeros((8, LANES), jnp.float32)
        for which in range(3):
            for axis in range(3):
                column = cell[:, 3 * which + axis : 3 * which + axis + 1]
                term = column * coords[axis][which + 1 : which + 2, :]
                shift = shift + term if which == 0 else shift - term
        step = shift.astype(jnp.int32) & 15
        cosine, sine = cosine_of(step), cosine_of((step - 4) & 15)
        for k in range(8):
            c, s = cosine[k : k + 1, :], sine[k : k + 1, :]
            wide[144 * k : 144 * (k + 1), :LANES] = (c * far_re - s * far_im).astype(jnp.bfloat16)
            wide[144 * k : 144 * (k + 1), LANES:] = (c * far_im + s * far_re).astype(jnp.bfloat16)

        freqs = [freqs_of[k : k + 1] for k in range(4)]
        occupied = [1.0 / (jnp.exp(f) - 1.0) for f in freqs]
        mismatch = freqs[0] + freqs[1] - freqs[2] - freqs[3]
        delta = jnp.exp(-((mismatch / SMEARING) ** 2)) / (SMEARING * math.sqrt(math.pi))
        weight = (1.0 + occupied[1]) * occupied[2] * occupied[3] / occupied[0]
        product = freqs[0] * freqs[1] * freqs[2] * freqs[3]
        number = LANES * (begin + index) + lax.broadcasted_iota(jnp.int32, (1, LANES), 1)
        valid = (raw[1:2, :] >= 0) & (number < count)
        scale[...] = jnp.where(valid, delta * weight / product, 0.0)

    def contract(wide, near, scale, term):
        weighted = jnp.dot(phi[...], wide[...], preferred_element_type=jnp.float32)
        w_re, w_im = weighted[:, :LANES], weighted[:, LANES:]
        near_re, near_im = near[0:144], near[144:288]
        value_re = jnp.sum(near_re * w_re - near_im * w_im, axis=0, keepdims=True)
        value_im = jnp.sum(near_re * w_im + near_im * w_re, axis=0, keepdims=True)
        term[...] = (value_re * value_re + value_im * value_im) * scale[...]

    def scatter(index, term):
        first = jnp.maximum(dense[begin + index][0:1, :], 0)
        high = floor_div(first, 192)
        low = first - 192 * high
        placed = jnp.where(lax.broadcasted_iota(jnp.int32, (NB, LANES), 0) == high, term, 0.0)
        one = placed.astype(jnp.bfloat16)
        rest = placed - one.astype(jnp.float32)
        two = rest.astype(jnp.bfloat16)
        three = (rest - two.astype(jnp.float32)).astype(jnp.bfloat16)
        spot = jnp.where(lax.broadcasted_iota(jnp.int32, (256, LANES), 0) == low, 1.0, 0.0).astype(jnp.bfloat16)
        sums[...] += lax.dot_general(
            jnp.concatenate([one, two, three], axis=0), spot, NT, preferred_element_type=jnp.float32
        )

    sides = (
        (rows_a, held_a, vectors_a, freqs_a, scale_a, wide_a, near_a, term_a, 0),
        (rows_b, held_b, vectors_b, freqs_b, scale_b, wide_b, near_b, term_b, 1),
    )

    def step_of(i, side):
        at, held, vectors, freqs_of, scale, wide, near, term, which = sides[side]
        _, _, next_vectors, next_freqs, next_scale, next_wide, next_near, last_term, _ = sides[1 - side]
        fetch(i + 2, at, which).wait()
        scatter(jnp.maximum(i - 1, 0), last_term[...])
        contract(wide, near, scale, term)
        products(i + 1, next_vectors, next_freqs, next_wide, next_near, next_scale)
        vectors_of(at, i + 2, held, vectors, freqs_of)
        fetch(i + 4, at, which).start()

    term_b[...] = jnp.zeros_like(term_b)
    fetch(0, rows_a, 0).start()
    fetch(1, rows_b, 1).start()
    fetch(0, rows_a, 0).wait()
    vectors_of(rows_a, 0, held_a, vectors_a, freqs_a)
    fetch(2, rows_a, 0).start()
    fetch(1, rows_b, 1).wait()
    products(0, vectors_a, freqs_a, wide_a, near_a, scale_a)
    vectors_of(rows_b, 1, held_b, vectors_b, freqs_b)
    fetch(3, rows_b, 1).start()

    def two_blocks(it, carry):
        step_of(2 * it, 0)

        @pl.when(2 * it + 1 < total)
        def _():
            step_of(2 * it + 1, 1)

        return carry

    lax.fori_loop(0, (total + 1) // 2, two_blocks, 0)
    scatter(jnp.maximum(total - 1, 0), jnp.where(total % 2 == 1, term_a[...], term_b[...]))
    fetch(0, rows_a, 0).wait()
    fetch(0, rows_b, 1).wait()
    result = sums[0:16] + sums[16:32] + sums[32:48]
    for w in range(NB):
        out[w] = result[w : w + 1]


def quartet_sums(*operands):
    vmem = pl.BlockSpec(memory_space=pltpu.VMEM)
    smem = pl.BlockSpec(memory_space=pltpu.SMEM)
    pinned = [pltpu.with_memory_space_constraint(a, pltpu.SMEM if k == 2 else pltpu.VMEM) for k, a in enumerate(operands)]
    return pl.pallas_call(
        quartet_kernel,
        out_shape=pltpu.VMEM((NB, 1, 256), jnp.float32),
        in_specs=[vmem, vmem, smem, vmem, vmem, vmem, vmem],
        out_specs=vmem,
        scratch_shapes=[
            pltpu.VMEM((1152, 256), jnp.bfloat16),
            pltpu.VMEM((1152, 256), jnp.bfloat16),
            pltpu.VMEM((288, LANES), jnp.float32),
            pltpu.VMEM((288, LANES), jnp.float32),
            pltpu.VMEM((1, LANES), jnp.float32),
            pltpu.VMEM((1, LANES), jnp.float32),
            pltpu.VMEM((1, LANES), jnp.float32),
            pltpu.VMEM((1, LANES), jnp.float32),
            pltpu.VMEM((4, LANES), jnp.float32),
            pltpu.VMEM((4, LANES), jnp.float32),
            pltpu.VMEM((64, 256), jnp.bfloat16),
            pltpu.VMEM((64, 256), jnp.bfloat16),
            pltpu.VMEM((4 * LANES, LANES), jnp.bfloat16),
            pltpu.VMEM((4 * LANES, LANES), jnp.bfloat16),
            pltpu.SMEM((4, LANES), jnp.int32),
            pltpu.SMEM((4, LANES), jnp.int32),
            pltpu.VMEM((4 * NB + 8, 8, LANES), jnp.int32),
            pltpu.VMEM((48, 256), jnp.float32),
            pltpu.SemaphoreType.DMA((2,)),
        ],
        compiler_params=pltpu.CompilerParams(
            vmem_limit_bytes=16 << 20
        ),
        name="quartets",
    )(*pinned)


def reduce_kernel(part, out, arrived, send, recv):
    pb, wa = lax.axis_index("pb"), lax.axis_index("wa")
    barrier = pltpu.get_barrier_semaphore()
    peers = [lax.rem(wa + k, NB) for k in range(1, NB)]
    for peer in peers:
        pl.semaphore_signal(barrier, inc=1, device_id=(pb, peer), device_id_type=MESH)
    pl.semaphore_wait(barrier, NB - 1)
    for k, peer in enumerate(peers):
        pltpu.make_async_remote_copy(
            src_ref=part.at[peer], dst_ref=arrived.at[k], send_sem=send.at[0], recv_sem=recv.at[0],
            device_id=(pb, peer), device_id_type=MESH,
        ).start()
    everything = pltpu.make_async_remote_copy(
        src_ref=part.at[pl.ds(0, NB - 1)], dst_ref=arrived, send_sem=send.at[0], recv_sem=recv.at[0],
        device_id=(pb, peers[0]), device_id_type=MESH,
    )
    everything.wait_recv()
    total = part[wa]
    for k in range(NB - 1):
        total = total + arrived[k]
    out[...] = total
    everything.wait_send()


def reduce_over_wa(part):
    vmem = pl.BlockSpec(memory_space=pltpu.VMEM)
    return pl.pallas_call(
        reduce_kernel,
        out_shape=jax.ShapeDtypeStruct((1, 256), jnp.float32),
        in_specs=[vmem],
        out_specs=vmem,
        scratch_shapes=[
            pltpu.VMEM((NB - 1, 1, 256), jnp.float32),
            pltpu.SemaphoreType.DMA((1,)),
            pltpu.SemaphoreType.DMA((1,)),
        ],
        compiler_params=pltpu.CompilerParams(collective_id=1, has_side_effects=True, vmem_limit_bytes=1 << 20),
        name="reduce_wa",
    )(pltpu.with_memory_space_constraint(part, pltpu.VMEM))


def body(quartets, counts, eig, freq, phi, cells):
    dealt = quartets.reshape(4, 8, 4, LANES)
    held = exchange(eig, freq.reshape(24, LANES), dealt, phi, cells, counts)
    part = quartet_sums(*held)
    return reduce_over_wa(part)[0, :192]


def solution(mesh):
    placed = (P(("pb", "wa"), None, None), P(("pb", "wa")), P(None, "pb"), P("pb"), P(), P())
    return jax.shard_map(body, mesh=mesh, in_specs=placed, out_specs=P(("pb", "wa")), check_vma=False)
```

```python
import functools
import math

import jax
import jax.numpy as jnp
from jax import lax
from jax.experimental import pallas as pl
from jax.experimental.pallas import tpu as pltpu
from jax.sharding import PartitionSpec as P

QMESH = 16
BR = 12
NB = 16
LOCAL = 3072
GROUP = 768
LANES = 128
GROUP_AT = (0, 768, 1664, 2432)
FREQ_AT = 1536
WIDTH = 3200
SMEARING = 0.5
MESH = pl.DeviceIdType.MESH
NT = (((1,), (1,)), ((), ()))


PIECES = {(1, 0): (0, 768), (1, 1): (768, 896), (-1, 1): (1664, 768), (-1, 0): (2432, 768)}
RELAY_CORE = 1
CHIPS = 8
ORDER = (
    (-1, 0), (1, 0), (0, -1), (0, 1), (2, 0), (-1, -1), (-1, 1), (0, 2), (1, -1), (1, 1), (-1, 2), (2, -1), (2, 1), (1, 2), (2, 2),
)
WAVES = (
    ((-1, 0), (1, 0), (0, -1), (0, 1)),
    ((2, 0), (0, 2)),
    ((-1, 1), (1, -1)),
    ((-1, -1), (1, 1)),
    ((-1, 2), (2, -1), (2, 1), (1, 2)),
    ((2, 2),),
)
LEND_AFTER = {3: (0,), 7: (1,), 8: (2,), 9: (3,), 13: (4,), 14: (5,)}
TURN_AFTER = {
    4: ((-1, 0),), 5: ((1, 0),), 6: ((0, -1),), 7: ((0, 1),), 8: ((2, 0),), 9: ((0, 2),), 10: ((-1, 1),),
    11: ((1, -1), (-1, -1), (1, 1)), 14: ((-1, 2), (2, -1), (2, 1), (1, 2), (2, 2)),
}


def wrapped(offset):
    return (offset + 1) % 4 - 1


def hit(rows, columns, where):
    r = lax.broadcasted_iota(jnp.int32, (rows, columns), 0)
    c = lax.broadcasted_iota(jnp.int32, (rows, columns), 1)
    return jnp.where(where(r) == c, 1.0, 0.0).astype(jnp.bfloat16)


def spread_column(r):
    kind = floor_div(r, 144)
    t = r - 144 * kind
    first = floor_div(t, BR)
    return ((kind + 2) & 3) * 16 + jnp.where((kind & 1) == 0, first, t - BR * first)


def order_column(r):
    t = r & 31
    lane = jnp.where(t < 12, t, jnp.where(t == 12, 24, jnp.where((t >= 16) & (t < 28), t - 4, -999)))
    return lane + (r - t)


def exchange_kernel(
    eig, freq, quartets, phi, cells, counts,
    table, packed, lengths, phi_v, cells_v, reorder, spread,
    blocks, tallies, lengths_v, tab, mine, eye, dealt, send, got, lent, dealt_sem, local,
):
    pb, wa = lax.axis_index("pb"), lax.axis_index("wa")
    x, y, z, core = pb // 4, pb % 4, wa // 2, wa % 2
    relays = core == RELAY_CORE
    sibling = (pb, wa + 1 - 2 * core)
    dealers = [(pb, 2 * lax.rem(z + k, CHIPS)) for k in range(1, CHIPS)]

    def place(dx, dy):
        return lax.rem(x + dx + 4, 4) * 4 + lax.rem(y + dy + 4, 4)

    left = pltpu.make_async_copy(eig.at[:, pl.ds(0, 1536)], tab.at[pb, :, pl.ds(0, 1536)], local.at[0])
    right = pltpu.make_async_copy(eig.at[:, pl.ds(1536, 1536)], tab.at[pb, :, pl.ds(1664, 1536)], local.at[1])
    copy_freq = pltpu.make_async_copy(freq, tab.at[pb, :, pl.ds(FREQ_AT, LANES)], local.at[2])
    copy_dealt = pltpu.make_async_copy(quartets, dealt.at[core], local.at[3])
    copy_phi = pltpu.make_async_copy(phi, phi_v, local.at[4])
    copy_cells = pltpu.make_async_copy(cells, cells_v, local.at[5])
    first_copies = (left, right, copy_freq, copy_dealt)
    for copy in first_copies + (copy_phi, copy_cells):
        copy.start()
    barrier = pltpu.get_barrier_semaphore()
    pl.semaphore_signal(barrier, inc=1, device_id=sibling, device_id_type=MESH)

    @pl.when(relays)
    def _():
        for step in (1, -1):
            pl.semaphore_signal(barrier, inc=1, device_id=(place(step, 0), wa), device_id_type=MESH)
            pl.semaphore_signal(barrier, inc=1, device_id=(place(0, step), wa), device_id_type=MESH)

    @pl.when(jnp.logical_not(relays))
    def _():
        for dealer in dealers:
            pl.semaphore_signal(barrier, inc=1, device_id=dealer, device_id_type=MESH)

    mine[core] = jnp.full((1, LANES), counts[0], jnp.int32)
    eye[...] = hit(256, 256, lambda r: r)
    reorder[...] = hit(LANES, LANES, order_column)
    spread[...] = hit(576, 64, spread_column)
    for copy in first_copies:
        copy.wait()

    pl.semaphore_wait(barrier, jnp.where(relays, 5, CHIPS))

    def push(src, dst, sent, arrival, device):
        pltpu.make_async_remote_copy(
            src_ref=src, dst_ref=dst, send_sem=send.at[sent], recv_sem=arrival, device_id=device, device_id_type=MESH
        ).start()

    def bytes_in(view, sem):
        pltpu.make_async_remote_copy(
            src_ref=view, dst_ref=view, send_sem=send.at[0], recv_sem=sem, device_id=sibling, device_id_type=MESH
        ).wait_recv()

    def bytes_out(view, sent):
        pltpu.make_async_remote_copy(
            src_ref=view, dst_ref=view, send_sem=send.at[sent], recv_sem=got.at[0], device_id=sibling, device_id_type=MESH
        ).wait_send()

    def at(way, part, first, second):
        return place(way * first, way * second) if part == 0 else place(way * second, way * first)

    def relay(way, part, first, second, axis, step):
        start, width = PIECES[way, part]
        view = tab.at[at(way, part, first, second), :, pl.ds(start, width)]
        key = (wrapped(first - step), second) if axis == 0 else (first, wrapped(second - step))
        target = at(way, part, step, 0) if axis == 0 else at(way, part, 0, step)
        push(view, view, 0, got.at[ORDER.index(key)], (target, wa))

    def lend(shard, wave):
        push(tab.at[shard], tab.at[shard], 1, lent.at[wave], sibling)

    def turn(shard):
        values = tab[shard, :, FREQ_AT : FREQ_AT + LANES].astype(jnp.float32)
        for j in range(3):
            stack = []
            for g in range(4):
                stack.append(tab[shard, :, GROUP_AT[g] + 256 * j : GROUP_AT[g] + 256 * (j + 1)].astype(jnp.float32))
                at_row = 6 * g + 2 * j
                stack.append(
                    jnp.concatenate(
                        [jnp.broadcast_to(values[at_row + h : at_row + h + 1, :], (8, LANES)) for h in range(2)], axis=1
                    )
                )
            stack = jnp.concatenate(stack, axis=0).astype(jnp.bfloat16)
            table[pl.ds(pl.multiple_of(shard * GROUP + 256 * j, 256), 256), :] = lax.dot_general(
                eye[...], stack, NT, preferred_element_type=jnp.float32
            )

    @pl.when(relays)
    def _():
        for axis in (0, 1):
            for way in (1, -1):
                for part in (0, 1):
                    relay(way, part, 0, 0, axis, 1)
                    relay(way, part, 0, 0, axis, -1)
        push(dealt.at[1], dealt.at[1], 2, dealt_sem.at[0], sibling)
        push(mine.at[1], mine.at[1], 3, dealt_sem.at[1], sibling)

    turn(pb)
    copy_lengths = pltpu.make_async_copy(lengths_v, lengths, local.at[0])

    def position(chip, source):
        return ((chip + source) & 3) + (chip & 4)

    def blocks_in():
        held = blocks[...]
        modes = jnp.maximum(held, 0)
        local_mode = lax.broadcasted_iota(jnp.int32, modes.shape, 3) == 0
        packed[:, :, :, 0:4] = held
        packed[:, :, :, 4:8] = rows_of(modes + jnp.where(local_mode, pb * LOCAL, 0))
        lane = lax.broadcasted_iota(jnp.int32, (CHIPS, 2, 1, LANES), 3)
        source = lax.broadcasted_iota(jnp.int32, (CHIPS, 2, 1, LANES), 0)
        length = jnp.zeros((CHIPS, 2, 1, LANES), jnp.int32)
        for high in range(4):
            last = jnp.max(jnp.where(held[:, :, high, 1:2] >= 0, lane + 1, 0), axis=3, keepdims=True)
            used = position(z, source) + 8 * high < tallies[...]
            length = jnp.where((lane == high) & used, last, length)
        lengths_v[...] = length

    @pl.when(relays)
    def _():
        for number, (first, second) in enumerate(ORDER):
            bytes_in(tab.at[0], got.at[number])
            if second == 0 and first == -1:
                for way in (1, -1):
                    for part in (0, 1):
                        relay(way, part, first, 0, 0, 1)
            if second in (0, -1):
                for way in (1, -1):
                    for part in (0, 1):
                        relay(way, part, first, second, 1, 1)
                        if second == 0:
                            relay(way, part, first, second, 1, -1)
            for wave in LEND_AFTER.get(number, ()):
                for offset in WAVES[wave]:
                    lend(place(*offset), wave)
            if number == len(ORDER) - 1:
                copy_lengths.start()
            for offset in TURN_AFTER.get(number, ()):
                turn(place(*offset))
            if number == 12:
                bytes_in(blocks, dealt_sem.at[2])
                bytes_in(tallies, dealt_sem.at[3])
                blocks_in()
        bytes_out(tab.at[pl.ds(0, 15)], 0)
        bytes_out(tab.at[pl.ds(0, 15)], 1)
        bytes_out(dealt.at[1], 2)
        bytes_out(mine.at[1], 3)

    @pl.when(jnp.logical_not(relays))
    def _():
        bytes_in(dealt.at[1], dealt_sem.at[0])
        bytes_in(mine.at[1], dealt_sem.at[1])
        for k, dealer in enumerate(dealers):
            push(dealt.at[:, :, position(lax.rem(z + k + 1, CHIPS), z)], blocks.at[z], 2, dealt_sem.at[2], dealer)
            push(mine, tallies.at[z], 3, dealt_sem.at[3], dealer)
        blocks[z] = dealt[:, :, position(z, z)]
        tallies[z] = mine[...]
        for wave, members in enumerate(WAVES):
            if wave == 1:
                bytes_in(blocks.at[pl.ds(0, CHIPS - 1)], dealt_sem.at[2])
                bytes_in(tallies.at[pl.ds(0, CHIPS - 1)], dealt_sem.at[3])
                push(blocks, blocks, 0, dealt_sem.at[2], sibling)
                push(tallies, tallies, 1, dealt_sem.at[3], sibling)
                blocks_in()
            bytes_in(tab.at[pl.ds(0, len(members))], lent.at[wave])
            if wave == 2:
                copy_lengths.start()
            for offset in members:
                turn(place(*offset))
        bytes_out(blocks.at[pl.ds(0, CHIPS - 1)], 2)
        bytes_out(tallies.at[pl.ds(0, CHIPS - 1)], 3)
        bytes_out(blocks, 0)
        bytes_out(tallies, 1)

    copy_phi.wait()
    copy_cells.wait()
    copy_lengths.wait()

def exchange(eig, freq, quartets, phi, cells, counts):
    hbm = pl.BlockSpec(memory_space=pltpu.HBM)
    vmem = pl.BlockSpec(memory_space=pltpu.VMEM)
    return pl.pallas_call(
        exchange_kernel,
        out_shape=(
            pltpu.VMEM((NB * GROUP, LANES), jnp.float32),
            pltpu.VMEM((CHIPS, 2, 4, 8, LANES), jnp.int32),
            pltpu.SMEM((CHIPS, 2, 1, LANES), jnp.int32),
            pltpu.VMEM((144, 1152), jnp.bfloat16),
            pltpu.VMEM((8, 9), jnp.int32),
            pltpu.VMEM((128, 128), jnp.bfloat16),
            pltpu.VMEM((576, 64), jnp.bfloat16),
        ),
        in_specs=[hbm] * 5 + [pl.BlockSpec(memory_space=pltpu.SMEM)],
        out_specs=(vmem, vmem, pl.BlockSpec(memory_space=pltpu.SMEM), vmem, vmem, vmem, vmem),
        scratch_shapes=[
            pltpu.VMEM((CHIPS, 2, 4, 4, LANES), jnp.int32),
            pltpu.VMEM((CHIPS, 2, 1, LANES), jnp.int32),
            pltpu.VMEM((CHIPS, 2, 1, LANES), jnp.int32),
            pltpu.VMEM((NB, 24, WIDTH), jnp.bfloat16),
            pltpu.VMEM((2, 1, LANES), jnp.int32),
            pltpu.VMEM((256, 256), jnp.bfloat16),
            pltpu.VMEM((2, 4, 8, 4, LANES), jnp.int32),
            pltpu.SemaphoreType.DMA((4,)),
            pltpu.SemaphoreType.DMA((len(ORDER),)),
            pltpu.SemaphoreType.DMA((len(WAVES),)),
            pltpu.SemaphoreType.DMA((4,)),
            pltpu.SemaphoreType.DMA((6,)),
        ],
        compiler_params=pltpu.CompilerParams(collective_id=0, has_side_effects=True, vmem_limit_bytes=24 << 20),
        name="exchange",
    )(*[pltpu.with_memory_space_constraint(a, pltpu.HBM) for a in (eig, freq, quartets, phi, cells)], counts)


def cosine_of(step):
    near = jnp.minimum(step, 16 - step)
    out = jnp.full(step.shape, -1.0, jnp.float32)
    for k in range(8):
        out = jnp.where(near == k, math.cos(math.pi * k / 8) if k != 4 else 0.0, out)
    return out


def floor_div(value, by):
    return jnp.floor((value.astype(jnp.float32) + 0.5) * (1.0 / by)).astype(jnp.int32)


def rows_of(modes):
    unit = floor_div(modes, GROUP)
    return (unit >> 2) * GROUP + modes - unit * GROUP


def quartet_kernel(
    table, packed, lengths, phi, cells, reorder, spread, out,
    wide_a, wide_b, near_a, near_b, scale_a, scale_b, term_a, term_b, freqs_a, freqs_b, vectors_a, vectors_b, held_a, held_b,
    rows_a, rows_b, dense, sums, sem,
):
    pb, wa = lax.axis_index("pb"), lax.axis_index("wa")

    lane8 = lax.broadcasted_iota(jnp.int32, (8, LANES), 1)
    count = jnp.int32(0)
    current = jnp.zeros((8, LANES), jnp.int32)
    for source in range(CHIPS):
        for slot in range(8):
            length = lengths[source, slot // 4, 0, slot % 4]
            offset = count & (LANES - 1)
            rolled = pltpu.roll(packed[source, slot // 4, slot % 4], offset, 1)
            current = jnp.where(lane8 >= offset, rolled, current)
            dense[count >> 7] = current
            current = jnp.where(offset + length >= LANES, rolled, current)
            count = count + length
    filled = (count + LANES - 1) >> 7
    dense[count >> 7] = current
    for k in range(6):
        dense[filled + k] = jnp.zeros((8, LANES), jnp.int32)
    half = (filled + 1) >> 1
    begin = (wa & 1) * half
    total = jnp.where((wa & 1) == 0, half, filled - half)

    sums[...] = jnp.zeros_like(sums)
    cell = cells[...].astype(jnp.float32)

    def fetch(index, into, which):
        return pltpu.make_async_copy(dense.at[begin + index, pl.ds(4, 4)], into, sem.at[which])

    sublane = lax.broadcasted_iota(jnp.int32, (8, LANES), 0)
    odd = [(sublane & (1 << bit)) != 0 for bit in range(3)]

    def gather(into, at):
        for k in range(4):
            for n in range(0, LANES, 16):
                pair = []
                for half in (n, n + 8):
                    level = [table[pl.ds(at[k, half + j], 8, stride=0), :] for j in range(8)]
                    for bit in range(3):
                        level = [jnp.where(odd[bit], high, low) for low, high in zip(level[::2], level[1::2])]
                    pair.append(level[0])
                into[LANES * k + n : LANES * k + n + 16, :] = jnp.concatenate(pair, axis=0).astype(jnp.bfloat16)

    def vectors_of(at, index, held, vectors, freqs_of):
        gather(held, at)
        raw = dense[begin + index][0:4]
        modes = jnp.maximum(raw, 0)
        fullmode = modes + jnp.where(lax.broadcasted_iota(jnp.int32, modes.shape, 0) == 0, pb * LOCAL, 0)
        group = floor_div(fullmode, GROUP) & 3
        turned = lax.dot_general(reorder[...], held[...], NT, preferred_element_type=jnp.float32)
        halves, freqs = [], []
        for k in range(4):
            which = group[k : k + 1, :]
            part = turned[:, LANES * k : LANES * (k + 1)]
            mine = jnp.where(
                which < 2,
                jnp.where(which == 0, part[0:32], part[32:64]),
                jnp.where(which == 2, part[64:96], part[96:128]),
            )
            halves.append(jnp.concatenate([mine[0:16], mine[16:32]], axis=1))
            freqs.append(mine[12:13])
        vectors[...] = jnp.concatenate(halves, axis=0).astype(jnp.bfloat16)
        freqs_of[...] = jnp.concatenate(freqs, axis=0)

    def products(index, vectors, freqs_of, wide, near, scale):
        raw = dense[begin + index][0:4]
        modes = jnp.maximum(raw, 0)
        pairs = jnp.dot(spread[...], vectors[...], preferred_element_type=jnp.float32)
        third, fourth, e1, e2 = (pairs[144 * k : 144 * (k + 1)] for k in range(4))
        far_re = third[:, :LANES] * fourth[:, :LANES] - third[:, LANES:] * fourth[:, LANES:]
        far_im = -(third[:, :LANES] * fourth[:, LANES:] + third[:, LANES:] * fourth[:, :LANES])
        near[0:144] = e1[:, :LANES] * e2[:, :LANES] - e1[:, LANES:] * e2[:, LANES:]
        near[144:288] = e1[:, :LANES] * e2[:, LANES:] + e1[:, LANES:] * e2[:, :LANES]

        point = floor_div(modes, BR)
        coords = [(point >> 8).astype(jnp.float32), ((point >> 4) & 15).astype(jnp.float32), (point & 15).astype(jnp.float32)]
        shift = jnp.zeros((8, LANES), jnp.float32)
        for which in range(3):
            for axis in range(3):
                column = cell[:, 3 * which + axis : 3 * which + axis + 1]
                term = column * coords[axis][which + 1 : which + 2, :]
                shift = shift + term if which == 0 else shift - term
        step = shift.astype(jnp.int32) & 15
        cosine, sine = cosine_of(step), cosine_of((step - 4) & 15)
        for k in range(8):
            c, s = cosine[k : k + 1, :], sine[k : k + 1, :]
            wide[144 * k : 144 * (k + 1), :LANES] = (c * far_re - s * far_im).astype(jnp.bfloat16)
            wide[144 * k : 144 * (k + 1), LANES:] = (c * far_im + s * far_re).astype(jnp.bfloat16)

        freqs = [freqs_of[k : k + 1] for k in range(4)]
        occupied = [1.0 / (jnp.exp(f) - 1.0) for f in freqs]
        mismatch = freqs[0] + freqs[1] - freqs[2] - freqs[3]
        delta = jnp.exp(-((mismatch / SMEARING) ** 2)) / (SMEARING * math.sqrt(math.pi))
        weight = (1.0 + occupied[1]) * occupied[2] * occupied[3] / occupied[0]
        product = freqs[0] * freqs[1] * freqs[2] * freqs[3]
        number = LANES * (begin + index) + lax.broadcasted_iota(jnp.int32, (1, LANES), 1)
        valid = (raw[1:2, :] >= 0) & (number < count)
        scale[...] = jnp.where(valid, delta * weight / product, 0.0)

    def contract(wide, near, scale, term):
        weighted = jnp.dot(phi[...], wide[...], preferred_element_type=jnp.float32)
        w_re, w_im = weighted[:, :LANES], weighted[:, LANES:]
        near_re, near_im = near[0:144], near[144:288]
        value_re = jnp.sum(near_re * w_re - near_im * w_im, axis=0, keepdims=True)
        value_im = jnp.sum(near_re * w_im + near_im * w_re, axis=0, keepdims=True)
        term[...] = (value_re * value_re + value_im * value_im) * scale[...]

    def scatter(index, term):
        first = jnp.maximum(dense[begin + index][0:1, :], 0)
        high = floor_div(first, 192)
        low = first - 192 * high
        placed = jnp.where(lax.broadcasted_iota(jnp.int32, (NB, LANES), 0) == high, term, 0.0)
        one = placed.astype(jnp.bfloat16)
        rest = placed - one.astype(jnp.float32)
        two = rest.astype(jnp.bfloat16)
        three = (rest - two.astype(jnp.float32)).astype(jnp.bfloat16)
        spot = jnp.where(lax.broadcasted_iota(jnp.int32, (256, LANES), 0) == low, 1.0, 0.0).astype(jnp.bfloat16)
        sums[...] += lax.dot_general(
            jnp.concatenate([one, two, three], axis=0), spot, NT, preferred_element_type=jnp.float32
        )

    sides = (
        (rows_a, held_a, vectors_a, freqs_a, scale_a, wide_a, near_a, term_a, 0),
        (rows_b, held_b, vectors_b, freqs_b, scale_b, wide_b, near_b, term_b, 1),
    )

    def step_of(i, side):
        at, held, vectors, freqs_of, scale, wide, near, term, which = sides[side]
        _, _, next_vectors, next_freqs, next_scale, next_wide, next_near, last_term, _ = sides[1 - side]
        fetch(i + 2, at, which).wait()
        scatter(jnp.maximum(i - 1, 0), last_term[...])
        contract(wide, near, scale, term)
        products(i + 1, next_vectors, next_freqs, next_wide, next_near, next_scale)
        vectors_of(at, i + 2, held, vectors, freqs_of)
        fetch(i + 4, at, which).start()

    term_b[...] = jnp.zeros_like(term_b)
    fetch(0, rows_a, 0).start()
    fetch(1, rows_b, 1).start()
    fetch(0, rows_a, 0).wait()
    vectors_of(rows_a, 0, held_a, vectors_a, freqs_a)
    fetch(2, rows_a, 0).start()
    fetch(1, rows_b, 1).wait()
    products(0, vectors_a, freqs_a, wide_a, near_a, scale_a)
    vectors_of(rows_b, 1, held_b, vectors_b, freqs_b)
    fetch(3, rows_b, 1).start()

    def two_blocks(it, carry):
        step_of(2 * it, 0)

        @pl.when(2 * it + 1 < total)
        def _():
            step_of(2 * it + 1, 1)

        return carry

    lax.fori_loop(0, (total + 1) // 2, two_blocks, 0)
    scatter(jnp.maximum(total - 1, 0), jnp.where(total % 2 == 1, term_a[...], term_b[...]))
    fetch(0, rows_a, 0).wait()
    fetch(0, rows_b, 1).wait()
    result = sums[0:16] + sums[16:32] + sums[32:48]
    for w in range(NB):
        out[w] = result[w : w + 1]


def quartet_sums(*operands):
    vmem = pl.BlockSpec(memory_space=pltpu.VMEM)
    smem = pl.BlockSpec(memory_space=pltpu.SMEM)
    pinned = [pltpu.with_memory_space_constraint(a, pltpu.SMEM if k == 2 else pltpu.VMEM) for k, a in enumerate(operands)]
    return pl.pallas_call(
        quartet_kernel,
        out_shape=pltpu.VMEM((NB, 1, 256), jnp.float32),
        in_specs=[vmem, vmem, smem, vmem, vmem, vmem, vmem],
        out_specs=vmem,
        scratch_shapes=[
            pltpu.VMEM((1152, 256), jnp.bfloat16),
            pltpu.VMEM((1152, 256), jnp.bfloat16),
            pltpu.VMEM((288, LANES), jnp.float32),
            pltpu.VMEM((288, LANES), jnp.float32),
            pltpu.VMEM((1, LANES), jnp.float32),
            pltpu.VMEM((1, LANES), jnp.float32),
            pltpu.VMEM((1, LANES), jnp.float32),
            pltpu.VMEM((1, LANES), jnp.float32),
            pltpu.VMEM((4, LANES), jnp.float32),
            pltpu.VMEM((4, LANES), jnp.float32),
            pltpu.VMEM((64, 256), jnp.bfloat16),
            pltpu.VMEM((64, 256), jnp.bfloat16),
            pltpu.VMEM((4 * LANES, LANES), jnp.bfloat16),
            pltpu.VMEM((4 * LANES, LANES), jnp.bfloat16),
            pltpu.SMEM((4, LANES), jnp.int32),
            pltpu.SMEM((4, LANES), jnp.int32),
            pltpu.VMEM((4 * NB + 8, 8, LANES), jnp.int32),
            pltpu.VMEM((48, 256), jnp.float32),
            pltpu.SemaphoreType.DMA((2,)),
        ],
        compiler_params=pltpu.CompilerParams(
            vmem_limit_bytes=16 << 20
        ),
        name="quartets",
    )(*pinned)


def reduce_kernel(part, out, arrived, send, recv):
    pb, wa = lax.axis_index("pb"), lax.axis_index("wa")
    barrier = pltpu.get_barrier_semaphore()
    peers = [lax.rem(wa + k, NB) for k in range(1, NB)]
    for peer in peers:
        pl.semaphore_signal(barrier, inc=1, device_id=(pb, peer), device_id_type=MESH)
    pl.semaphore_wait(barrier, NB - 1)
    for k, peer in enumerate(peers):
        pltpu.make_async_remote_copy(
            src_ref=part.at[peer], dst_ref=arrived.at[k], send_sem=send.at[0], recv_sem=recv.at[0],
            device_id=(pb, peer), device_id_type=MESH,
        ).start()
    everything = pltpu.make_async_remote_copy(
        src_ref=part.at[pl.ds(0, NB - 1)], dst_ref=arrived, send_sem=send.at[0], recv_sem=recv.at[0],
        device_id=(pb, peers[0]), device_id_type=MESH,
    )
    everything.wait_recv()
    total = part[wa]
    for k in range(NB - 1):
        total = total + arrived[k]
    out[...] = total
    everything.wait_send()


def reduce_over_wa(part):
    vmem = pl.BlockSpec(memory_space=pltpu.VMEM)
    return pl.pallas_call(
        reduce_kernel,
        out_shape=jax.ShapeDtypeStruct((1, 256), jnp.float32),
        in_specs=[vmem],
        out_specs=vmem,
        scratch_shapes=[
            pltpu.VMEM((NB - 1, 1, 256), jnp.float32),
            pltpu.SemaphoreType.DMA((1,)),
            pltpu.SemaphoreType.DMA((1,)),
        ],
        compiler_params=pltpu.CompilerParams(collective_id=1, has_side_effects=True, vmem_limit_bytes=1 << 20),
        name="reduce_wa",
    )(pltpu.with_memory_space_constraint(part, pltpu.VMEM))


def body(quartets, counts, eig, freq, phi, cells):
    dealt = quartets.reshape(4, 8, 4, LANES)
    held = exchange(eig, freq.reshape(24, LANES), dealt, phi, cells, counts)
    part = quartet_sums(*held)
    return reduce_over_wa(part)[0, :192]


def solution(mesh):
    placed = (P(("pb", "wa"), None, None), P(("pb", "wa")), P(None, "pb"), P("pb"), P(), P())
    return jax.shard_map(body, mesh=mesh, in_specs=placed, out_specs=P(("pb", "wa")), check_vma=False)
```

```python
import functools
import math

import jax
import jax.numpy as jnp
from jax import lax
from jax.experimental import pallas as pl
from jax.experimental.pallas import tpu as pltpu
from jax.sharding import PartitionSpec as P

QMESH = 16
BR = 12
NB = 16
LOCAL = 3072
GROUP = 768
LANES = 128
GROUP_AT = (0, 768, 1664, 2432)
FREQ_AT = 1536
WIDTH = 3200
SMEARING = 0.5
MESH = pl.DeviceIdType.MESH
NT = (((1,), (1,)), ((), ()))


PIECES = {(1, 0): (0, 768), (1, 1): (768, 896), (-1, 1): (1664, 768), (-1, 0): (2432, 768)}
RELAY_CORE = 1
CHIPS = 8
ORDER = (
    (-1, 0), (1, 0), (0, -1), (0, 1), (2, 0), (-1, -1), (-1, 1), (0, 2), (1, -1), (1, 1), (-1, 2), (2, -1), (2, 1), (1, 2), (2, 2),
)
WAVES = (
    ((-1, 0), (1, 0), (0, -1), (0, 1)),
    ((2, 0), (0, 2)),
    ((-1, 1), (1, -1)),
    ((-1, -1), (1, 1)),
    ((-1, 2), (2, -1), (2, 1), (1, 2)),
    ((2, 2),),
)
LEND_AFTER = {3: (0,), 7: (1,), 8: (2,), 9: (3,), 13: (4,), 14: (5,)}
TURN_AFTER = {
    4: ((-1, 0),), 5: ((1, 0),), 6: ((0, -1),), 7: ((0, 1),), 8: ((2, 0),), 9: ((0, 2),), 10: ((-1, 1),),
    11: ((1, -1), (-1, -1), (1, 1)), 14: ((-1, 2), (2, -1), (2, 1), (1, 2), (2, 2)),
}


def wrapped(offset):
    return (offset + 1) % 4 - 1


def hit(rows, columns, where):
    r = lax.broadcasted_iota(jnp.int32, (rows, columns), 0)
    c = lax.broadcasted_iota(jnp.int32, (rows, columns), 1)
    return jnp.where(where(r) == c, 1.0, 0.0).astype(jnp.bfloat16)


def spread_column(r):
    kind = floor_div(r, 144)
    t = r - 144 * kind
    first = floor_div(t, BR)
    return ((kind + 2) & 3) * 16 + jnp.where((kind & 1) == 0, first, t - BR * first)


def order_column(r):
    t = r & 31
    lane = jnp.where(t < 12, t, jnp.where(t == 12, 24, jnp.where((t >= 16) & (t < 28), t - 4, -999)))
    return lane + (r - t)


def exchange_kernel(
    eig, freq, quartets, phi, cells, counts,
    table, packed, lengths, phi_v, cells_v, reorder, spread,
    blocks, tallies, lengths_v, tab, mine, eye, dealt, send, got, lent, dealt_sem, local,
):
    pb, wa = lax.axis_index("pb"), lax.axis_index("wa")
    x, y, z, core = pb // 4, pb % 4, wa // 2, wa % 2
    relays = core == RELAY_CORE
    sibling = (pb, wa + 1 - 2 * core)
    dealers = [(pb, 2 * lax.rem(z + k, CHIPS)) for k in range(1, CHIPS)]

    def place(dx, dy):
        return lax.rem(x + dx + 4, 4) * 4 + lax.rem(y + dy + 4, 4)

    left = pltpu.make_async_copy(eig.at[:, pl.ds(0, 1536)], tab.at[pb, :, pl.ds(0, 1536)], local.at[0])
    right = pltpu.make_async_copy(eig.at[:, pl.ds(1536, 1536)], tab.at[pb, :, pl.ds(1664, 1536)], local.at[1])
    copy_freq = pltpu.make_async_copy(freq, tab.at[pb, :, pl.ds(FREQ_AT, LANES)], local.at[2])
    copy_dealt = pltpu.make_async_copy(quartets, dealt.at[core], local.at[3])
    copy_phi = pltpu.make_async_copy(phi, phi_v, local.at[4])
    copy_cells = pltpu.make_async_copy(cells, cells_v, local.at[5])
    first_copies = (left, right, copy_freq, copy_dealt)
    for copy in first_copies + (copy_phi, copy_cells):
        copy.start()
    barrier = pltpu.get_barrier_semaphore()
    pl.semaphore_signal(barrier, inc=1, device_id=sibling, device_id_type=MESH)

    @pl.when(relays)
    def _():
        for step in (1, -1):
            pl.semaphore_signal(barrier, inc=1, device_id=(place(step, 0), wa), device_id_type=MESH)
            pl.semaphore_signal(barrier, inc=1, device_id=(place(0, step), wa), device_id_type=MESH)

    @pl.when(jnp.logical_not(relays))
    def _():
        for dealer in dealers:
            pl.semaphore_signal(barrier, inc=1, device_id=dealer, device_id_type=MESH)

    mine[core] = jnp.full((1, LANES), counts[0], jnp.int32)
    eye[...] = hit(256, 256, lambda r: r)
    reorder[...] = hit(LANES, LANES, order_column)
    spread[...] = hit(576, 64, spread_column)
    for copy in first_copies:
        copy.wait()

    pl.semaphore_wait(barrier, jnp.where(relays, 5, CHIPS))

    def push(src, dst, sent, arrival, device):
        pltpu.make_async_remote_copy(
            src_ref=src, dst_ref=dst, send_sem=send.at[sent], recv_sem=arrival, device_id=device, device_id_type=MESH
        ).start()

    def bytes_in(view, sem):
        pltpu.make_async_remote_copy(
            src_ref=view, dst_ref=view, send_sem=send.at[0], recv_sem=sem, device_id=sibling, device_id_type=MESH
        ).wait_recv()

    def bytes_out(view, sent):
        pltpu.make_async_remote_copy(
            src_ref=view, dst_ref=view, send_sem=send.at[sent], recv_sem=got.at[0], device_id=sibling, device_id_type=MESH
        ).wait_send()

    def at(way, part, first, second):
        return place(way * first, way * second) if part == 0 else place(way * second, way * first)

    def relay(way, part, first, second, axis, step):
        start, width = PIECES[way, part]
        view = tab.at[at(way, part, first, second), :, pl.ds(start, width)]
        key = (wrapped(first - step), second) if axis == 0 else (first, wrapped(second - step))
        target = at(way, part, step, 0) if axis == 0 else at(way, part, 0, step)
        push(view, view, 0, got.at[ORDER.index(key)], (target, wa))

    def lend(shard, wave):
        push(tab.at[shard], tab.at[shard], 1, lent.at[wave], sibling)

    def turn(shard):
        values = tab[shard, :, FREQ_AT : FREQ_AT + LANES].astype(jnp.float32)
        for j in range(3):
            stack = []
            for g in range(4):
                stack.append(tab[shard, :, GROUP_AT[g] + 256 * j : GROUP_AT[g] + 256 * (j + 1)].astype(jnp.float32))
                at_row = 6 * g + 2 * j
                stack.append(
                    jnp.concatenate(
                        [jnp.broadcast_to(values[at_row + h : at_row + h + 1, :], (8, LANES)) for h in range(2)], axis=1
                    )
                )
            stack = jnp.concatenate(stack, axis=0).astype(jnp.bfloat16)
            table[pl.ds(pl.multiple_of(shard * GROUP + 256 * j, 256), 256), :] = lax.dot_general(
                eye[...], stack, NT, preferred_element_type=jnp.float32
            )

    @pl.when(relays)
    def _():
        for axis in (0, 1):
            for way in (1, -1):
                for part in (0, 1):
                    relay(way, part, 0, 0, axis, 1)
                    relay(way, part, 0, 0, axis, -1)
        push(dealt.at[1], dealt.at[1], 2, dealt_sem.at[0], sibling)
        push(mine.at[1], mine.at[1], 3, dealt_sem.at[1], sibling)

    turn(pb)
    copy_lengths = pltpu.make_async_copy(lengths_v, lengths, local.at[0])

    def deal(chip, source):
        return chip >> 2, (chip + source) & 3

    def dealt_to(chip):
        half, p = deal(chip, z)
        return dealt.at[:, :, half, :, p]

    def blocks_in():
        held = blocks[...]
        modes = jnp.maximum(held, 0)
        local_mode = lax.broadcasted_iota(jnp.int32, modes.shape, 4) == 0
        packed[:, :, :, :, 0:4] = held
        packed[:, :, :, :, 4:8] = rows_of(modes + jnp.where(local_mode, pb * LOCAL, 0))
        lane = lax.broadcasted_iota(jnp.int32, (CHIPS, 2, 1, LANES), 3)
        source = lax.broadcasted_iota(jnp.int32, (CHIPS, 2, 1, LANES), 0)
        length = jnp.zeros((CHIPS, 2, 1, LANES), jnp.int32)
        half, p = deal(z, source)
        for high in range(4):
            last = jnp.max(jnp.where(held[:, :, high >> 1, high & 1, 1:2] >= 0, lane + 1, 0), axis=3, keepdims=True)
            used = p + 16 * (high >> 1) + 8 * half + 4 * (high & 1) < tallies[...]
            length = jnp.where((lane == high) & used, last, length)
        lengths_v[...] = length

    @pl.when(relays)
    def _():
        for number, (first, second) in enumerate(ORDER):
            bytes_in(tab.at[0], got.at[number])
            if second == 0 and first == -1:
                for way in (1, -1):
                    for part in (0, 1):
                        relay(way, part, first, 0, 0, 1)
            if second in (0, -1):
                for way in (1, -1):
                    for part in (0, 1):
                        relay(way, part, first, second, 1, 1)
                        if second == 0:
                            relay(way, part, first, second, 1, -1)
            for wave in LEND_AFTER.get(number, ()):
                for offset in WAVES[wave]:
                    lend(place(*offset), wave)
            if number == len(ORDER) - 1:
                copy_lengths.start()
            for offset in TURN_AFTER.get(number, ()):
                turn(place(*offset))
            if number == 12:
                bytes_in(blocks, dealt_sem.at[2])
                bytes_in(tallies, dealt_sem.at[3])
                blocks_in()
        bytes_out(tab.at[pl.ds(0, 15)], 0)
        bytes_out(tab.at[pl.ds(0, 15)], 1)
        bytes_out(dealt.at[1], 2)
        bytes_out(mine.at[1], 3)

    @pl.when(jnp.logical_not(relays))
    def _():
        bytes_in(dealt.at[1], dealt_sem.at[0])
        bytes_in(mine.at[1], dealt_sem.at[1])
        for k, dealer in enumerate(dealers):
            push(dealt_to(lax.rem(z + k + 1, CHIPS)), blocks.at[z], 2, dealt_sem.at[2], dealer)
            push(mine, tallies.at[z], 3, dealt_sem.at[3], dealer)
        blocks[z] = dealt_to(z)[...]
        tallies[z] = mine[...]
        for wave, members in enumerate(WAVES):
            if wave == 1:
                bytes_in(blocks.at[pl.ds(0, CHIPS - 1)], dealt_sem.at[2])
                bytes_in(tallies.at[pl.ds(0, CHIPS - 1)], dealt_sem.at[3])
                push(blocks, blocks, 0, dealt_sem.at[2], sibling)
                push(tallies, tallies, 1, dealt_sem.at[3], sibling)
                blocks_in()
            bytes_in(tab.at[pl.ds(0, len(members))], lent.at[wave])
            if wave == 2:
                copy_lengths.start()
            for offset in members:
                turn(place(*offset))
        bytes_out(blocks.at[pl.ds(0, CHIPS - 1)], 2)
        bytes_out(tallies.at[pl.ds(0, CHIPS - 1)], 3)
        bytes_out(blocks, 0)
        bytes_out(tallies, 1)

    copy_phi.wait()
    copy_cells.wait()
    copy_lengths.wait()

def exchange(eig, freq, quartets, phi, cells, counts):
    hbm = pl.BlockSpec(memory_space=pltpu.HBM)
    vmem = pl.BlockSpec(memory_space=pltpu.VMEM)
    return pl.pallas_call(
        exchange_kernel,
        out_shape=(
            pltpu.VMEM((NB * GROUP, LANES), jnp.float32),
            pltpu.VMEM((CHIPS, 2, 2, 2, 8, LANES), jnp.int32),
            pltpu.SMEM((CHIPS, 2, 1, LANES), jnp.int32),
            pltpu.VMEM((144, 1152), jnp.bfloat16),
            pltpu.VMEM((8, 9), jnp.int32),
            pltpu.VMEM((128, 128), jnp.bfloat16),
            pltpu.VMEM((576, 64), jnp.bfloat16),
        ),
        in_specs=[hbm] * 5 + [pl.BlockSpec(memory_space=pltpu.SMEM)],
        out_specs=(vmem, vmem, pl.BlockSpec(memory_space=pltpu.SMEM), vmem, vmem, vmem, vmem),
        scratch_shapes=[
            pltpu.VMEM((CHIPS, 2, 2, 2, 4, LANES), jnp.int32),
            pltpu.VMEM((CHIPS, 2, 1, LANES), jnp.int32),
            pltpu.VMEM((CHIPS, 2, 1, LANES), jnp.int32),
            pltpu.VMEM((NB, 24, WIDTH), jnp.bfloat16),
            pltpu.VMEM((2, 1, LANES), jnp.int32),
            pltpu.VMEM((256, 256), jnp.bfloat16),
            pltpu.VMEM((2, 2, 2, 2, 4, 4, LANES), jnp.int32),
            pltpu.SemaphoreType.DMA((4,)),
            pltpu.SemaphoreType.DMA((len(ORDER),)),
            pltpu.SemaphoreType.DMA((len(WAVES),)),
            pltpu.SemaphoreType.DMA((4,)),
            pltpu.SemaphoreType.DMA((6,)),
        ],
        compiler_params=pltpu.CompilerParams(collective_id=0, has_side_effects=True, vmem_limit_bytes=24 << 20),
        name="exchange",
    )(*[pltpu.with_memory_space_constraint(a, pltpu.HBM) for a in (eig, freq, quartets, phi, cells)], counts)


def cosine_of(step):
    near = jnp.minimum(step, 16 - step)
    out = jnp.full(step.shape, -1.0, jnp.float32)
    for k in range(8):
        out = jnp.where(near == k, math.cos(math.pi * k / 8) if k != 4 else 0.0, out)
    return out


def floor_div(value, by):
    return jnp.floor((value.astype(jnp.float32) + 0.5) * (1.0 / by)).astype(jnp.int32)


def rows_of(modes):
    unit = floor_div(modes, GROUP)
    return (unit >> 2) * GROUP + modes - unit * GROUP


def quartet_kernel(
    table, packed, lengths, phi, cells, reorder, spread, out,
    wide_a, wide_b, near_a, near_b, scale_a, scale_b, term_a, term_b, freqs_a, freqs_b, vectors_a, vectors_b, held_a, held_b,
    rows_a, rows_b, dense, sums, sem,
):
    pb, wa = lax.axis_index("pb"), lax.axis_index("wa")

    lane8 = lax.broadcasted_iota(jnp.int32, (8, LANES), 1)
    count = jnp.int32(0)
    current = jnp.zeros((8, LANES), jnp.int32)
    for source in range(CHIPS):
        for slot in range(8):
            length = lengths[source, slot // 4, 0, slot % 4]
            offset = count & (LANES - 1)
            rolled = pltpu.roll(packed[source, slot // 4, slot % 4 // 2, slot % 2], offset, 1)
            current = jnp.where(lane8 >= offset, rolled, current)
            dense[count >> 7] = current
            current = jnp.where(offset + length >= LANES, rolled, current)
            count = count + length
    filled = (count + LANES - 1) >> 7
    dense[count >> 7] = current
    for k in range(6):
        dense[filled + k] = jnp.zeros((8, LANES), jnp.int32)
    half = (filled + 1) >> 1
    begin = (wa & 1) * half
    total = jnp.where((wa & 1) == 0, half, filled - half)

    sums[...] = jnp.zeros_like(sums)
    cell = cells[...].astype(jnp.float32)

    def fetch(index, into, which):
        return pltpu.make_async_copy(dense.at[begin + index, pl.ds(4, 4)], into, sem.at[which])

    sublane = lax.broadcasted_iota(jnp.int32, (8, LANES), 0)
    odd = [(sublane & (1 << bit)) != 0 for bit in range(3)]

    def gather(into, at):
        for k in range(4):
            for n in range(0, LANES, 16):
                pair = []
                for half in (n, n + 8):
                    level = [table[pl.ds(at[k, half + j], 8, stride=0), :] for j in range(8)]
                    for bit in range(3):
                        level = [jnp.where(odd[bit], high, low) for low, high in zip(level[::2], level[1::2])]
                    pair.append(level[0])
                into[LANES * k + n : LANES * k + n + 16, :] = jnp.concatenate(pair, axis=0).astype(jnp.bfloat16)

    def vectors_of(at, index, held, vectors, freqs_of):
        gather(held, at)
        raw = dense[begin + index][0:4]
        modes = jnp.maximum(raw, 0)
        fullmode = modes + jnp.where(lax.broadcasted_iota(jnp.int32, modes.shape, 0) == 0, pb * LOCAL, 0)
        group = floor_div(fullmode, GROUP) & 3
        turned = lax.dot_general(reorder[...], held[...], NT, preferred_element_type=jnp.float32)
        halves, freqs = [], []
        for k in range(4):
            which = group[k : k + 1, :]
            part = turned[:, LANES * k : LANES * (k + 1)]
            mine = jnp.where(
                which < 2,
                jnp.where(which == 0, part[0:32], part[32:64]),
                jnp.where(which == 2, part[64:96], part[96:128]),
            )
            halves.append(jnp.concatenate([mine[0:16], mine[16:32]], axis=1))
            freqs.append(mine[12:13])
        vectors[...] = jnp.concatenate(halves, axis=0).astype(jnp.bfloat16)
        freqs_of[...] = jnp.concatenate(freqs, axis=0)

    def products(index, vectors, freqs_of, wide, near, scale):
        raw = dense[begin + index][0:4]
        modes = jnp.maximum(raw, 0)
        pairs = jnp.dot(spread[...], vectors[...], preferred_element_type=jnp.float32)
        third, fourth, e1, e2 = (pairs[144 * k : 144 * (k + 1)] for k in range(4))
        far_re = third[:, :LANES] * fourth[:, :LANES] - third[:, LANES:] * fourth[:, LANES:]
        far_im = -(third[:, :LANES] * fourth[:, LANES:] + third[:, LANES:] * fourth[:, :LANES])
        near[0:144] = e1[:, :LANES] * e2[:, :LANES] - e1[:, LANES:] * e2[:, LANES:]
        near[144:288] = e1[:, :LANES] * e2[:, LANES:] + e1[:, LANES:] * e2[:, :LANES]

        point = floor_div(modes, BR)
        coords = [(point >> 8).astype(jnp.float32), ((point >> 4) & 15).astype(jnp.float32), (point & 15).astype(jnp.float32)]
        shift = jnp.zeros((8, LANES), jnp.float32)
        for which in range(3):
            for axis in range(3):
                column = cell[:, 3 * which + axis : 3 * which + axis + 1]
                term = column * coords[axis][which + 1 : which + 2, :]
                shift = shift + term if which == 0 else shift - term
        step = shift.astype(jnp.int32) & 15
        cosine, sine = cosine_of(step), cosine_of((step - 4) & 15)
        for k in range(8):
            c, s = cosine[k : k + 1, :], sine[k : k + 1, :]
            wide[144 * k : 144 * (k + 1), :LANES] = (c * far_re - s * far_im).astype(jnp.bfloat16)
            wide[144 * k : 144 * (k + 1), LANES:] = (c * far_im + s * far_re).astype(jnp.bfloat16)

        freqs = [freqs_of[k : k + 1] for k in range(4)]
        occupied = [1.0 / (jnp.exp(f) - 1.0) for f in freqs]
        mismatch = freqs[0] + freqs[1] - freqs[2] - freqs[3]
        delta = jnp.exp(-((mismatch / SMEARING) ** 2)) / (SMEARING * math.sqrt(math.pi))
        weight = (1.0 + occupied[1]) * occupied[2] * occupied[3] / occupied[0]
        product = freqs[0] * freqs[1] * freqs[2] * freqs[3]
        number = LANES * (begin + index) + lax.broadcasted_iota(jnp.int32, (1, LANES), 1)
        valid = (raw[1:2, :] >= 0) & (number < count)
        scale[...] = jnp.where(valid, delta * weight / product, 0.0)

    def contract(wide, near, scale, term):
        weighted = jnp.dot(phi[...], wide[...], preferred_element_type=jnp.float32)
        w_re, w_im = weighted[:, :LANES], weighted[:, LANES:]
        near_re, near_im = near[0:144], near[144:288]
        value_re = jnp.sum(near_re * w_re - near_im * w_im, axis=0, keepdims=True)
        value_im = jnp.sum(near_re * w_im + near_im * w_re, axis=0, keepdims=True)
        term[...] = (value_re * value_re + value_im * value_im) * scale[...]

    def scatter(index, term):
        first = jnp.maximum(dense[begin + index][0:1, :], 0)
        high = floor_div(first, 192)
        low = first - 192 * high
        placed = jnp.where(lax.broadcasted_iota(jnp.int32, (NB, LANES), 0) == high, term, 0.0)
        one = placed.astype(jnp.bfloat16)
        rest = placed - one.astype(jnp.float32)
        two = rest.astype(jnp.bfloat16)
        three = (rest - two.astype(jnp.float32)).astype(jnp.bfloat16)
        spot = jnp.where(lax.broadcasted_iota(jnp.int32, (256, LANES), 0) == low, 1.0, 0.0).astype(jnp.bfloat16)
        sums[...] += lax.dot_general(
            jnp.concatenate([one, two, three], axis=0), spot, NT, preferred_element_type=jnp.float32
        )

    sides = (
        (rows_a, held_a, vectors_a, freqs_a, scale_a, wide_a, near_a, term_a, 0),
        (rows_b, held_b, vectors_b, freqs_b, scale_b, wide_b, near_b, term_b, 1),
    )

    def step_of(i, side):
        at, held, vectors, freqs_of, scale, wide, near, term, which = sides[side]
        _, _, next_vectors, next_freqs, next_scale, next_wide, next_near, last_term, _ = sides[1 - side]
        fetch(i + 2, at, which).wait()
        scatter(jnp.maximum(i - 1, 0), last_term[...])
        contract(wide, near, scale, term)
        products(i + 1, next_vectors, next_freqs, next_wide, next_near, next_scale)
        vectors_of(at, i + 2, held, vectors, freqs_of)
        fetch(i + 4, at, which).start()

    term_b[...] = jnp.zeros_like(term_b)
    fetch(0, rows_a, 0).start()
    fetch(1, rows_b, 1).start()
    fetch(0, rows_a, 0).wait()
    vectors_of(rows_a, 0, held_a, vectors_a, freqs_a)
    fetch(2, rows_a, 0).start()
    fetch(1, rows_b, 1).wait()
    products(0, vectors_a, freqs_a, wide_a, near_a, scale_a)
    vectors_of(rows_b, 1, held_b, vectors_b, freqs_b)
    fetch(3, rows_b, 1).start()

    def two_blocks(it, carry):
        step_of(2 * it, 0)

        @pl.when(2 * it + 1 < total)
        def _():
            step_of(2 * it + 1, 1)

        return carry

    lax.fori_loop(0, (total + 1) // 2, two_blocks, 0)
    scatter(jnp.maximum(total - 1, 0), jnp.where(total % 2 == 1, term_a[...], term_b[...]))
    fetch(0, rows_a, 0).wait()
    fetch(0, rows_b, 1).wait()
    result = sums[0:16] + sums[16:32] + sums[32:48]
    for w in range(NB):
        out[w] = result[w : w + 1]


def quartet_sums(*operands):
    vmem = pl.BlockSpec(memory_space=pltpu.VMEM)
    smem = pl.BlockSpec(memory_space=pltpu.SMEM)
    pinned = [pltpu.with_memory_space_constraint(a, pltpu.SMEM if k == 2 else pltpu.VMEM) for k, a in enumerate(operands)]
    return pl.pallas_call(
        quartet_kernel,
        out_shape=pltpu.VMEM((NB, 1, 256), jnp.float32),
        in_specs=[vmem, vmem, smem, vmem, vmem, vmem, vmem],
        out_specs=vmem,
        scratch_shapes=[
            pltpu.VMEM((1152, 256), jnp.bfloat16),
            pltpu.VMEM((1152, 256), jnp.bfloat16),
            pltpu.VMEM((288, LANES), jnp.float32),
            pltpu.VMEM((288, LANES), jnp.float32),
            pltpu.VMEM((1, LANES), jnp.float32),
            pltpu.VMEM((1, LANES), jnp.float32),
            pltpu.VMEM((1, LANES), jnp.float32),
            pltpu.VMEM((1, LANES), jnp.float32),
            pltpu.VMEM((4, LANES), jnp.float32),
            pltpu.VMEM((4, LANES), jnp.float32),
            pltpu.VMEM((64, 256), jnp.bfloat16),
            pltpu.VMEM((64, 256), jnp.bfloat16),
            pltpu.VMEM((4 * LANES, LANES), jnp.bfloat16),
            pltpu.VMEM((4 * LANES, LANES), jnp.bfloat16),
            pltpu.SMEM((4, LANES), jnp.int32),
            pltpu.SMEM((4, LANES), jnp.int32),
            pltpu.VMEM((4 * NB + 8, 8, LANES), jnp.int32),
            pltpu.VMEM((48, 256), jnp.float32),
            pltpu.SemaphoreType.DMA((2,)),
        ],
        compiler_params=pltpu.CompilerParams(
            vmem_limit_bytes=16 << 20
        ),
        name="quartets",
    )(*pinned)


def reduce_kernel(part, out, arrived, send, recv):
    pb, wa = lax.axis_index("pb"), lax.axis_index("wa")
    barrier = pltpu.get_barrier_semaphore()
    peers = [lax.rem(wa + k, NB) for k in range(1, NB)]
    for peer in peers:
        pl.semaphore_signal(barrier, inc=1, device_id=(pb, peer), device_id_type=MESH)
    pl.semaphore_wait(barrier, NB - 1)
    for k, peer in enumerate(peers):
        pltpu.make_async_remote_copy(
            src_ref=part.at[peer], dst_ref=arrived.at[k], send_sem=send.at[0], recv_sem=recv.at[0],
            device_id=(pb, peer), device_id_type=MESH,
        ).start()
    everything = pltpu.make_async_remote_copy(
        src_ref=part.at[pl.ds(0, NB - 1)], dst_ref=arrived, send_sem=send.at[0], recv_sem=recv.at[0],
        device_id=(pb, peers[0]), device_id_type=MESH,
    )
    everything.wait_recv()
    total = part[wa]
    for k in range(NB - 1):
        total = total + arrived[k]
    out[...] = total
    everything.wait_send()


def reduce_over_wa(part):
    vmem = pl.BlockSpec(memory_space=pltpu.VMEM)
    return pl.pallas_call(
        reduce_kernel,
        out_shape=jax.ShapeDtypeStruct((1, 256), jnp.float32),
        in_specs=[vmem],
        out_specs=vmem,
        scratch_shapes=[
            pltpu.VMEM((NB - 1, 1, 256), jnp.float32),
            pltpu.SemaphoreType.DMA((1,)),
            pltpu.SemaphoreType.DMA((1,)),
        ],
        compiler_params=pltpu.CompilerParams(collective_id=1, has_side_effects=True, vmem_limit_bytes=1 << 20),
        name="reduce_wa",
    )(pltpu.with_memory_space_constraint(part, pltpu.VMEM))


def body(quartets, counts, eig, freq, phi, cells):
    dealt = quartets.reshape(2, 2, 2, 4, 4, LANES)
    held = exchange(eig, freq.reshape(24, LANES), dealt, phi, cells, counts)
    part = quartet_sums(*held)
    return reduce_over_wa(part)[0, :192]


def solution(mesh):
    placed = (P(("pb", "wa"), None, None), P(("pb", "wa")), P(None, "pb"), P("pb"), P(), P())
    return jax.shard_map(body, mesh=mesh, in_specs=placed, out_specs=P(("pb", "wa")), check_vma=False)
```
